128 devices in a mesh: own: 32 (over x, z, core), rep: 4 (over y).
Axes of the slice: x: 4, y: 4, z: 4, core: 2. Of those that a mesh axis runs over, the one named last changes fastest.
Arguments:
- block_pool: bfloat16 [8192, 64, 576], P(('own', 'rep')), may hold values from -16 to 16
- sel_index: int32 [4096], P(('own', 'rep')), may hold values from 0 to 63
- sel_layer: int32 [4096], P(('own', 'rep')), may hold values from 0 to 15, as said below
- counts: int32 [128], P(('own', 'rep')), may hold values from 8 to 32, as said below
Outputs:
- quant_codes: bfloat16 [32, 4, 32, 8, 18432], P('own', 'rep')
- quant_steps: float32 [32, 288], P('own')
- clip_error: float32 [32, 288], P('own')
The draws below stay inside these ranges and needn't reach their ends.
Inputs may be any that keep to these rules, and one draw needn't show every extreme that they name: `sel_layer`: among the 32 entries of one device, at most 8 name any one layer; the first 8 entries of every device all name one and the same layer. `counts`: some device has all 32 entries live.
All inputs are finite; a program needn't handle non-finite values.
Results may differ from the reference program's by a relative error of at most 0.001.
Values may be sent and summed in bfloat16 or wider, within the bound.
A program may use at most 128 MiB of HBM per device.

```python
import math
import jax
import jax.numpy as jnp
from jax import lax

LATENT = 576
TOKB = 64
SLICES = 2
CAP = 8
POOL_DEV = 64
SEL_DEV = 32
LAYERS = 16
HALF = 288
SEL_ALL = 4096
N_OWN = 32
N_REP = 4


def draw_block_pool(key, part):
    base_key = jax.random.fold_in(key, 11)
    key_chan, key_base, key_rows = jax.random.split(base_key, 3)
    shape = (N_OWN * N_REP * POOL_DEV, TOKB, LATENT)
    channel = jnp.exp(jax.random.uniform(key_chan, (LATENT,), jnp.float32, math.log(0.3), math.log(3.0)))
    base = jnp.clip(jax.random.normal(key_base, shape, jnp.float32), -5.0, 5.0)
    row_scale = jnp.ones((shape[0], 1, 1), jnp.float32)
    return (base * channel * row_scale).astype(jnp.bfloat16)


def draw_sel_layer(key, part):
    devices = N_OWN * N_REP
    base_key = jax.random.fold_in(key, 31)
    key_star, key_perm = jax.random.split(base_key, 2)
    star_layer = jax.random.randint(key_star, (), 0, LAYERS)
    items = jnp.arange((LAYERS - 1) * CAP, dtype=jnp.int32) // CAP
    device_keys = jax.random.split(key_perm, devices)

    def per_device(device_key):
        shuffled = jax.random.permutation(device_key, items)[:SEL_DEV - CAP]
        others = (star_layer + 1 + shuffled) % LAYERS
        front = jnp.full((CAP,), star_layer, jnp.int32)
        return jnp.concatenate([front, others.astype(jnp.int32)])
    return jax.vmap(per_device)(device_keys).reshape(-1).astype(jnp.int32)


def draw_counts(key, part):
    devices = N_OWN * N_REP
    base_key = jax.random.fold_in(key, 21)
    key_low, key_full, key_first = jax.random.split(base_key, 3)
    lower = jax.random.randint(key_low, (devices,), CAP, CAP + (SEL_DEV - CAP) // 3 + 1)
    full_mask = jax.random.randint(key_full, (devices,), 0, 8) == 0
    first_full = jax.random.randint(key_first, (), 0, devices)
    full_mask = full_mask | (jnp.arange(devices) == first_full)
    return jnp.where(full_mask, SEL_DEV, lower).astype(jnp.int32)


def touch_ends(drawn, stream_key, low, high):
    index_at = [jax.random.randint(jax.random.fold_in(stream_key, axis), (), 0, length) for axis, length in enumerate(drawn.shape)]
    main_axis = drawn.shape.index(max(drawn.shape))
    neighbour = index_at[:main_axis] + [(index_at[main_axis] + 1) % drawn.shape[main_axis]] + index_at[main_axis + 1:]
    return drawn.at[tuple(index_at)].set(low).at[tuple(neighbour)].set(high)


def setup_inputs(seed: int = 0) -> dict:
    seeds = jax.random.split(jax.random.key(seed), 5)
    return {
        "block_pool": draw_block_pool(jax.random.fold_in(seeds[4], 71), 0),
        "sel_index": touch_ends(jax.random.randint(seeds[1], (SEL_ALL,), 0, POOL_DEV), jax.random.fold_in(seeds[1], 1), 0, POOL_DEV - 1).astype(jnp.int32),
        "sel_layer": draw_sel_layer(jax.random.fold_in(seeds[4], 71), 0),
        "counts": draw_counts(jax.random.fold_in(seeds[4], 71), 0),
    }


headroom = 0.5


def slot_table(index_row, layer_row, live_count, group_layer, capacity):
    n_select = index_row.shape[0]
    is_live = jnp.arange(n_select) < live_count
    matches = (layer_row[None, :] == group_layer[:, None]) & is_live[None, :]
    ranking = jnp.cumsum(matches.astype(jnp.int32), axis=1) - 1
    slot_hit = matches[:, None, :] & (ranking[:, None, :] == jnp.arange(capacity)[None, :, None])
    chosen = jnp.sum(jnp.where(slot_hit, index_row[None, None, :], 0), axis=2).astype(jnp.int32)
    filled = jnp.any(slot_hit, axis=2)
    return chosen, filled


def reference(block_pool, sel_index, sel_layer, counts):
    devices = N_OWN * N_REP
    group_layer = (jnp.arange(N_OWN) // SLICES).astype(jnp.int32)
    index_rows = sel_index.reshape(devices, SEL_DEV)
    layer_rows = sel_layer.reshape(devices, SEL_DEV)
    chosen, filled = jax.vmap(lambda a, b, c: slot_table(a, b, c, group_layer, CAP))(index_rows, layer_rows, counts)
    pools = block_pool.reshape(devices, POOL_DEV, TOKB, SLICES, HALF)
    device_ids = jnp.arange(devices)[:, None]
    denominator = float(N_OWN * N_REP * CAP * TOKB)

    def one_group(group):
        slice_of = group % SLICES
        picked = jnp.take(chosen, group, axis=1)
        keep_mask = jnp.take(filled, group, axis=1)
        blocks = pools[device_ids, picked, :, slice_of]
        blocks = jnp.where(keep_mask[:, :, None, None], blocks, jnp.zeros((), blocks.dtype))
        values = blocks.astype(jnp.float32)
        peak_abs = jnp.max(jnp.abs(values), axis=(0, 1, 2))
        step_size = headroom * jnp.maximum(peak_abs, 1.0) / 127.0
        encoded = jnp.clip(values / step_size, -127.0, 127.0).astype(jnp.bfloat16)
        encoded = lax.optimization_barrier(encoded)
        decoded = encoded.astype(jnp.float32) * step_size
        sq_error = jnp.sum((values - decoded) ** 2, axis=(0, 1, 2))
        error_out = sq_error / (step_size * step_size * denominator)
        codes_out = encoded.reshape(N_OWN, N_REP, CAP, TOKB * HALF).transpose(1, 0, 2, 3)
        return codes_out, step_size, error_out

    quant_codes, quant_steps, clip_error = lax.map(one_group, jnp.arange(N_OWN))
    return quant_codes, quant_steps, clip_error
```

```python
import functools
import jax
import jax.numpy as jnp
from jax import lax
from jax.experimental import pallas as pl
from jax.experimental.pallas import tpu as pltpu
from jax.sharding import PartitionSpec as P

HEADROOM = 0.5
HALF = 288
PIECE = 4 * HALF
TOK = 64
STEP_TOK = 16
CAP = 8
LAYERS = 16
SEL = 32
DENOM = 32.0 * 4.0 * 8.0 * 64.0


def flatten_kernel(idx_ref, layer_ref, count_ref, pool_ref, out_ref, blocks, picks, seen, sems):
    step = pl.program_id(0)
    rows = STEP_TOK * LAYERS * CAP
    cols = SEL * STEP_TOK

    @pl.when(step == 0)
    def _():
        for j in range(SEL):
            pltpu.make_async_copy(pool_ref.at[idx_ref[j]], blocks.at[j], sems.at[j]).start()
        for layer in range(LAYERS):
            seen[layer] = 0
        col = lax.broadcasted_iota(jnp.int32, (1, cols), 1)
        key = jnp.full((1, cols), -1, jnp.int32)
        live = count_ref[0]
        for j in range(SEL):
            layer = layer_ref[j]
            rank = seen[layer]
            seen[layer] = rank + 1
            slot = jnp.where(j < live, layer * CAP + rank, -1)
            key = jnp.where(col // STEP_TOK == j, slot, key)
        row = lax.broadcasted_iota(jnp.int32, (rows, cols), 0)
        hit = (row % (LAYERS * CAP) == key) & (row // (LAYERS * CAP) == col % STEP_TOK)
        picks[...] = jnp.where(hit, 1.0, 0.0).astype(jnp.bfloat16)
        for j in range(SEL):
            pltpu.make_async_copy(pool_ref.at[idx_ref[j]], blocks.at[j], sems.at[j]).wait()

    start = pl.multiple_of(step * STEP_TOK, STEP_TOK)
    data = blocks[:, pl.ds(start, STEP_TOK), :].reshape(cols, 2 * HALF)
    slots = LAYERS * CAP
    for part in range(STEP_TOK // 4):
        moved = jnp.dot(picks[part * 4 * slots:(part + 1) * 4 * slots, :], data, preferred_element_type=jnp.float32)
        for half in range(2):
            lanes = [moved[t * slots:(t + 1) * slots, half * HALF:(half + 1) * HALF] for t in range(4)]
            flat = jnp.concatenate(lanes, axis=1).astype(jnp.bfloat16)
            out_ref[:, half, :, part * PIECE:(part + 1) * PIECE] = flat.reshape(LAYERS, CAP, PIECE)


def flatten(block_pool, sel_index, sel_layer, counts):
    smem = pl.BlockSpec(memory_space=pltpu.SMEM)
    return pl.pallas_call(
        flatten_kernel,
        grid=(TOK // STEP_TOK,),
        out_shape=jax.ShapeDtypeStruct((LAYERS, 2, CAP, TOK * HALF), jnp.bfloat16),
        in_specs=[smem, smem, smem, pl.BlockSpec(memory_space=pl.ANY)],
        out_specs=pl.BlockSpec((LAYERS, 2, CAP, STEP_TOK * HALF), lambda i: (0, 0, 0, i)),
        scratch_shapes=[
            pltpu.VMEM((SEL, TOK, 2 * HALF), jnp.bfloat16),
            pltpu.VMEM((STEP_TOK * LAYERS * CAP, SEL * STEP_TOK), jnp.bfloat16),
            pltpu.SMEM((LAYERS,), jnp.int32),
            pltpu.SemaphoreType.DMA((SEL,)),
        ],
        compiler_params=pltpu.CompilerParams(dimension_semantics=("arbitrary",), vmem_limit_bytes=48 << 20),
        name="flatten",
    )(sel_index, sel_layer, counts, block_pool)


def rep_exchange(value, inbox, send_sems, recv_sems):
    reps = lax.axis_size("rep")
    me = lax.axis_index("rep")
    inbox[0] = value
    copies = []
    for k in range(1, reps):
        copies.append(pltpu.make_async_remote_copy(
            src_ref=inbox.at[0], dst_ref=inbox.at[k],
            send_sem=send_sems.at[k], recv_sem=recv_sems.at[k],
            device_id={"rep": lax.rem(me + k, reps)}, device_id_type=pl.DeviceIdType.MESH))
    for copy in copies:
        copy.start()
    for copy in copies:
        copy.wait()


def rep_barrier_signal():
    reps = lax.axis_size("rep")
    me = lax.axis_index("rep")
    barrier = pltpu.get_barrier_semaphore()
    for k in range(1, reps):
        pl.semaphore_signal(barrier, inc=1, device_id={"rep": lax.rem(me + k, reps)},
                            device_id_type=pl.DeviceIdType.MESH)
    return barrier


def fold4(row):
    return [row[:, k * HALF:(k + 1) * HALF] for k in range(4)]


def peak_kernel(got_ref, steps_ref, inbox, send_sems, recv_sems):
    barrier = rep_barrier_signal()
    rows = got_ref.shape[0]

    def chunk(i, peak):
        at = pl.multiple_of(i * 16, 16)
        for q in range(TOK // 4):
            part = jnp.abs(got_ref[pl.ds(at, 16), q * PIECE:(q + 1) * PIECE])
            peak = jnp.maximum(peak, part)
        return peak

    peak = lax.fori_loop(0, rows // 16, chunk, jnp.zeros((16, PIECE), jnp.bfloat16))
    row = jnp.max(peak.astype(jnp.float32), axis=0, keepdims=True)
    a, b, c, d = fold4(row)
    row = jnp.maximum(jnp.maximum(a, b), jnp.maximum(c, d))
    pl.semaphore_wait(barrier, 3)
    rep_exchange(jnp.concatenate([row, row[:, :384 - HALF]], axis=1), inbox, send_sems, recv_sems)
    top = jnp.maximum(jnp.maximum(inbox[0], inbox[1]), jnp.maximum(inbox[2], inbox[3]))
    steps_ref[...] = HEADROOM * jnp.maximum(top[:, :HALF], 1.0) / 127.0


def small_scratch():
    return [
        pltpu.VMEM((4, 1, 384), jnp.float32),
        pltpu.SemaphoreType.DMA((4,)),
        pltpu.SemaphoreType.DMA((4,)),
    ]


def peak_steps(got):
    vmem = pl.BlockSpec(memory_space=pltpu.VMEM)
    return pl.pallas_call(
        peak_kernel,
        out_shape=jax.ShapeDtypeStruct((1, HALF), jnp.float32),
        in_specs=[vmem], out_specs=vmem,
        scratch_shapes=small_scratch(),
        compiler_params=pltpu.CompilerParams(collective_id=0, has_side_effects=True, vmem_limit_bytes=24 << 20),
        name="peak_steps",
    )(got)


def error_kernel(sums_ref, out_ref, inbox, send_sems, recv_sems):
    barrier = rep_barrier_signal()
    pl.semaphore_wait(barrier, 3)
    rep_exchange(sums_ref[...], inbox, send_sems, recv_sems)
    total = (inbox[0] + inbox[1]) + (inbox[2] + inbox[3])
    out_ref[...] = total[:, :HALF] * (1.0 / DENOM)


def error_mean(sums):
    vmem = pl.BlockSpec(memory_space=pltpu.VMEM)
    return pl.pallas_call(
        error_kernel,
        out_shape=jax.ShapeDtypeStruct((1, HALF), jnp.float32),
        in_specs=[vmem], out_specs=vmem,
        scratch_shapes=small_scratch(),
        compiler_params=pltpu.CompilerParams(collective_id=1, has_side_effects=True),
        name="error_mean",
    )(sums)


ENC_ROWS = 32


def encode_kernel(got_ref, steps_ref, codes_ref, sums_ref, inv_ref, acc_ref):
    step = pl.program_id(0)

    @pl.when(step == 0)
    def _():
        inv = 1.0 / steps_ref[...]
        inv_ref[...] = jnp.broadcast_to(jnp.concatenate([inv] * 4, axis=1), inv_ref.shape)
        acc_ref[...] = jnp.zeros_like(acc_ref)

    for q in range(TOK // 4):
        lanes = slice(q * PIECE, (q + 1) * PIECE)
        scaled = got_ref[:, lanes].astype(jnp.float32).reshape(ENC_ROWS // 8, 8, PIECE) * inv_ref[...][None]
        code = jnp.clip(scaled, -127.0, 127.0).astype(jnp.bfloat16)
        gap = scaled - code.astype(jnp.float32)
        codes_ref[:, lanes] = code.reshape(ENC_ROWS, PIECE)
        acc_ref[...] += jnp.sum(gap * gap, axis=0)

    @pl.when(step == pl.num_programs(0) - 1)
    def _():
        row = jnp.sum(acc_ref[...], axis=0, keepdims=True)
        a, b, c, d = fold4(row)
        row = (a + b) + (c + d)
        sums_ref[...] = jnp.concatenate([row, row[:, :384 - HALF]], axis=1)


def encode(got, steps):
    rows = got.shape[0]
    return pl.pallas_call(
        encode_kernel,
        grid=(rows // ENC_ROWS,),
        out_shape=(jax.ShapeDtypeStruct(got.shape, jnp.bfloat16), jax.ShapeDtypeStruct((1, 384), jnp.float32)),
        in_specs=[pl.BlockSpec((ENC_ROWS, TOK * HALF), lambda i: (i, 0)), pl.BlockSpec((1, HALF), lambda i: (0, 0))],
        out_specs=(pl.BlockSpec((ENC_ROWS, TOK * HALF), lambda i: (i, 0)), pl.BlockSpec((1, 384), lambda i: (0, 0))),
        scratch_shapes=[pltpu.VMEM((8, PIECE), jnp.float32), pltpu.VMEM((8, PIECE), jnp.float32)],
        compiler_params=pltpu.CompilerParams(dimension_semantics=("arbitrary",), vmem_limit_bytes=24 << 20),
        name="encode",
    )(got, steps)


def body(block_pool, sel_index, sel_layer, counts):
    parted = flatten(block_pool, sel_index, sel_layer, counts).reshape(2 * LAYERS, CAP, TOK * HALF)
    got = lax.all_to_all(parted, "own", split_axis=0, concat_axis=0, tiled=True)
    got = got.reshape(2 * LAYERS * CAP, TOK * HALF)
    steps = peak_steps(got)
    codes, sums = encode(got, steps)
    error = error_mean(sums)
    return codes.reshape(1, 1, 2 * LAYERS, CAP, TOK * HALF), steps, error


def solution(mesh):
    return jax.shard_map(
        body,
        mesh=mesh,
        in_specs=(
            P(("own", "rep"), None, None),
            P(("own", "rep")),
            P(("own", "rep")),
            P(("own", "rep")),
        ),
        out_specs=(P("own", "rep", None, None, None), P("own", None), P("own", None)),
        check_vma=False,
    )
```

```python
import functools
import jax
import jax.numpy as jnp
from jax import lax
from jax.experimental import pallas as pl
from jax.experimental.pallas import tpu as pltpu
from jax.sharding import PartitionSpec as P

HEADROOM = 0.5
HALF = 288
PIECE = 4 * HALF
TOK = 64
STEP_TOK = 16
CAP = 8
LAYERS = 16
SEL = 32
CHIPS = 16
QS = 16
REST = SEL - CAP
ROOM = 32
WIDE = PIECE + 128
DENOM = 32.0 * 4.0 * 8.0 * 64.0


def flatten_kernel(idx_ref, layer_ref, count_ref, pool_ref, out_ref, blocks, picks, seen, sems):
    step = pl.program_id(0)
    rows = STEP_TOK * LAYERS * CAP
    cols = SEL * STEP_TOK

    @pl.when(step == 0)
    def _():
        for j in range(SEL):
            pltpu.make_async_copy(pool_ref.at[idx_ref[j]], blocks.at[j], sems.at[j]).start()
        for layer in range(LAYERS):
            seen[layer] = 0
        col = lax.broadcasted_iota(jnp.int32, (1, cols), 1)
        key = jnp.full((1, cols), -1, jnp.int32)
        live = count_ref[0]
        for j in range(SEL):
            layer = layer_ref[j]
            rank = seen[layer]
            seen[layer] = rank + 1
            slot = jnp.where(j < live, layer * CAP + rank, -1)
            key = jnp.where(col // STEP_TOK == j, slot, key)
        row = lax.broadcasted_iota(jnp.int32, (rows, cols), 0)
        hit = (row % (LAYERS * CAP) == key) & (row // (LAYERS * CAP) == col % STEP_TOK)
        picks[...] = jnp.where(hit, 1.0, 0.0).astype(jnp.bfloat16)
        for j in range(SEL):
            pltpu.make_async_copy(pool_ref.at[idx_ref[j]], blocks.at[j], sems.at[j]).wait()

    start = pl.multiple_of(step * STEP_TOK, STEP_TOK)
    data = blocks[:, pl.ds(start, STEP_TOK), :].reshape(cols, 2 * HALF)
    slots = LAYERS * CAP
    for part in range(STEP_TOK // 4):
        moved = jnp.dot(picks[part * 4 * slots:(part + 1) * 4 * slots, :], data, preferred_element_type=jnp.float32)
        for half in range(2):
            lanes = [moved[t * slots:(t + 1) * slots, half * HALF:(half + 1) * HALF] for t in range(4)]
            flat = jnp.concatenate(lanes, axis=1).astype(jnp.bfloat16)
            out_ref[:, half, :, part * PIECE:(part + 1) * PIECE] = flat.reshape(LAYERS, CAP, PIECE)


def flatten(block_pool, sel_index, sel_layer, counts):
    smem = pl.BlockSpec(memory_space=pltpu.SMEM)
    return pl.pallas_call(
        flatten_kernel,
        grid=(TOK // STEP_TOK,),
        out_shape=jax.ShapeDtypeStruct((LAYERS, 2, CAP, TOK * HALF), jnp.bfloat16),
        in_specs=[smem, smem, smem, pl.BlockSpec(memory_space=pl.ANY)],
        out_specs=pl.BlockSpec((LAYERS, 2, CAP, STEP_TOK * HALF), lambda i: (0, 0, 0, i)),
        scratch_shapes=[
            pltpu.VMEM((SEL, TOK, 2 * HALF), jnp.bfloat16),
            pltpu.VMEM((STEP_TOK * LAYERS * CAP, SEL * STEP_TOK), jnp.bfloat16),
            pltpu.SMEM((LAYERS,), jnp.int32),
            pltpu.SemaphoreType.DMA((SEL,)),
        ],
        compiler_params=pltpu.CompilerParams(dimension_semantics=("arbitrary",), vmem_limit_bytes=48 << 20),
        name="flatten",
    )(sel_index, sel_layer, counts, block_pool)


def rep_exchange(value, inbox, send_sems, recv_sems):
    reps = lax.axis_size("rep")
    me = lax.axis_index("rep")
    inbox[0] = value
    copies = []
    for k in range(1, reps):
        copies.append(pltpu.make_async_remote_copy(
            src_ref=inbox.at[0], dst_ref=inbox.at[k],
            send_sem=send_sems.at[k], recv_sem=recv_sems.at[k],
            device_id={"rep": lax.rem(me + k, reps)}, device_id_type=pl.DeviceIdType.MESH))
    for copy in copies:
        copy.start()
    for copy in copies:
        copy.wait()


def rep_barrier_signal():
    reps = lax.axis_size("rep")
    me = lax.axis_index("rep")
    barrier = pltpu.get_barrier_semaphore()
    for k in range(1, reps):
        pl.semaphore_signal(barrier, inc=1, device_id={"rep": lax.rem(me + k, reps)},
                            device_id_type=pl.DeviceIdType.MESH)
    return barrier


def fold4(row):
    return [row[:, k * HALF:(k + 1) * HALF] for k in range(4)]


def peak_kernel(got_ref, steps_ref, inbox, send_sems, recv_sems):
    barrier = rep_barrier_signal()
    rows = got_ref.shape[0]

    def chunk(i, peak):
        at = pl.multiple_of(i * 16, 16)
        for q in range(TOK // 4):
            part = jnp.abs(got_ref[pl.ds(at, 16), q * PIECE:(q + 1) * PIECE])
            peak = jnp.maximum(peak, part)
        return peak

    peak = lax.fori_loop(0, rows // 16, chunk, jnp.zeros((16, PIECE), jnp.bfloat16))
    row = jnp.max(peak.astype(jnp.float32), axis=0, keepdims=True)
    a, b, c, d = fold4(row)
    row = jnp.maximum(jnp.maximum(a, b), jnp.maximum(c, d))
    pl.semaphore_wait(barrier, 3)
    rep_exchange(jnp.concatenate([row, row[:, :384 - HALF]], axis=1), inbox, send_sems, recv_sems)
    top = jnp.maximum(jnp.maximum(inbox[0], inbox[1]), jnp.maximum(inbox[2], inbox[3]))
    steps_ref[...] = HEADROOM * jnp.maximum(top[:, :HALF], 1.0) / 127.0


def small_scratch():
    return [
        pltpu.VMEM((4, 1, 384), jnp.float32),
        pltpu.SemaphoreType.DMA((4,)),
        pltpu.SemaphoreType.DMA((4,)),
    ]


def peak_steps(got):
    vmem = pl.BlockSpec(memory_space=pltpu.VMEM)
    return pl.pallas_call(
        peak_kernel,
        out_shape=jax.ShapeDtypeStruct((1, HALF), jnp.float32),
        in_specs=[vmem], out_specs=vmem,
        scratch_shapes=small_scratch(),
        compiler_params=pltpu.CompilerParams(collective_id=0, has_side_effects=True, vmem_limit_bytes=24 << 20),
        name="peak_steps",
    )(got)


def error_kernel(sums_ref, out_ref, inbox, send_sems, recv_sems):
    barrier = rep_barrier_signal()
    pl.semaphore_wait(barrier, 3)
    rep_exchange(sums_ref[...], inbox, send_sems, recv_sems)
    total = (inbox[0] + inbox[1]) + (inbox[2] + inbox[3])
    out_ref[...] = total[:, :HALF] * (1.0 / DENOM)


def error_mean(sums):
    vmem = pl.BlockSpec(memory_space=pltpu.VMEM)
    return pl.pallas_call(
        error_kernel,
        out_shape=jax.ShapeDtypeStruct((1, HALF), jnp.float32),
        in_specs=[vmem], out_specs=vmem,
        scratch_shapes=small_scratch(),
        compiler_params=pltpu.CompilerParams(collective_id=1, has_side_effects=True),
        name="error_mean",
    )(sums)


ENC_ROWS = 32


def encode_kernel(got_ref, steps_ref, codes_ref, sums_ref, inv_ref, acc_ref):
    step = pl.program_id(0)

    @pl.when(step == 0)
    def _():
        inv = 1.0 / steps_ref[...]
        inv_ref[...] = jnp.broadcast_to(jnp.concatenate([inv] * 4, axis=1), inv_ref.shape)
        acc_ref[...] = jnp.zeros_like(acc_ref)

    for q in range(TOK // 4):
        lanes = slice(q * PIECE, (q + 1) * PIECE)
        scaled = got_ref[:, lanes].astype(jnp.float32).reshape(ENC_ROWS // 8, 8, PIECE) * inv_ref[...][None]
        code = jnp.clip(scaled, -127.0, 127.0).astype(jnp.bfloat16)
        gap = scaled - code.astype(jnp.float32)
        codes_ref[:, lanes] = code.reshape(ENC_ROWS, PIECE)
        acc_ref[...] += jnp.sum(gap * gap, axis=0)

    @pl.when(step == pl.num_programs(0) - 1)
    def _():
        row = jnp.sum(acc_ref[...], axis=0, keepdims=True)
        a, b, c, d = fold4(row)
        row = (a + b) + (c + d)
        sums_ref[...] = jnp.concatenate([row, row[:, :384 - HALF]], axis=1)


def encode(got, steps):
    rows = got.shape[0]
    return pl.pallas_call(
        encode_kernel,
        grid=(rows // ENC_ROWS,),
        out_shape=(jax.ShapeDtypeStruct(got.shape, jnp.bfloat16), jax.ShapeDtypeStruct((1, 384), jnp.float32)),
        in_specs=[pl.BlockSpec((ENC_ROWS, TOK * HALF), lambda i: (i, 0)), pl.BlockSpec((1, HALF), lambda i: (0, 0))],
        out_specs=(pl.BlockSpec((ENC_ROWS, TOK * HALF), lambda i: (i, 0)), pl.BlockSpec((1, 384), lambda i: (0, 0))),
        scratch_shapes=[pltpu.VMEM((8, PIECE), jnp.float32), pltpu.VMEM((8, PIECE), jnp.float32)],
        compiler_params=pltpu.CompilerParams(dimension_semantics=("arbitrary",), vmem_limit_bytes=24 << 20),
        name="encode",
    )(got, steps)


def pack_kernel(idx_ref, layer_ref, count_ref, pool_ref, star_ref, rest_ref, top_ref, blocks, picks, tops, sems):
    step = pl.program_id(0)
    size = SEL * STEP_TOK

    @pl.when(step == 0)
    def _():
        for j in range(SEL):
            pltpu.make_async_copy(pool_ref.at[idx_ref[j]], blocks.at[j], sems.at[j]).start()
        row = lax.broadcasted_iota(jnp.int32, (size, size), 0)
        col = lax.broadcasted_iota(jnp.int32, (size, size), 1)
        hit = (row % SEL == col // STEP_TOK) & (row // SEL == col % STEP_TOK)
        picks[...] = jnp.where(hit, 1.0, 0.0).astype(jnp.bfloat16)
        tops[...] = jnp.zeros_like(tops)
        for j in range(SEL):
            pltpu.make_async_copy(pool_ref.at[idx_ref[j]], blocks.at[j], sems.at[j]).wait()

    line = lax.broadcasted_iota(jnp.int32, (REST, 128), 0)
    layers = jnp.full((REST, 128), -1.0, jnp.float32)
    live = count_ref[0]
    for j in range(CAP, SEL):
        name = jnp.where(j < live, layer_ref[j], -1).astype(jnp.float32)
        layers = jnp.where(line == j - CAP, name, layers)
    layers = layers.astype(jnp.bfloat16)

    start = pl.multiple_of(step * STEP_TOK, STEP_TOK)
    data = blocks[:, pl.ds(start, STEP_TOK), :].reshape(size, 2 * HALF)
    for part in range(STEP_TOK // 4):
        moved = jnp.dot(picks[part * 4 * SEL:(part + 1) * 4 * SEL, :], data, preferred_element_type=jnp.float32)
        for half in range(2):
            lanes = [moved[t * SEL:(t + 1) * SEL, half * HALF:(half + 1) * HALF] for t in range(4)]
            flat = jnp.concatenate(lanes, axis=1)
            star_ref[half, part] = flat[:CAP].astype(jnp.bfloat16)
            rest_ref[part, half, :, :PIECE] = flat[CAP:].astype(jnp.bfloat16)
            rest_ref[part, half, :, PIECE:] = layers
            tops[half] = jnp.maximum(tops[half], jnp.abs(flat[:CAP]))

    @pl.when(step == pl.num_programs(0) - 1)
    def _():
        for half in range(2):
            top_ref[half] = pad_row(fold_max(jnp.max(tops[half], axis=0, keepdims=True)))


def fold_max(row):
    a, b, c, d = fold4(row)
    return jnp.maximum(jnp.maximum(a, b), jnp.maximum(c, d))


def pad_row(row):
    return jnp.concatenate([row, jnp.zeros((1, 384 - HALF), jnp.float32)], axis=1)


def pack(block_pool, sel_index, sel_layer, counts):
    smem = pl.BlockSpec(memory_space=pltpu.SMEM)
    parts = STEP_TOK // 4
    return pl.pallas_call(
        pack_kernel,
        grid=(TOK // STEP_TOK,),
        out_shape=(
            jax.ShapeDtypeStruct((2, QS, CAP, PIECE), jnp.bfloat16),
            jax.ShapeDtypeStruct((QS, 2, REST, WIDE), jnp.bfloat16),
            jax.ShapeDtypeStruct((2, 1, 384), jnp.float32),
        ),
        in_specs=[smem, smem, smem, pl.BlockSpec(memory_space=pl.ANY)],
        out_specs=(
            pl.BlockSpec((2, parts, CAP, PIECE), lambda i: (0, i, 0, 0)),
            pl.BlockSpec((parts, 2, REST, WIDE), lambda i: (i, 0, 0, 0)),
            pl.BlockSpec((2, 1, 384), lambda i: (0, 0, 0)),
        ),
        scratch_shapes=[
            pltpu.VMEM((SEL, TOK, 2 * HALF), jnp.bfloat16),
            pltpu.VMEM((SEL * STEP_TOK, SEL * STEP_TOK), jnp.bfloat16),
            pltpu.VMEM((2, CAP, PIECE), jnp.float32),
            pltpu.SemaphoreType.DMA((SEL,)),
        ],
        compiler_params=pltpu.CompilerParams(dimension_semantics=("arbitrary",), vmem_limit_bytes=24 << 20),
        name="pack",
    )(sel_index, sel_layer, counts, block_pool)


def tree(star):
    sx, sz = divmod(star, 4)

    def at(dx, dz):
        return (sx + dx) % 4 * 4 + (sz + dz) % 4

    near = [at(0, 1), at(1, 0), at(0, 3), at(3, 0)]
    diag = [at(1, 1), at(1, 3), at(3, 3), at(3, 1)]
    third = [at(1, 2), at(2, 3), at(3, 2), at(2, 1)]
    straight = [(at(0, 2), 0, 2), (at(2, 0), 1, 3)]
    far = at(2, 2)
    role = {star: 0, far: 4}
    hop = {}
    up = {}
    origin = {}
    shift = {}
    for r in range(4):
        role[near[r]], role[diag[r]], role[third[r]] = 1, 2, 3
        up[near[r]], up[diag[r]], up[third[r]] = star, near[r], diag[r]
        hop[diag[r]] = [(near[r], k) for k in range(4)]
        hop[third[r]] = [(diag[r], k) for k in range(4)]
    hop[far] = [(third[r], 0) for r in range(4)]
    for chip, a, b in straight:
        role[chip] = 5
        hop[chip] = [(near[a], 9), (near[a], 10), (near[b], 9), (near[b], 10)]
        for r, first in ((a, 0), (b, 2)):
            origin[near[r]] = (diag[r], third[r], far, chip)
            shift[near[r]] = (r, first)
    return role, hop, up, origin, shift


def pick(index, table, default=0):
    out = jnp.int32(default)
    for key, value in table.items():
        out = jnp.where(index == key, jnp.int32(value), out)
    return out


MESH = pl.DeviceIdType.MESH


def move_kernel(star, star_ref, rest_ref, top_ref, got_ref, few_ref, map_ref, info_ref,
                mail, chosen, inbox, relay, tops, inrep,
                mail_send, mail_recv, few_send, few_recv, own_send, pass_send, relay_recv, star_recv,
                top_send, top_recv, rep_send, rep_recv, local_sem):
    own = lax.axis_index("own")
    rep = lax.axis_index("rep")
    n_own = 2 * CHIPS
    chip = own // 2
    core = own % 2
    role_of, hop_of, up_of, origin_of, shift_of = tree(star)
    role = pick(chip, role_of)
    up = pick(chip, up_of)
    is_star = role == 0
    not_star = role != 0

    barrier = pltpu.get_barrier_semaphore()

    @pl.loop(1, n_own)
    def _(k):
        pl.semaphore_signal(barrier, inc=1, device_id={"own": lax.rem(own + k, n_own)}, device_id_type=MESH)

    for k in range(1, 4):
        pl.semaphore_signal(barrier, inc=1, device_id={"rep": lax.rem(rep + k, 4)}, device_id_type=MESH)
    pl.semaphore_wait(barrier, n_own - 1 + 3)

    def remote(src, dst, send, recv, to):
        return pltpu.make_async_remote_copy(src_ref=src, dst_ref=dst, send_sem=send, recv_sem=recv,
                                            device_id={"own": to}, device_id_type=MESH)

    def mail_copy(to, frm):
        return remote(rest_ref.at[to // 2, to % 2], mail.at[frm], mail_send.at[to], mail_recv.at[frm], to)

    @pl.loop(1, n_own)
    def _(k):
        mail_copy(lax.rem(own + k, n_own), own).start()

    def top_copy(half, frm):
        return remote(top_ref.at[half], tops.at[frm], top_send.at[half], top_recv.at[frm], 2 * star + half)

    for half in range(2):
        @pl.when(own != 2 * star + half)
        def _():
            top_copy(half, own).start()

        @pl.when(own == 2 * star + half)
        def _():
            tops[own] = top_ref[half]

    def near_copy(half):
        return remote(star_ref.at[half], got_ref.at[own], own_send.at[half], star_recv.at[own], 2 * star + half)

    def hop_copy(k):
        to = pick(chip, {c: h[k][0] for c, h in hop_of.items()}) * 2 + core
        slot = pick(chip, {c: h[k][1] for c, h in hop_of.items()})
        return remote(star_ref.at[:, pl.ds(4 * k, 4)], relay.at[slot], own_send.at[k], relay_recv.at[slot], to)

    @pl.when(role == 1)
    def _():
        for half in range(2):
            near_copy(half).start()

    @pl.when(role > 1)
    def _():
        for k in range(4):
            hop_copy(k).start()

    def keep_copy():
        return pltpu.make_async_copy(star_ref.at[core], got_ref.at[own], local_sem.at[0])

    def partner_copy():
        return remote(star_ref.at[1 - core], got_ref.at[own], own_send.at[0], star_recv.at[own], 2 * star + 1 - core)

    @pl.when(is_star)
    def _():
        keep_copy().start()
        partner_copy().start()

    def relay_in(k):
        return remote(relay.at[k], relay.at[k], pass_send.at[k, 0], relay_recv.at[k], own)

    def pass_near(k, half):
        origins = [pick(chip, {c: o[i] for c, o in origin_of.items()}) for i in range(4)]
        origin = jnp.where(k < 4, origins[0], jnp.where(k < 8, origins[1], jnp.where(k == 8, origins[2], origins[3])))
        turn = pick(chip, {c: s[0] for c, s in shift_of.items()})
        first = pick(chip, {c: s[1] for c, s in shift_of.items()})
        quarter = jnp.where(k < 4, k, jnp.where(k < 8, k - 4, jnp.where(k == 8, turn, first + k - 9)))
        frm = 2 * origin + core
        return remote(relay.at[k, half], got_ref.at[frm, pl.ds(4 * quarter, 4)],
                      pass_send.at[k, half], star_recv.at[frm], 2 * star + half)

    def pass_diag(k):
        return remote(relay.at[k], relay.at[4 + k], pass_send.at[k, 0], relay_recv.at[4 + k], 2 * up + core)

    def pass_third():
        return remote(relay.at[0], relay.at[4], pass_send.at[0, 0], relay_recv.at[4], 2 * up + core)

    def near_order(i):
        return jnp.where(i < 4, i, jnp.where(i < 6, i + 5, i - 2))

    def pass_near_range(low, high):
        @pl.when(role == 1)
        def _():
            @pl.loop(low, high)
            def _(i):
                k = near_order(i)
                relay_in(k).wait_recv()
                for half in range(2):
                    pass_near(k, half).start()

    def pass_diag_range(low, high):
        @pl.when(role == 2)
        def _():
            @pl.loop(low, high)
            def _(k):
                relay_in(k).wait_recv()
                pass_diag(k).start()

    @pl.when(role == 3)
    def _():
        relay_in(0).wait_recv()
        pass_third().start()

    pass_diag_range(0, 4)
    pass_near_range(0, 6)

    mail[own] = rest_ref[chip, core]

    @pl.loop(1, n_own)
    def _(k):
        frm = lax.rem(own + n_own - k, n_own)
        mail_copy(own, frm).wait_recv()

    many = n_own * REST
    names = mail[:, :, PIECE:].reshape(many, 128).astype(jnp.float32)
    lane = lax.broadcasted_iota(jnp.int32, (many, 128), 1).astype(jnp.float32)
    hits = jnp.where(names == lane, 1.0, 0.0)
    hits16 = hits.astype(jnp.bfloat16)
    row = lax.broadcasted_iota(jnp.int32, (many, many), 0)
    col = lax.broadcasted_iota(jnp.int32, (many, many), 1)
    before = jnp.where(col < row, 1.0, 0.0)
    same = jnp.where((col < row) & (col // REST == row // REST), 1.0, 0.0)
    rank = jnp.dot(before.astype(jnp.bfloat16), hits16, preferred_element_type=jnp.float32)
    slot = jnp.dot(same.astype(jnp.bfloat16), hits16, preferred_element_type=jnp.float32)
    rank = jnp.sum(rank * hits, axis=1, keepdims=True)
    slot = jnp.sum(slot * hits, axis=1, keepdims=True)
    total = jnp.sum(hits, axis=0, keepdims=True)
    source = (lax.broadcasted_iota(jnp.int32, (many, 128), 0) // REST).astype(jnp.float32)
    key = jnp.where(rank < ROOM, names * ROOM + rank, -1.0)
    place = jnp.where(names == chip.astype(jnp.float32), source * CAP + slot, -1.0)
    key_row = jnp.transpose(key)[:1]
    place_row = jnp.transpose(place)[:1]
    want = lax.broadcasted_iota(jnp.int32, (CHIPS * ROOM, many), 0).astype(jnp.float32)
    select = jnp.where(want == key_row, 1.0, 0.0).astype(jnp.bfloat16)
    for part in range(3):
        lanes = slice(part * 384, (part + 1) * 384)
        data = mail[:, :, lanes].reshape(many, 384)
        chosen[:, :, lanes] = jnp.dot(select, data, preferred_element_type=jnp.float32).astype(
            jnp.bfloat16).reshape(CHIPS, ROOM, 384)

    def few_copy(to, frm):
        return remote(chosen.at[to], inbox.at[frm], few_send.at[to], few_recv.at[frm], 2 * to + core)

    @pl.loop(1, CHIPS)
    def _(k):
        to = lax.rem(chip + k, CHIPS)

        @pl.when(to != star)
        def _():
            few_copy(to, chip).start()

    pass_diag_range(4, 5)
    pass_near_range(6, 11)

    spot = lax.broadcasted_iota(jnp.int32, (n_own * CAP, many), 0).astype(jnp.float32)
    spread = jnp.where(spot == place_row, 1.0, 0.0).astype(jnp.bfloat16)
    order = lax.broadcasted_iota(jnp.int32, (many, ROOM), 1).astype(jnp.float32)
    ranked = jnp.where(order == rank, 1.0, 0.0).astype(jnp.bfloat16)
    map_ref[...] = jnp.dot(spread, ranked, preferred_element_type=jnp.float32).astype(jnp.bfloat16)

    @pl.when(not_star)
    def _():
        inbox[chip] = chosen[chip]

        @pl.loop(1, CHIPS)
        def _(k):
            frm = lax.rem(chip + CHIPS - k, CHIPS)
            few_copy(chip, frm).wait_recv()

        few_ref[...] = inbox[...]
        best = jnp.max(jnp.abs(inbox[...].reshape(CHIPS * ROOM, PIECE)), axis=0, keepdims=True)
        inrep[0] = pad_row(fold_max(best.astype(jnp.float32)))

    @pl.when(is_star)
    def _():
        @pl.loop(1, n_own)
        def _(k):
            frm = lax.rem(own + n_own - k, n_own)
            remote(tops.at[frm], tops.at[frm], top_send.at[0], top_recv.at[frm], frm).wait_recv()

        inrep[0] = jnp.max(tops[...], axis=0)

    full = jnp.max(jnp.where(total > ROOM, 1.0, 0.0), axis=1, keepdims=True)
    tail = lax.broadcasted_iota(jnp.int32, (1, 384), 1)
    inrep[0] = jnp.where(tail < HALF, inrep[0], full)

    copies = [pltpu.make_async_remote_copy(
        src_ref=inrep.at[0], dst_ref=inrep.at[k], send_sem=rep_send.at[k], recv_sem=rep_recv.at[k],
        device_id={"rep": lax.rem(rep + k, 4)}, device_id_type=MESH) for k in range(1, 4)]
    for copy in copies:
        copy.start()
    for copy in copies:
        copy.wait()
    top = jnp.maximum(jnp.maximum(inrep[0], inrep[1]), jnp.maximum(inrep[2], inrep[3]))
    info_ref[...] = jnp.where(tail < HALF, HEADROOM * jnp.maximum(top, 1.0) / 127.0, top)

    @pl.when(is_star)
    def _():
        @pl.loop(1, n_own)
        def _(k):
            frm = lax.rem(own + n_own - k, n_own)
            remote(got_ref.at[frm], got_ref.at[frm], own_send.at[0], star_recv.at[frm], frm).wait_recv()

        keep_copy().wait()
        partner_copy().wait_send()

    @pl.when(role == 1)
    def _():
        for half in range(2):
            near_copy(half).wait_send()

        @pl.loop(0, 11)
        def _(k):
            for half in range(2):
                pass_near(k, half).wait_send()

    @pl.when(role > 1)
    def _():
        for k in range(4):
            hop_copy(k).wait_send()

    @pl.when(role == 2)
    def _():
        @pl.loop(0, 5)
        def _(k):
            pass_diag(k).wait_send()

    @pl.when(role == 3)
    def _():
        pass_third().wait_send()

    for half in range(2):
        @pl.when(own != 2 * star + half)
        def _():
            top_copy(half, own).wait_send()

    @pl.loop(1, n_own)
    def _(k):
        mail_copy(lax.rem(own + k, n_own), own).wait_send()

    @pl.loop(1, CHIPS)
    def _(k):
        to = lax.rem(chip + k, CHIPS)

        @pl.when(to != star)
        def _():
            few_copy(to, chip).wait_send()


def move(star, star_data, rest_data, top_data):
    vmem = pl.BlockSpec(memory_space=pltpu.VMEM)
    dma = pltpu.SemaphoreType.DMA
    n_own = 2 * CHIPS
    return pl.pallas_call(
        functools.partial(move_kernel, star),
        out_shape=(
            jax.ShapeDtypeStruct((n_own, QS, CAP, PIECE), jnp.bfloat16),
            jax.ShapeDtypeStruct((QS, ROOM, PIECE), jnp.bfloat16),
            jax.ShapeDtypeStruct((n_own * CAP, ROOM), jnp.bfloat16),
            jax.ShapeDtypeStruct((1, 384), jnp.float32),
        ),
        in_specs=[vmem, vmem, vmem],
        out_specs=(pl.BlockSpec(memory_space=pl.ANY), vmem, vmem, vmem),
        scratch_shapes=[
            pltpu.VMEM((n_own, REST, WIDE), jnp.bfloat16),
            pltpu.VMEM((CHIPS, ROOM, PIECE), jnp.bfloat16),
            pltpu.VMEM((CHIPS, ROOM, PIECE), jnp.bfloat16),
            pltpu.VMEM((11, 2, 4, CAP, PIECE), jnp.bfloat16),
            pltpu.VMEM((n_own, 1, 384), jnp.float32),
            pltpu.VMEM((4, 1, 384), jnp.float32),
            dma((n_own,)), dma((n_own,)), dma((CHIPS,)), dma((CHIPS,)),
            dma((4,)), dma((11, 2)), dma((11,)), dma((n_own,)),
            dma((2,)), dma((n_own,)), dma((4,)), dma((4,)), dma((1,)),
        ],
        compiler_params=pltpu.CompilerParams(collective_id=2 + star, has_side_effects=True, vmem_limit_bytes=40 << 20),
        name="move",
    )(star_data, rest_data, top_data)


def finish_kernel(flag_ref, got_ref, few_ref, map_ref, info_ref, codes_ref, sums_ref, inv_ref, acc_ref, done_ref):
    step = pl.program_id(0)
    star = flag_ref[0] != 0

    @pl.when(step == 0)
    def _():
        inv = 1.0 / info_ref[:, :HALF]
        inv_ref[...] = jnp.broadcast_to(jnp.concatenate([inv] * 4, axis=1), inv_ref.shape)
        acc_ref[...] = jnp.zeros_like(acc_ref)

    def code_of(data):
        scaled = data.astype(jnp.float32) * inv_ref[...][None]
        code = jnp.clip(scaled, -127.0, 127.0).astype(jnp.bfloat16)
        gap = scaled - code.astype(jnp.float32)
        acc_ref[...] += jnp.sum(gap * gap, axis=0)
        return code

    @pl.when(star)
    def _():
        for q in range(QS):
            lanes = slice(q * PIECE, (q + 1) * PIECE)
            codes_ref[:, lanes] = code_of(got_ref[:, q]).reshape(ENC_ROWS, PIECE)

    @pl.when(jnp.logical_not(star))
    def _():
        @pl.when(step == 0)
        def _():
            for q in range(QS):
                done_ref[q] = code_of(few_ref[q].reshape(ROOM // 8, 8, PIECE)).reshape(ROOM, PIECE)

        for q in range(QS):
            lanes = slice(q * PIECE, (q + 1) * PIECE)
            codes_ref[:, lanes] = jnp.dot(map_ref[...], done_ref[q], preferred_element_type=jnp.float32).astype(jnp.bfloat16)

    @pl.when(step == pl.num_programs(0) - 1)
    def _():
        row = jnp.sum(acc_ref[...], axis=0, keepdims=True)
        a, b, c, d = fold4(row)
        sums_ref[...] = pad_row((a + b) + (c + d))


def finish(flag, got, few, spread, info):
    rows = got.shape[0] * CAP
    grid_spec = pltpu.PrefetchScalarGridSpec(
        num_scalar_prefetch=1,
        grid=(rows // ENC_ROWS,),
        in_specs=[
            pl.BlockSpec((ENC_ROWS // CAP, QS, CAP, PIECE), lambda i, flag: (i * flag[0], 0, 0, 0)),
            pl.BlockSpec((QS, ROOM, PIECE), lambda i, flag: (0, 0, 0)),
            pl.BlockSpec((ENC_ROWS, ROOM), lambda i, flag: (i, 0)),
            pl.BlockSpec((1, 384), lambda i, flag: (0, 0)),
        ],
        out_specs=(
            pl.BlockSpec((ENC_ROWS, TOK * HALF), lambda i, flag: (i, 0)),
            pl.BlockSpec((1, 384), lambda i, flag: (0, 0)),
        ),
        scratch_shapes=[
            pltpu.VMEM((8, PIECE), jnp.float32),
            pltpu.VMEM((8, PIECE), jnp.float32),
            pltpu.VMEM((QS, ROOM, PIECE), jnp.bfloat16),
        ],
    )
    return pl.pallas_call(
        finish_kernel,
        grid_spec=grid_spec,
        out_shape=(jax.ShapeDtypeStruct((rows, TOK * HALF), jnp.bfloat16), jax.ShapeDtypeStruct((1, 384), jnp.float32)),
        compiler_params=pltpu.CompilerParams(dimension_semantics=("arbitrary",), vmem_limit_bytes=24 << 20),
        name="finish",
    )(flag, got, few, spread, info)


def body(block_pool, sel_index, sel_layer, counts):
    star = sel_layer[0]
    star_data, rest_data, top_data = pack(block_pool, sel_index, sel_layer, counts)
    got, few, spread, info = lax.switch(
        star, [functools.partial(move, layer) for layer in range(LAYERS)], star_data, rest_data, top_data)

    def sparse():
        flag = (lax.axis_index("own") // 2 == star).astype(jnp.int32)[None]
        codes, sums = finish(flag, got, few, spread, info)
        return codes, info[:, :HALF], sums

    def dense():
        parted = flatten(block_pool, sel_index, sel_layer, counts).reshape(2 * LAYERS, CAP, TOK * HALF)
        arrived = lax.all_to_all(parted, "own", split_axis=0, concat_axis=0, tiled=True)
        arrived = arrived.reshape(2 * LAYERS * CAP, TOK * HALF)
        steps = peak_steps(arrived)
        codes, sums = encode(arrived, steps)
        return codes, steps, sums

    codes, steps, sums = lax.cond(info[0, HALF] > 0.5, dense, sparse)
    error = error_mean(sums)
    return codes.reshape(1, 1, 2 * LAYERS, CAP, TOK * HALF), steps, error


def solution(mesh):
    return jax.shard_map(
        body,
        mesh=mesh,
        in_specs=(
            P(("own", "rep"), None, None),
            P(("own", "rep")),
            P(("own", "rep")),
            P(("own", "rep")),
        ),
        out_specs=(P("own", "rep", None, None, None), P("own", None), P("own", None)),
        check_vma=False,
    )
```

```python
import functools
import jax
import jax.numpy as jnp
from jax import lax
from jax.experimental import pallas as pl
from jax.experimental.pallas import tpu as pltpu
from jax.sharding import PartitionSpec as P

HEADROOM = 0.5
HALF = 288
PIECE = 4 * HALF
TOK = 64
STEP_TOK = 16
CAP = 8
LAYERS = 16
SEL = 32
CHIPS = 16
QS = 16
REST = SEL - CAP
ROOM = 32
BLOCK = 384
BLOCKS = 2
WIDE = PIECE + 128
DENOM = 32.0 * 4.0 * 8.0 * 64.0


def flatten_kernel(idx_ref, layer_ref, count_ref, pool_ref, out_ref, blocks, picks, seen, sems):
    step = pl.program_id(0)
    rows = STEP_TOK * LAYERS * CAP
    cols = SEL * STEP_TOK

    @pl.when(step == 0)
    def _():
        for j in range(SEL):
            pltpu.make_async_copy(pool_ref.at[idx_ref[j]], blocks.at[j], sems.at[j]).start()
        for layer in range(LAYERS):
            seen[layer] = 0
        col = lax.broadcasted_iota(jnp.int32, (1, cols), 1)
        key = jnp.full((1, cols), -1, jnp.int32)
        live = count_ref[0]
        for j in range(SEL):
            layer = layer_ref[j]
            rank = seen[layer]
            seen[layer] = rank + 1
            slot = jnp.where(j < live, layer * CAP + rank, -1)
            key = jnp.where(col // STEP_TOK == j, slot, key)
        row = lax.broadcasted_iota(jnp.int32, (rows, cols), 0)
        hit = (row % (LAYERS * CAP) == key) & (row // (LAYERS * CAP) == col % STEP_TOK)
        picks[...] = jnp.where(hit, 1.0, 0.0).astype(jnp.bfloat16)
        for j in range(SEL):
            pltpu.make_async_copy(pool_ref.at[idx_ref[j]], blocks.at[j], sems.at[j]).wait()

    start = pl.multiple_of(step * STEP_TOK, STEP_TOK)
    data = blocks[:, pl.ds(start, STEP_TOK), :].reshape(cols, 2 * HALF)
    slots = LAYERS * CAP
    for part in range(STEP_TOK // 4):
        moved = jnp.dot(picks[part * 4 * slots:(part + 1) * 4 * slots, :], data, preferred_element_type=jnp.float32)
        for half in range(2):
            lanes = [moved[t * slots:(t + 1) * slots, half * HALF:(half + 1) * HALF] for t in range(4)]
            flat = jnp.concatenate(lanes, axis=1).astype(jnp.bfloat16)
            out_ref[:, half, :, part * PIECE:(part + 1) * PIECE] = flat.reshape(LAYERS, CAP, PIECE)


def flatten(block_pool, sel_index, sel_layer, counts):
    smem = pl.BlockSpec(memory_space=pltpu.SMEM)
    return pl.pallas_call(
        flatten_kernel,
        grid=(TOK // STEP_TOK,),
        out_shape=jax.ShapeDtypeStruct((LAYERS, 2, CAP, TOK * HALF), jnp.bfloat16),
        in_specs=[smem, smem, smem, pl.BlockSpec(memory_space=pl.ANY)],
        out_specs=pl.BlockSpec((LAYERS, 2, CAP, STEP_TOK * HALF), lambda i: (0, 0, 0, i)),
        scratch_shapes=[
            pltpu.VMEM((SEL, TOK, 2 * HALF), jnp.bfloat16),
            pltpu.VMEM((STEP_TOK * LAYERS * CAP, SEL * STEP_TOK), jnp.bfloat16),
            pltpu.SMEM((LAYERS,), jnp.int32),
            pltpu.SemaphoreType.DMA((SEL,)),
        ],
        compiler_params=pltpu.CompilerParams(dimension_semantics=("arbitrary",), vmem_limit_bytes=48 << 20),
        name="flatten",
    )(sel_index, sel_layer, counts, block_pool)


def rep_exchange(value, inbox, send_sems, recv_sems):
    reps = lax.axis_size("rep")
    me = lax.axis_index("rep")
    inbox[0] = value
    copies = []
    for k in range(1, reps):
        copies.append(pltpu.make_async_remote_copy(
            src_ref=inbox.at[0], dst_ref=inbox.at[k],
            send_sem=send_sems.at[k], recv_sem=recv_sems.at[k],
            device_id={"rep": lax.rem(me + k, reps)}, device_id_type=pl.DeviceIdType.MESH))
    for copy in copies:
        copy.start()
    for copy in copies:
        copy.wait()


def rep_barrier_signal():
    reps = lax.axis_size("rep")
    me = lax.axis_index("rep")
    barrier = pltpu.get_barrier_semaphore()
    for k in range(1, reps):
        pl.semaphore_signal(barrier, inc=1, device_id={"rep": lax.rem(me + k, reps)},
                            device_id_type=pl.DeviceIdType.MESH)
    return barrier


def fold4(row):
    return [row[:, k * HALF:(k + 1) * HALF] for k in range(4)]


def peak_kernel(got_ref, steps_ref, inbox, send_sems, recv_sems):
    barrier = rep_barrier_signal()
    rows = got_ref.shape[0]

    def chunk(i, peak):
        at = pl.multiple_of(i * 16, 16)
        for q in range(TOK // 4):
            part = jnp.abs(got_ref[pl.ds(at, 16), q * PIECE:(q + 1) * PIECE])
            peak = jnp.maximum(peak, part)
        return peak

    peak = lax.fori_loop(0, rows // 16, chunk, jnp.zeros((16, PIECE), jnp.bfloat16))
    row = jnp.max(peak.astype(jnp.float32), axis=0, keepdims=True)
    a, b, c, d = fold4(row)
    row = jnp.maximum(jnp.maximum(a, b), jnp.maximum(c, d))
    pl.semaphore_wait(barrier, 3)
    rep_exchange(jnp.concatenate([row, row[:, :384 - HALF]], axis=1), inbox, send_sems, recv_sems)
    top = jnp.maximum(jnp.maximum(inbox[0], inbox[1]), jnp.maximum(inbox[2], inbox[3]))
    steps_ref[...] = HEADROOM * jnp.maximum(top[:, :HALF], 1.0) / 127.0


def small_scratch():
    return [
        pltpu.VMEM((4, 1, 384), jnp.float32),
        pltpu.SemaphoreType.DMA((4,)),
        pltpu.SemaphoreType.DMA((4,)),
    ]


def peak_steps(got):
    vmem = pl.BlockSpec(memory_space=pltpu.VMEM)
    return pl.pallas_call(
        peak_kernel,
        out_shape=jax.ShapeDtypeStruct((1, HALF), jnp.float32),
        in_specs=[vmem], out_specs=vmem,
        scratch_shapes=small_scratch(),
        compiler_params=pltpu.CompilerParams(collective_id=0, has_side_effects=True, vmem_limit_bytes=24 << 20),
        name="peak_steps",
    )(got)


def error_kernel(sums_ref, out_ref, inbox, send_sems, recv_sems):
    barrier = rep_barrier_signal()
    pl.semaphore_wait(barrier, 3)
    rep_exchange(sums_ref[...], inbox, send_sems, recv_sems)
    total = (inbox[0] + inbox[1]) + (inbox[2] + inbox[3])
    out_ref[...] = total[:, :HALF] * (1.0 / DENOM)


def error_mean(sums):
    vmem = pl.BlockSpec(memory_space=pltpu.VMEM)
    return pl.pallas_call(
        error_kernel,
        out_shape=jax.ShapeDtypeStruct((1, HALF), jnp.float32),
        in_specs=[vmem], out_specs=vmem,
        scratch_shapes=small_scratch(),
        compiler_params=pltpu.CompilerParams(collective_id=1, has_side_effects=True),
        name="error_mean",
    )(sums)


ENC_ROWS = 32


def encode_kernel(got_ref, steps_ref, codes_ref, sums_ref, inv_ref, acc_ref):
    step = pl.program_id(0)

    @pl.when(step == 0)
    def _():
        inv = 1.0 / steps_ref[...]
        inv_ref[...] = jnp.broadcast_to(jnp.concatenate([inv] * 4, axis=1), inv_ref.shape)
        acc_ref[...] = jnp.zeros_like(acc_ref)

    for q in range(TOK // 4):
        lanes = slice(q * PIECE, (q + 1) * PIECE)
        scaled = got_ref[:, lanes].astype(jnp.float32).reshape(ENC_ROWS // 8, 8, PIECE) * inv_ref[...][None]
        code = jnp.clip(scaled, -127.0, 127.0).astype(jnp.bfloat16)
        gap = scaled - code.astype(jnp.float32)
        codes_ref[:, lanes] = code.reshape(ENC_ROWS, PIECE)
        acc_ref[...] += jnp.sum(gap * gap, axis=0)

    @pl.when(step == pl.num_programs(0) - 1)
    def _():
        row = jnp.sum(acc_ref[...], axis=0, keepdims=True)
        a, b, c, d = fold4(row)
        row = (a + b) + (c + d)
        sums_ref[...] = jnp.concatenate([row, row[:, :384 - HALF]], axis=1)


def encode(got, steps):
    rows = got.shape[0]
    return pl.pallas_call(
        encode_kernel,
        grid=(rows // ENC_ROWS,),
        out_shape=(jax.ShapeDtypeStruct(got.shape, jnp.bfloat16), jax.ShapeDtypeStruct((1, 384), jnp.float32)),
        in_specs=[pl.BlockSpec((ENC_ROWS, TOK * HALF), lambda i: (i, 0)), pl.BlockSpec((1, HALF), lambda i: (0, 0))],
        out_specs=(pl.BlockSpec((ENC_ROWS, TOK * HALF), lambda i: (i, 0)), pl.BlockSpec((1, 384), lambda i: (0, 0))),
        scratch_shapes=[pltpu.VMEM((8, PIECE), jnp.float32), pltpu.VMEM((8, PIECE), jnp.float32)],
        compiler_params=pltpu.CompilerParams(dimension_semantics=("arbitrary",), vmem_limit_bytes=24 << 20),
        name="encode",
    )(got, steps)


def pack_kernel(idx_ref, layer_ref, count_ref, pool_ref, star_ref, rest_ref, top_ref, blocks, picks, tops, sems):
    step = pl.program_id(0)
    size = SEL * STEP_TOK

    @pl.when(step == 0)
    def _():
        for j in range(SEL):
            pltpu.make_async_copy(pool_ref.at[idx_ref[j]], blocks.at[j], sems.at[j]).start()
        row = lax.broadcasted_iota(jnp.int32, (size, size), 0)
        col = lax.broadcasted_iota(jnp.int32, (size, size), 1)
        hit = (row % SEL == col // STEP_TOK) & (row // SEL == col % STEP_TOK)
        picks[...] = jnp.where(hit, 1.0, 0.0).astype(jnp.bfloat16)
        tops[...] = jnp.zeros_like(tops)
        for j in range(SEL):
            pltpu.make_async_copy(pool_ref.at[idx_ref[j]], blocks.at[j], sems.at[j]).wait()

    line = lax.broadcasted_iota(jnp.int32, (REST, 128), 0)
    layers = jnp.full((REST, 128), -1.0, jnp.float32)
    live = count_ref[0]
    for j in range(CAP, SEL):
        name = jnp.where(j < live, layer_ref[j], -1).astype(jnp.float32)
        layers = jnp.where(line == j - CAP, name, layers)
    layers = layers.astype(jnp.bfloat16)

    start = pl.multiple_of(step * STEP_TOK, STEP_TOK)
    data = blocks[:, pl.ds(start, STEP_TOK), :].reshape(size, 2 * HALF)
    for part in range(STEP_TOK // 4):
        moved = jnp.dot(picks[part * 4 * SEL:(part + 1) * 4 * SEL, :], data, preferred_element_type=jnp.float32)
        for half in range(2):
            lanes = [moved[t * SEL:(t + 1) * SEL, half * HALF:(half + 1) * HALF] for t in range(4)]
            flat = jnp.concatenate(lanes, axis=1)
            star_ref[half, part] = flat[:CAP].astype(jnp.bfloat16)
            rest_ref[part, half, :, :PIECE] = flat[CAP:].astype(jnp.bfloat16)
            rest_ref[part, half, :, PIECE:] = layers
            tops[half] = jnp.maximum(tops[half], jnp.abs(flat[:CAP]))

    @pl.when(step == pl.num_programs(0) - 1)
    def _():
        for half in range(2):
            top_ref[half] = pad_row(fold_max(jnp.max(tops[half], axis=0, keepdims=True)))


def fold_max(row):
    a, b, c, d = fold4(row)
    return jnp.maximum(jnp.maximum(a, b), jnp.maximum(c, d))


def pad_row(row):
    return jnp.concatenate([row, jnp.zeros((1, 384 - HALF), jnp.float32)], axis=1)


def pack(block_pool, sel_index, sel_layer, counts):
    smem = pl.BlockSpec(memory_space=pltpu.SMEM)
    parts = STEP_TOK // 4
    return pl.pallas_call(
        pack_kernel,
        grid=(TOK // STEP_TOK,),
        out_shape=(
            jax.ShapeDtypeStruct((2, QS, CAP, PIECE), jnp.bfloat16),
            jax.ShapeDtypeStruct((QS, 2, REST, WIDE), jnp.bfloat16),
            jax.ShapeDtypeStruct((2, 1, 384), jnp.float32),
        ),
        in_specs=[smem, smem, smem, pl.BlockSpec(memory_space=pl.ANY)],
        out_specs=(
            pl.BlockSpec((2, parts, CAP, PIECE), lambda i: (0, i, 0, 0)),
            pl.BlockSpec((parts, 2, REST, WIDE), lambda i: (i, 0, 0, 0)),
            pl.BlockSpec((2, 1, 384), lambda i: (0, 0, 0)),
        ),
        scratch_shapes=[
            pltpu.VMEM((SEL, TOK, 2 * HALF), jnp.bfloat16),
            pltpu.VMEM((SEL * STEP_TOK, SEL * STEP_TOK), jnp.bfloat16),
            pltpu.VMEM((2, CAP, PIECE), jnp.float32),
            pltpu.SemaphoreType.DMA((SEL,)),
        ],
        compiler_params=pltpu.CompilerParams(dimension_semantics=("arbitrary",), vmem_limit_bytes=24 << 20),
        name="pack",
    )(sel_index, sel_layer, counts, block_pool)


def tree(star):
    sx, sz = divmod(star, 4)

    def at(dx, dz):
        return (sx + dx) % 4 * 4 + (sz + dz) % 4

    near = [at(0, 1), at(1, 0), at(0, 3), at(3, 0)]
    diag = [at(1, 1), at(1, 3), at(3, 3), at(3, 1)]
    third = [at(1, 2), at(2, 3), at(3, 2), at(2, 1)]
    straight = [(at(0, 2), 0, 2), (at(2, 0), 1, 3)]
    far = at(2, 2)
    role = {star: 0, far: 4}
    hop = {}
    up = {}
    origin = {}
    shift = {}
    for r in range(4):
        role[near[r]], role[diag[r]], role[third[r]] = 1, 2, 3
        up[near[r]], up[diag[r]], up[third[r]] = star, near[r], diag[r]
        hop[diag[r]] = [(near[r], k) for k in range(4)]
        hop[third[r]] = [(diag[r], k) for k in range(4)]
    hop[far] = [(third[r], 0) for r in range(4)]
    for chip, a, b in straight:
        role[chip] = 5
        hop[chip] = [(near[a], 9), (near[a], 10), (near[b], 9), (near[b], 10)]
        for r, first in ((a, 0), (b, 2)):
            origin[near[r]] = (diag[r], third[r], far, chip)
            shift[near[r]] = (r, first)
    return role, hop, up, origin, shift


def pick(index, table, default=0):
    out = jnp.int32(default)
    for key, value in table.items():
        out = jnp.where(index == key, jnp.int32(value), out)
    return out


MESH = pl.DeviceIdType.MESH


def sort_mail(mail, chip, key_ref, place_ref, select):
    sources = BLOCK // REST
    lane = lax.broadcasted_iota(jnp.int32, (BLOCK, 128), 1).astype(jnp.float32)
    row = lax.broadcasted_iota(jnp.int32, (BLOCK, BLOCK), 0)
    col = lax.broadcasted_iota(jnp.int32, (BLOCK, BLOCK), 1)
    before = jnp.where(col < row, 1.0, 0.0).astype(jnp.bfloat16)
    same = jnp.where((col < row) & (col // REST == row // REST), 1.0, 0.0).astype(jnp.bfloat16)
    local = lax.broadcasted_iota(jnp.int32, (BLOCK, 128), 0) // REST
    mine = chip.astype(jnp.float32)

    def block(i, carry):
        names = mail[pl.ds(i * sources, sources), :, PIECE:].reshape(BLOCK, 128).astype(jnp.float32)
        hits = jnp.where(names == lane, 1.0, 0.0)
        hits16 = hits.astype(jnp.bfloat16)
        rank = jnp.dot(before, hits16, preferred_element_type=jnp.float32) + carry
        slot = jnp.dot(same, hits16, preferred_element_type=jnp.float32)
        rank = jnp.sum(rank * hits, axis=1, keepdims=True)
        slot = jnp.sum(slot * hits, axis=1, keepdims=True)
        source = (local + i * sources).astype(jnp.float32)
        key = jnp.where(rank < ROOM, names * ROOM + rank, -1.0)
        place = jnp.where(names == mine, source * CAP + slot, -1.0)
        key_ref[i] = jnp.transpose(key)[:1]
        place_ref[i] = jnp.transpose(place)[:1]
        return carry + jnp.sum(hits, axis=0, keepdims=True)

    total = lax.fori_loop(0, BLOCKS, block, jnp.zeros((1, 128), jnp.float32))

    @pl.loop(0, CHIPS)
    def _(layer):
        at = pl.multiple_of(layer * ROOM, ROOM)
        want = (lax.broadcasted_iota(jnp.int32, (ROOM, BLOCK), 0) + at).astype(jnp.float32)
        for i in range(BLOCKS):
            hit = jnp.where(want == key_ref[i], 1.0, 0.0).astype(jnp.bfloat16)
            select[pl.ds(at, ROOM), i * BLOCK:(i + 1) * BLOCK] = hit

    return total


def move_kernel(star, star_ref, rest_ref, top_ref, got_ref, few_ref, key_ref, place_ref, info_ref, full_ref,
                mail, select, chosen, inbox, relay, tops, inrep,
                mail_send, mail_recv, few_send, few_recv, own_send, pass_send, relay_recv, star_recv,
                top_send, top_recv, rep_send, rep_recv, local_sem):
    own = lax.axis_index("own")
    rep = lax.axis_index("rep")
    n_own = 2 * CHIPS
    chip = own // 2
    core = own % 2
    role_of, hop_of, up_of, origin_of, shift_of = tree(star)
    role = pick(chip, role_of)
    up = pick(chip, up_of)
    is_star = role == 0
    not_star = role != 0

    barrier = pltpu.get_barrier_semaphore()

    @pl.loop(1, n_own)
    def _(k):
        pl.semaphore_signal(barrier, inc=1, device_id={"own": lax.rem(own + k, n_own)}, device_id_type=MESH)

    for k in range(1, 4):
        pl.semaphore_signal(barrier, inc=1, device_id={"rep": lax.rem(rep + k, 4)}, device_id_type=MESH)
    pl.semaphore_wait(barrier, n_own - 1 + 3)

    def remote(src, dst, send, recv, to):
        return pltpu.make_async_remote_copy(src_ref=src, dst_ref=dst, send_sem=send, recv_sem=recv,
                                            device_id={"own": to}, device_id_type=MESH)

    def mail_copy(to, frm):
        return remote(rest_ref.at[to // 2, to % 2], mail.at[frm], mail_send.at[0], mail_recv.at[0], to)

    @pl.loop(1, n_own)
    def _(k):
        mail_copy(lax.rem(own + k, n_own), own).start()

    def top_copy(half, frm):
        return remote(top_ref.at[half], tops.at[frm], top_send.at[half], top_recv.at[0], 2 * star + half)

    for half in range(2):
        @pl.when(own != 2 * star + half)
        def _():
            top_copy(half, own).start()

        @pl.when(own == 2 * star + half)
        def _():
            tops[own] = top_ref[half]

    def near_copy(half):
        return remote(star_ref.at[half], got_ref.at[own], own_send.at[0], star_recv.at[0], 2 * star + half)

    def hop_copy(k):
        to = pick(chip, {c: h[k][0] for c, h in hop_of.items()}) * 2 + core
        slot = pick(chip, {c: h[k][1] for c, h in hop_of.items()})
        return remote(star_ref.at[:, pl.ds(4 * k, 4)], relay.at[slot], own_send.at[0], relay_recv.at[slot], to)

    @pl.when(role == 1)
    def _():
        for half in range(2):
            near_copy(half).start()

    @pl.when(role > 1)
    def _():
        for k in range(4):
            hop_copy(k).start()

    def keep_copy():
        return pltpu.make_async_copy(star_ref.at[core], got_ref.at[own], local_sem.at[0])

    def partner_copy():
        return remote(star_ref.at[1 - core], got_ref.at[own], own_send.at[0], star_recv.at[0], 2 * star + 1 - core)

    @pl.when(is_star)
    def _():
        keep_copy().start()
        partner_copy().start()

    def relay_in(k):
        return remote(relay.at[k], relay.at[k], pass_send.at[0], relay_recv.at[k], own)

    def pass_near(k, half):
        origins = [pick(chip, {c: o[i] for c, o in origin_of.items()}) for i in range(4)]
        origin = jnp.where(k < 4, origins[0], jnp.where(k < 8, origins[1], jnp.where(k == 8, origins[2], origins[3])))
        turn = pick(chip, {c: s[0] for c, s in shift_of.items()})
        first = pick(chip, {c: s[1] for c, s in shift_of.items()})
        quarter = jnp.where(k < 4, k, jnp.where(k < 8, k - 4, jnp.where(k == 8, turn, first + k - 9)))
        frm = 2 * origin + core
        return remote(relay.at[k, half], got_ref.at[frm, pl.ds(4 * quarter, 4)],
                      pass_send.at[0], star_recv.at[0], 2 * star + half)

    def pass_diag(k):
        return remote(relay.at[k], relay.at[4 + k], pass_send.at[0], relay_recv.at[4 + k], 2 * up + core)

    def pass_third():
        return remote(relay.at[0], relay.at[4], pass_send.at[0], relay_recv.at[4], 2 * up + core)

    def near_order(i):
        return jnp.where(i < 4, i, jnp.where(i < 6, i + 5, i - 2))

    def pass_near_range(low, high):
        @pl.when(role == 1)
        def _():
            @pl.loop(low, high)
            def _(i):
                k = near_order(i)
                relay_in(k).wait_recv()
                for half in range(2):
                    pass_near(k, half).start()

    def pass_diag_range(low, high):
        @pl.when(role == 2)
        def _():
            @pl.loop(low, high)
            def _(k):
                relay_in(k).wait_recv()
                pass_diag(k).start()

    @pl.when(role == 3)
    def _():
        relay_in(0).wait_recv()
        pass_third().start()

    pass_diag_range(0, 4)
    pass_near_range(0, 6)

    mail[own] = rest_ref[chip, core]

    def mail_all():
        return remote(mail.at[pl.ds(0, n_own - 1)], mail.at[pl.ds(0, n_own - 1)], mail_send.at[0], mail_recv.at[0], own)

    mail_all().wait_recv()
    count_by_layer = sort_mail(mail, chip, key_ref, place_ref, select)

    @pl.loop(0, PIECE // 128)
    def _(part):
        lanes = pl.ds(pl.multiple_of(part * 128, 128), 128)
        data = mail[:, :, lanes].reshape(n_own * REST, 128)
        for rows in range(2):
            size = CHIPS * ROOM // 2
            out = jnp.dot(select[rows * size:(rows + 1) * size], data, preferred_element_type=jnp.float32)
            chosen[rows * 8:(rows + 1) * 8, :, lanes] = out.astype(jnp.bfloat16).reshape(8, ROOM, 128)

    def few_copy(to, frm):
        return remote(chosen.at[to], inbox.at[frm], few_send.at[0], few_recv.at[0], 2 * to + core)

    def few_part(low, size):
        part = pl.ds(low, size)
        return remote(inbox.at[part], inbox.at[part], few_send.at[0], few_recv.at[0], own)

    @pl.loop(1, CHIPS)
    def _(k):
        to = lax.rem(chip + k, CHIPS)

        @pl.when(to != star)
        def _():
            few_copy(to, chip).start()

    pass_diag_range(4, 5)
    pass_near_range(6, 11)

    @pl.when(not_star)
    def _():
        inbox[chip] = chosen[chip]

        few_part(0, CHIPS - 1).wait_recv()

        def largest(q, best):
            data = inbox[q]
            few_ref[q] = data
            return jnp.maximum(best, jnp.abs(data))

        best = lax.fori_loop(0, QS, largest, jnp.zeros((ROOM, PIECE), jnp.bfloat16))
        inrep[0] = pad_row(fold_max(jnp.max(best.astype(jnp.float32), axis=0, keepdims=True)))

    @pl.when(is_star)
    def _():
        others = pl.ds(0, n_own - 1)
        remote(tops.at[others], tops.at[others], top_send.at[0], top_recv.at[0], own).wait_recv()

        inrep[0] = jnp.max(tops[...], axis=0)

    full = jnp.max(jnp.where(count_by_layer > ROOM, 1.0, 0.0), axis=1, keepdims=True)
    tail = lax.broadcasted_iota(jnp.int32, (1, 384), 1)
    inrep[0] = jnp.where(tail < HALF, inrep[0], full)

    copies = [pltpu.make_async_remote_copy(
        src_ref=inrep.at[0], dst_ref=inrep.at[k], send_sem=rep_send.at[k], recv_sem=rep_recv.at[k],
        device_id={"rep": lax.rem(rep + k, 4)}, device_id_type=MESH) for k in range(1, 4)]
    for copy in copies:
        copy.start()
    for copy in copies:
        copy.wait()
    top = jnp.maximum(jnp.maximum(inrep[0], inrep[1]), jnp.maximum(inrep[2], inrep[3]))
    info_ref[...] = HEADROOM * jnp.maximum(top, 1.0) / 127.0
    full_ref[0] = jnp.max(jnp.where(tail < HALF, 0.0, top)).astype(jnp.int32)

    def own_all():
        return remote(star_ref, star_ref, own_send.at[0], star_recv.at[0], own)

    def pass_all(size):
        return remote(relay.at[pl.ds(0, size)], relay.at[pl.ds(0, size)], pass_send.at[0], star_recv.at[0], own)

    @pl.when(is_star)
    def _():
        others = pl.ds(0, n_own - 1)
        remote(got_ref.at[others], got_ref.at[others], own_send.at[0], star_recv.at[0], own).wait_recv()

        keep_copy().wait()
        partner_copy().wait_send()

    @pl.when(role == 1)
    def _():
        own_all().wait_send()
        pass_all(11).wait_send()

    @pl.when(role > 1)
    def _():
        own_all().wait_send()

    @pl.when(role == 2)
    def _():
        pass_all(5).wait_send()

    @pl.when(role == 3)
    def _():
        pass_third().wait_send()

    for half in range(2):
        @pl.when(own != 2 * star + half)
        def _():
            top_copy(half, own).wait_send()

    mail_all().wait_send()

    few_part(0, CHIPS - 2).wait_send()

    @pl.when(is_star)
    def _():
        few_part(0, 1).wait_send()


def move(star, star_data, rest_data, top_data):
    vmem = pl.BlockSpec(memory_space=pltpu.VMEM)
    dma = pltpu.SemaphoreType.DMA
    n_own = 2 * CHIPS
    return pl.pallas_call(
        functools.partial(move_kernel, star),
        out_shape=(
            jax.ShapeDtypeStruct((n_own, QS, CAP, PIECE), jnp.bfloat16),
            jax.ShapeDtypeStruct((QS, ROOM, PIECE), jnp.bfloat16),
            jax.ShapeDtypeStruct((BLOCKS, 1, BLOCK), jnp.float32),
            jax.ShapeDtypeStruct((BLOCKS, 1, BLOCK), jnp.float32),
            jax.ShapeDtypeStruct((1, 384), jnp.float32),
            jax.ShapeDtypeStruct((1,), jnp.int32),
        ),
        in_specs=[vmem, vmem, vmem],
        out_specs=(pl.BlockSpec(memory_space=pl.ANY), vmem, vmem, vmem, vmem, pl.BlockSpec(memory_space=pltpu.SMEM)),
        scratch_shapes=[
            pltpu.VMEM((n_own, REST, WIDE), jnp.bfloat16),
            pltpu.VMEM((CHIPS * ROOM, n_own * REST), jnp.bfloat16),
            pltpu.VMEM((CHIPS, ROOM, PIECE), jnp.bfloat16),
            pltpu.VMEM((CHIPS, ROOM, PIECE), jnp.bfloat16),
            pltpu.VMEM((11, 2, 4, CAP, PIECE), jnp.bfloat16),
            pltpu.VMEM((n_own, 1, 384), jnp.float32),
            pltpu.VMEM((4, 1, 384), jnp.float32),
            dma((1,)), dma((1,)), dma((1,)), dma((1,)),
            dma((1,)), dma((1,)), dma((11,)), dma((1,)),
            dma((2,)), dma((1,)), dma((4,)), dma((4,)), dma((1,)),
        ],
        compiler_params=pltpu.CompilerParams(collective_id=2 + star, has_side_effects=True, vmem_limit_bytes=40 << 20),
        name="move",
    )(star_data, rest_data, top_data)


def finish_kernel(flag_ref, got_ref, few_ref, key_ref, place_ref, info_ref, codes_ref, sums_ref, steps_ref,
                  inv_ref, acc_ref, done_ref, map_ref):
    step = pl.program_id(0)
    star = flag_ref[0] != 0

    @pl.when(step == 0)
    def _():
        steps_ref[...] = info_ref[:, :HALF]
        inv = 1.0 / info_ref[:, :HALF]
        inv_ref[...] = jnp.broadcast_to(jnp.concatenate([inv] * 4, axis=1), inv_ref.shape)
        acc_ref[...] = jnp.zeros_like(acc_ref)

    def code_of(data):
        scaled = data.astype(jnp.float32) * inv_ref[...][None]
        code = jnp.clip(scaled, -127.0, 127.0).astype(jnp.bfloat16)
        gap = scaled - code.astype(jnp.float32)
        acc_ref[...] += jnp.sum(gap * gap, axis=0)
        return code

    @pl.when(star)
    def _():
        for q in range(QS):
            lanes = slice(q * PIECE, (q + 1) * PIECE)
            codes_ref[:, lanes] = code_of(got_ref[:, q]).reshape(ENC_ROWS, PIECE)

    @pl.when(jnp.logical_not(star))
    def _():
        @pl.when(step == 0)
        def _():
            for q in range(QS):
                done_ref[q] = code_of(few_ref[q].reshape(ROOM // 8, 8, PIECE)).reshape(ROOM, PIECE)
            rows = map_ref.shape[0]
            first = (lax.broadcasted_iota(jnp.int32, (ROOM, BLOCK), 0) + flag_ref[1] * ROOM).astype(jnp.float32)
            spot = lax.broadcasted_iota(jnp.int32, (rows, BLOCK), 0).astype(jnp.float32)
            total = jnp.zeros((rows, ROOM), jnp.float32)
            for i in range(BLOCKS):
                spread = jnp.where(spot == place_ref[i], 1.0, 0.0).astype(jnp.bfloat16)
                ranked = jnp.where(first == key_ref[i], 1.0, 0.0).astype(jnp.bfloat16)
                total += lax.dot_general(spread, ranked, (((1,), (1,)), ((), ())), preferred_element_type=jnp.float32)
            map_ref[...] = total.astype(jnp.bfloat16)

        spread = map_ref[pl.ds(pl.multiple_of(step * ENC_ROWS, ENC_ROWS), ENC_ROWS), :]
        for q in range(QS):
            lanes = slice(q * PIECE, (q + 1) * PIECE)
            codes_ref[:, lanes] = jnp.dot(spread, done_ref[q], preferred_element_type=jnp.float32).astype(jnp.bfloat16)

    @pl.when(step == pl.num_programs(0) - 1)
    def _():
        row = jnp.sum(acc_ref[...], axis=0, keepdims=True)
        a, b, c, d = fold4(row)
        sums_ref[...] = pad_row((a + b) + (c + d))


def finish(flag, got, few, keys, places, info):
    rows = got.shape[0] * CAP
    grid_spec = pltpu.PrefetchScalarGridSpec(
        num_scalar_prefetch=1,
        grid=(rows // ENC_ROWS,),
        in_specs=[
            pl.BlockSpec((ENC_ROWS // CAP, QS, CAP, PIECE), lambda i, flag: (i * flag[0], 0, 0, 0)),
            pl.BlockSpec((QS, ROOM, PIECE), lambda i, flag: (0, 0, 0)),
            pl.BlockSpec((BLOCKS, 1, BLOCK), lambda i, flag: (0, 0, 0)),
            pl.BlockSpec((BLOCKS, 1, BLOCK), lambda i, flag: (0, 0, 0)),
            pl.BlockSpec((1, 384), lambda i, flag: (0, 0)),
        ],
        out_specs=(
            pl.BlockSpec((ENC_ROWS, TOK * HALF), lambda i, flag: (i, 0)),
            pl.BlockSpec((1, 384), lambda i, flag: (0, 0)),
            pl.BlockSpec((1, HALF), lambda i, flag: (0, 0)),
        ),
        scratch_shapes=[
            pltpu.VMEM((8, PIECE), jnp.float32),
            pltpu.VMEM((8, PIECE), jnp.float32),
            pltpu.VMEM((QS, ROOM, PIECE), jnp.bfloat16),
            pltpu.VMEM((rows, ROOM), jnp.bfloat16),
        ],
    )
    return pl.pallas_call(
        finish_kernel,
        grid_spec=grid_spec,
        out_shape=(
            jax.ShapeDtypeStruct((rows, TOK * HALF), jnp.bfloat16),
            jax.ShapeDtypeStruct((1, 384), jnp.float32),
            jax.ShapeDtypeStruct((1, HALF), jnp.float32),
        ),
        compiler_params=pltpu.CompilerParams(dimension_semantics=("arbitrary",), vmem_limit_bytes=24 << 20),
        name="finish",
    )(flag, got, few, keys, places, info)


def body(block_pool, sel_index, sel_layer, counts):
    star = sel_layer[0]
    star_data, rest_data, top_data = pack(block_pool, sel_index, sel_layer, counts)
    got, few, keys, places, info, full = lax.switch(
        star, [functools.partial(move, layer) for layer in range(LAYERS)], star_data, rest_data, top_data)

    def sparse():
        chip = lax.axis_index("own") // 2
        flag = jnp.stack([(chip == star).astype(jnp.int32), chip.astype(jnp.int32)])
        codes, sums, steps = finish(flag, got, few, keys, places, info)
        return codes, steps, sums

    def dense():
        parted = flatten(block_pool, sel_index, sel_layer, counts).reshape(2 * LAYERS, CAP, TOK * HALF)
        arrived = lax.all_to_all(parted, "own", split_axis=0, concat_axis=0, tiled=True)
        arrived = arrived.reshape(2 * LAYERS * CAP, TOK * HALF)
        steps = peak_steps(arrived)
        codes, sums = encode(arrived, steps)
        return codes, steps, sums

    codes, steps, sums = lax.cond(full[0] > 0, dense, sparse)
    error = error_mean(sums)
    return codes.reshape(1, 1, 2 * LAYERS, CAP, TOK * HALF), steps, error


def solution(mesh):
    return jax.shard_map(
        body,
        mesh=mesh,
        in_specs=(
            P(("own", "rep"), None, None),
            P(("own", "rep")),
            P(("own", "rep")),
            P(("own", "rep")),
        ),
        out_specs=(P("own", "rep", None, None, None), P("own", None), P("own", None)),
        check_vma=False,
    )
```

```python
import functools
import jax
import jax.numpy as jnp
from jax import lax
from jax.experimental import pallas as pl
from jax.experimental.pallas import tpu as pltpu
from jax.sharding import PartitionSpec as P

HEADROOM = 0.5
HALF = 288
PIECE = 4 * HALF
TOK = 64
STEP_TOK = 16
CAP = 8
LAYERS = 16
SEL = 32
CHIPS = 16
QS = 16
REST = SEL - CAP
ROOM = 32
BLOCK = 384
BLOCKS = 2
WIDE = PIECE + 128
DENOM = 32.0 * 4.0 * 8.0 * 64.0


def flatten_kernel(idx_ref, layer_ref, count_ref, pool_ref, out_ref, blocks, picks, seen, sems):
    step = pl.program_id(0)
    rows = STEP_TOK * LAYERS * CAP
    cols = SEL * STEP_TOK

    @pl.when(step == 0)
    def _():
        for j in range(SEL):
            pltpu.make_async_copy(pool_ref.at[idx_ref[j]], blocks.at[j], sems.at[j]).start()
        for layer in range(LAYERS):
            seen[layer] = 0
        col = lax.broadcasted_iota(jnp.int32, (1, cols), 1)
        key = jnp.full((1, cols), -1, jnp.int32)
        live = count_ref[0]
        for j in range(SEL):
            layer = layer_ref[j]
            rank = seen[layer]
            seen[layer] = rank + 1
            slot = jnp.where(j < live, layer * CAP + rank, -1)
            key = jnp.where(col // STEP_TOK == j, slot, key)
        row = lax.broadcasted_iota(jnp.int32, (rows, cols), 0)
        hit = (row % (LAYERS * CAP) == key) & (row // (LAYERS * CAP) == col % STEP_TOK)
        picks[...] = jnp.where(hit, 1.0, 0.0).astype(jnp.bfloat16)
        for j in range(SEL):
            pltpu.make_async_copy(pool_ref.at[idx_ref[j]], blocks.at[j], sems.at[j]).wait()

    start = pl.multiple_of(step * STEP_TOK, STEP_TOK)
    data = blocks[:, pl.ds(start, STEP_TOK), :].reshape(cols, 2 * HALF)
    slots = LAYERS * CAP
    for part in range(STEP_TOK // 4):
        moved = jnp.dot(picks[part * 4 * slots:(part + 1) * 4 * slots, :], data, preferred_element_type=jnp.float32)
        for half in range(2):
            lanes = [moved[t * slots:(t + 1) * slots, half * HALF:(half + 1) * HALF] for t in range(4)]
            flat = jnp.concatenate(lanes, axis=1).astype(jnp.bfloat16)
            out_ref[:, half, :, part * PIECE:(part + 1) * PIECE] = flat.reshape(LAYERS, CAP, PIECE)


def flatten(block_pool, sel_index, sel_layer, counts):
    smem = pl.BlockSpec(memory_space=pltpu.SMEM)
    return pl.pallas_call(
        flatten_kernel,
        grid=(TOK // STEP_TOK,),
        out_shape=jax.ShapeDtypeStruct((LAYERS, 2, CAP, TOK * HALF), jnp.bfloat16),
        in_specs=[smem, smem, smem, pl.BlockSpec(memory_space=pl.ANY)],
        out_specs=pl.BlockSpec((LAYERS, 2, CAP, STEP_TOK * HALF), lambda i: (0, 0, 0, i)),
        scratch_shapes=[
            pltpu.VMEM((SEL, TOK, 2 * HALF), jnp.bfloat16),
            pltpu.VMEM((STEP_TOK * LAYERS * CAP, SEL * STEP_TOK), jnp.bfloat16),
            pltpu.SMEM((LAYERS,), jnp.int32),
            pltpu.SemaphoreType.DMA((SEL,)),
        ],
        compiler_params=pltpu.CompilerParams(dimension_semantics=("arbitrary",), vmem_limit_bytes=48 << 20),
        name="flatten",
    )(sel_index, sel_layer, counts, block_pool)


def rep_exchange(value, inbox, send_sems, recv_sems):
    reps = lax.axis_size("rep")
    me = lax.axis_index("rep")
    inbox[0] = value
    copies = []
    for k in range(1, reps):
        copies.append(pltpu.make_async_remote_copy(
            src_ref=inbox.at[0], dst_ref=inbox.at[k],
            send_sem=send_sems.at[k], recv_sem=recv_sems.at[k],
            device_id={"rep": lax.rem(me + k, reps)}, device_id_type=pl.DeviceIdType.MESH))
    for copy in copies:
        copy.start()
    for copy in copies:
        copy.wait()


def rep_barrier_signal():
    reps = lax.axis_size("rep")
    me = lax.axis_index("rep")
    barrier = pltpu.get_barrier_semaphore()
    for k in range(1, reps):
        pl.semaphore_signal(barrier, inc=1, device_id={"rep": lax.rem(me + k, reps)},
                            device_id_type=pl.DeviceIdType.MESH)
    return barrier


def fold4(row):
    return [row[:, k * HALF:(k + 1) * HALF] for k in range(4)]


def peak_kernel(got_ref, steps_ref, inbox, send_sems, recv_sems):
    barrier = rep_barrier_signal()
    rows = got_ref.shape[0]

    def chunk(i, peak):
        at = pl.multiple_of(i * 16, 16)
        for q in range(TOK // 4):
            part = jnp.abs(got_ref[pl.ds(at, 16), q * PIECE:(q + 1) * PIECE])
            peak = jnp.maximum(peak, part)
        return peak

    peak = lax.fori_loop(0, rows // 16, chunk, jnp.zeros((16, PIECE), jnp.bfloat16))
    row = jnp.max(peak.astype(jnp.float32), axis=0, keepdims=True)
    a, b, c, d = fold4(row)
    row = jnp.maximum(jnp.maximum(a, b), jnp.maximum(c, d))
    pl.semaphore_wait(barrier, 3)
    rep_exchange(jnp.concatenate([row, row[:, :384 - HALF]], axis=1), inbox, send_sems, recv_sems)
    top = jnp.maximum(jnp.maximum(inbox[0], inbox[1]), jnp.maximum(inbox[2], inbox[3]))
    steps_ref[...] = HEADROOM * jnp.maximum(top[:, :HALF], 1.0) / 127.0


def small_scratch():
    return [
        pltpu.VMEM((4, 1, 384), jnp.float32),
        pltpu.SemaphoreType.DMA((4,)),
        pltpu.SemaphoreType.DMA((4,)),
    ]


def peak_steps(got):
    vmem = pl.BlockSpec(memory_space=pltpu.VMEM)
    return pl.pallas_call(
        peak_kernel,
        out_shape=jax.ShapeDtypeStruct((1, HALF), jnp.float32),
        in_specs=[vmem], out_specs=vmem,
        scratch_shapes=small_scratch(),
        compiler_params=pltpu.CompilerParams(collective_id=0, has_side_effects=True, vmem_limit_bytes=24 << 20),
        name="peak_steps",
    )(got)


def error_kernel(sums_ref, out_ref, inbox, send_sems, recv_sems):
    barrier = rep_barrier_signal()
    pl.semaphore_wait(barrier, 3)
    rep_exchange(sums_ref[...], inbox, send_sems, recv_sems)
    total = (inbox[0] + inbox[1]) + (inbox[2] + inbox[3])
    out_ref[...] = total[:, :HALF] * (1.0 / DENOM)


def error_mean(sums):
    vmem = pl.BlockSpec(memory_space=pltpu.VMEM)
    return pl.pallas_call(
        error_kernel,
        out_shape=jax.ShapeDtypeStruct((1, HALF), jnp.float32),
        in_specs=[vmem], out_specs=vmem,
        scratch_shapes=small_scratch(),
        compiler_params=pltpu.CompilerParams(collective_id=1, has_side_effects=True),
        name="error_mean",
    )(sums)


ENC_ROWS = 32


def encode_kernel(got_ref, steps_ref, codes_ref, sums_ref, inv_ref, acc_ref):
    step = pl.program_id(0)

    @pl.when(step == 0)
    def _():
        inv = 1.0 / steps_ref[...]
        inv_ref[...] = jnp.broadcast_to(jnp.concatenate([inv] * 4, axis=1), inv_ref.shape)
        acc_ref[...] = jnp.zeros_like(acc_ref)

    for q in range(TOK // 4):
        lanes = slice(q * PIECE, (q + 1) * PIECE)
        scaled = got_ref[:, lanes].astype(jnp.float32).reshape(ENC_ROWS // 8, 8, PIECE) * inv_ref[...][None]
        code = jnp.clip(scaled, -127.0, 127.0).astype(jnp.bfloat16)
        gap = scaled - code.astype(jnp.float32)
        codes_ref[:, lanes] = code.reshape(ENC_ROWS, PIECE)
        acc_ref[...] += jnp.sum(gap * gap, axis=0)

    @pl.when(step == pl.num_programs(0) - 1)
    def _():
        row = jnp.sum(acc_ref[...], axis=0, keepdims=True)
        a, b, c, d = fold4(row)
        row = (a + b) + (c + d)
        sums_ref[...] = jnp.concatenate([row, row[:, :384 - HALF]], axis=1)


def encode(got, steps):
    rows = got.shape[0]
    return pl.pallas_call(
        encode_kernel,
        grid=(rows // ENC_ROWS,),
        out_shape=(jax.ShapeDtypeStruct(got.shape, jnp.bfloat16), jax.ShapeDtypeStruct((1, 384), jnp.float32)),
        in_specs=[pl.BlockSpec((ENC_ROWS, TOK * HALF), lambda i: (i, 0)), pl.BlockSpec((1, HALF), lambda i: (0, 0))],
        out_specs=(pl.BlockSpec((ENC_ROWS, TOK * HALF), lambda i: (i, 0)), pl.BlockSpec((1, 384), lambda i: (0, 0))),
        scratch_shapes=[pltpu.VMEM((8, PIECE), jnp.float32), pltpu.VMEM((8, PIECE), jnp.float32)],
        compiler_params=pltpu.CompilerParams(dimension_semantics=("arbitrary",), vmem_limit_bytes=24 << 20),
        name="encode",
    )(got, steps)


def pack_kernel(idx_ref, layer_ref, count_ref, pool_ref, star_ref, rest_ref, top_ref, blocks, picks, tops, sems):
    step = pl.program_id(0)
    size = SEL * STEP_TOK

    @pl.when(step == 0)
    def _():
        for j in range(SEL):
            pltpu.make_async_copy(pool_ref.at[idx_ref[j]], blocks.at[j], sems.at[j]).start()
        row = lax.broadcasted_iota(jnp.int32, (size, size), 0)
        col = lax.broadcasted_iota(jnp.int32, (size, size), 1)
        hit = (row % SEL == col // STEP_TOK) & (row // SEL == col % STEP_TOK)
        picks[...] = jnp.where(hit, 1.0, 0.0).astype(jnp.bfloat16)
        tops[...] = jnp.zeros_like(tops)
        for j in range(SEL):
            pltpu.make_async_copy(pool_ref.at[idx_ref[j]], blocks.at[j], sems.at[j]).wait()

    line = lax.broadcasted_iota(jnp.int32, (REST, 128), 0)
    layers = jnp.full((REST, 128), -1.0, jnp.float32)
    live = count_ref[0]
    for j in range(CAP, SEL):
        name = jnp.where(j < live, layer_ref[j], -1).astype(jnp.float32)
        layers = jnp.where(line == j - CAP, name, layers)
    layers = layers.astype(jnp.bfloat16)

    start = pl.multiple_of(step * STEP_TOK, STEP_TOK)
    data = blocks[:, pl.ds(start, STEP_TOK), :].reshape(size, 2 * HALF)
    for part in range(STEP_TOK // 4):
        moved = jnp.dot(picks[part * 4 * SEL:(part + 1) * 4 * SEL, :], data, preferred_element_type=jnp.float32)
        for half in range(2):
            lanes = [moved[t * SEL:(t + 1) * SEL, half * HALF:(half + 1) * HALF] for t in range(4)]
            flat = jnp.concatenate(lanes, axis=1)
            star_ref[half, part] = flat[:CAP].astype(jnp.bfloat16)
            rest_ref[part, half, :, :PIECE] = flat[CAP:].astype(jnp.bfloat16)
            rest_ref[part, half, :, PIECE:] = layers
            tops[half] = jnp.maximum(tops[half], jnp.abs(flat[:CAP]))

    @pl.when(step == pl.num_programs(0) - 1)
    def _():
        for half in range(2):
            top_ref[half] = pad_row(fold_max(jnp.max(tops[half], axis=0, keepdims=True)))


def fold_max(row):
    a, b, c, d = fold4(row)
    return jnp.maximum(jnp.maximum(a, b), jnp.maximum(c, d))


def pad_row(row):
    return jnp.concatenate([row, jnp.zeros((1, 384 - HALF), jnp.float32)], axis=1)


def pack(block_pool, sel_index, sel_layer, counts):
    smem = pl.BlockSpec(memory_space=pltpu.SMEM)
    parts = STEP_TOK // 4
    return pl.pallas_call(
        pack_kernel,
        grid=(TOK // STEP_TOK,),
        out_shape=(
            jax.ShapeDtypeStruct((2, QS, CAP, PIECE), jnp.bfloat16),
            jax.ShapeDtypeStruct((QS, 2, REST, WIDE), jnp.bfloat16),
            jax.ShapeDtypeStruct((2, 1, 384), jnp.float32),
        ),
        in_specs=[smem, smem, smem, pl.BlockSpec(memory_space=pl.ANY)],
        out_specs=(
            pl.BlockSpec((2, parts, CAP, PIECE), lambda i: (0, i, 0, 0)),
            pl.BlockSpec((parts, 2, REST, WIDE), lambda i: (i, 0, 0, 0)),
            pl.BlockSpec((2, 1, 384), lambda i: (0, 0, 0)),
        ),
        scratch_shapes=[
            pltpu.VMEM((SEL, TOK, 2 * HALF), jnp.bfloat16),
            pltpu.VMEM((SEL * STEP_TOK, SEL * STEP_TOK), jnp.bfloat16),
            pltpu.VMEM((2, CAP, PIECE), jnp.float32),
            pltpu.SemaphoreType.DMA((SEL,)),
        ],
        compiler_params=pltpu.CompilerParams(dimension_semantics=("arbitrary",), vmem_limit_bytes=24 << 20),
        name="pack",
    )(sel_index, sel_layer, counts, block_pool)


def tree(star):
    sx, sz = divmod(star, 4)

    def at(dx, dz):
        return (sx + dx) % 4 * 4 + (sz + dz) % 4

    near = [at(0, 1), at(1, 0), at(0, 3), at(3, 0)]
    diag = [at(1, 1), at(1, 3), at(3, 3), at(3, 1)]
    third = [at(1, 2), at(2, 3), at(3, 2), at(2, 1)]
    far = at(2, 2)
    over_z, over_x = at(0, 2), at(2, 0)
    role = {star: 0, far: 4, over_z: 4, over_x: 4, third[0]: 4, third[2]: 4}
    count, hop, up, origin, shift = {}, {}, {}, {}, {}
    for r in range(4):
        role[near[r]], role[diag[r]] = 1, 2
        up[near[r]], up[diag[r]] = star, near[r]
        count[near[r]], count[diag[r]] = (14, 8) if r % 2 == 0 else (8, 2)
        hop[diag[r]] = [(near[r], k) for k in range(4)]
    for r in (1, 3):
        role[third[r]] = 3
        up[third[r]] = diag[r]
        count[third[r]] = 2
    for own, to, low in ((0, 0, 0), (3, 0, 4), (2, 2, 0), (1, 2, 4)):
        hop[third[own]] = [(diag[to], low + k) for k in range(4)]
    hop[far] = [(third[1], 0), (third[1], 1), (third[3], 0), (third[3], 1)]
    for chip, a, b in ((over_z, 0, 2), (over_x, 1, 3)):
        hop[chip] = [(near[a], 12), (near[a], 13), (near[b], 12), (near[b], 13)]
    origin[near[0]] = (diag[0], third[0], third[3], over_z)
    origin[near[2]] = (diag[2], third[2], third[1], over_z)
    origin[near[1]] = (diag[1], far, far, over_x)
    origin[near[3]] = (diag[3], far, far, over_x)
    shift[near[0]], shift[near[1]], shift[near[2]], shift[near[3]] = (0, 0), (0, 0), (0, 2), (2, 2)
    away = {at(dx, dz): (dx - 1) * 3 + dz - 1 for dx in range(1, 4) for dz in range(1, 4)}
    return role, count, hop, up, origin, shift, away


ORDER = {4: 1, 5: 0, 6: 3, 7: 2, 12: 3, 13: 0, 14: 1, 15: 2, 8: 2, 9: 0, 10: 1, 11: 3, 0: 1, 1: 3, 2: 2, 3: 0}


def turn(chip, step):
    lead = lax.rem(step, 4)
    dx = jnp.where(lead == 0, 1, jnp.where(lead == 1, 3, jnp.where(lead == 2, 2, 0)))
    dz = pick(dx * 4 + step // 4, ORDER)
    return lax.rem(chip // 4 + dx, 4) * 4 + lax.rem(lax.rem(chip, 4) + dz, 4)


def pick(index, table, default=0):
    out = jnp.int32(default)
    for key, value in table.items():
        out = jnp.where(index == key, jnp.int32(value), out)
    return out


MESH = pl.DeviceIdType.MESH


def sort_mail(mail, chip, key_ref, place_ref, select):
    sources = BLOCK // REST
    lane = lax.broadcasted_iota(jnp.int32, (BLOCK, 128), 1).astype(jnp.float32)
    row = lax.broadcasted_iota(jnp.int32, (BLOCK, BLOCK), 0)
    col = lax.broadcasted_iota(jnp.int32, (BLOCK, BLOCK), 1)
    before = jnp.where(col < row, 1.0, 0.0).astype(jnp.bfloat16)
    same = jnp.where((col < row) & (col // REST == row // REST), 1.0, 0.0).astype(jnp.bfloat16)
    local = lax.broadcasted_iota(jnp.int32, (BLOCK, 128), 0) // REST
    mine = chip.astype(jnp.float32)

    def block(i, carry):
        names = mail[pl.ds(i * sources, sources), :, PIECE:WIDE].reshape(BLOCK, 128).astype(jnp.float32)
        hits = jnp.where(names == lane, 1.0, 0.0)
        hits16 = hits.astype(jnp.bfloat16)
        rank = jnp.dot(before, hits16, preferred_element_type=jnp.float32) + carry
        slot = jnp.dot(same, hits16, preferred_element_type=jnp.float32)
        rank = jnp.sum(rank * hits, axis=1, keepdims=True)
        slot = jnp.sum(slot * hits, axis=1, keepdims=True)
        source = (local + i * sources).astype(jnp.float32)
        key = jnp.where(rank < ROOM, names * ROOM + rank, -1.0)
        place = jnp.where(names == mine, source * CAP + slot, -1.0)
        key_ref[i] = jnp.transpose(key)[:1]
        place_ref[i] = jnp.transpose(place)[:1]
        return carry + jnp.sum(hits, axis=0, keepdims=True)

    total = lax.fori_loop(0, BLOCKS, block, jnp.zeros((1, 128), jnp.float32))

    @pl.loop(0, CHIPS)
    def _(layer):
        at = pl.multiple_of(layer * ROOM, ROOM)
        want = (lax.broadcasted_iota(jnp.int32, (ROOM, BLOCK), 0) + at).astype(jnp.float32)
        for i in range(BLOCKS):
            hit = jnp.where(want == key_ref[i], 1.0, 0.0).astype(jnp.bfloat16)
            select[pl.ds(at, ROOM), i * BLOCK:(i + 1) * BLOCK] = hit

    return total


def move_kernel(star, star_ref, rest_ref, top_ref, got_ref, few_ref, key_ref, place_ref, info_ref, full_ref,
                mail, select, chosen, inbox, relay, tops, inrep,
                mail_send, mail_recv, few_send, few_recv, own_send, pass_send, relay_recv, star_recv,
                top_send, top_recv, rep_send, rep_recv, local_sem):
    own = lax.axis_index("own")
    rep = lax.axis_index("rep")
    n_own = 2 * CHIPS
    chip = own // 2
    core = own % 2
    role_of, count_of, hop_of, up_of, origin_of, shift_of, away_of = tree(star)
    role = pick(chip, role_of)
    up = pick(chip, up_of)
    count = pick(chip, count_of)
    tile = pick(chip, away_of, -1)
    is_star = role == 0
    not_star = role != 0

    barrier = pltpu.get_barrier_semaphore()

    @pl.loop(1, n_own)
    def _(k):
        pl.semaphore_signal(barrier, inc=1, device_id={"own": lax.rem(own + k, n_own)}, device_id_type=MESH)

    for k in range(1, 4):
        pl.semaphore_signal(barrier, inc=1, device_id={"rep": lax.rem(rep + k, 4)}, device_id_type=MESH)
    pl.semaphore_wait(barrier, n_own - 1 + 3)

    def remote(src, dst, send, recv, to):
        return pltpu.make_async_remote_copy(src_ref=src, dst_ref=dst, send_sem=send, recv_sem=recv,
                                            device_id={"own": to}, device_id_type=MESH)

    def mail_copy(to, frm):
        return remote(rest_ref.at[to // 2, to % 2], mail.at[frm, :, pl.ds(0, WIDE)], mail_send.at[0], mail_recv.at[0], to)

    def name_copy(half):
        return remote(rest_ref.at[star, half, :, pl.ds(PIECE, 128)], mail.at[own, :, pl.ds(PIECE, 128)],
                      mail_send.at[1], mail_recv.at[0], 2 * star + half)

    def lane_of(which):
        return pl.ds(pl.multiple_of(which * 128, 128), 128)

    def extra_copy(to_chip, half):
        return remote(rest_ref.at[star, half, :, lane_of(pick(to_chip, away_of))], mail.at[own, :, pl.ds(WIDE, 128)],
                      mail_send.at[2], mail_recv.at[1], 2 * to_chip + half)

    def top_copy(half, frm):
        return remote(top_ref.at[half], tops.at[frm], top_send.at[half], top_recv.at[0], 2 * star + half)

    for half in range(2):
        @pl.when(own != 2 * star + half)
        def _():
            top_copy(half, own).start()

        @pl.when(own == 2 * star + half)
        def _():
            tops[own] = top_ref[half]

    def near_copy(half):
        return remote(star_ref.at[half], got_ref.at[own], own_send.at[0], star_recv.at[0], 2 * star + half)

    def hop_copy(k):
        to = pick(chip, {c: h[k][0] for c, h in hop_of.items()}) * 2 + core
        slot = pick(chip, {c: h[k][1] for c, h in hop_of.items()})
        return remote(star_ref.at[:, pl.ds(4 * k, 4)], relay.at[slot], own_send.at[0], relay_recv.at[slot], to)

    @pl.when(role == 1)
    def _():
        for half in range(2):
            near_copy(half).start()

    @pl.when(role > 1)
    def _():
        for k in range(4):
            hop_copy(k).start()

    def keep_copy():
        return pltpu.make_async_copy(star_ref.at[core], got_ref.at[own], local_sem.at[0])

    def partner_copy():
        return remote(star_ref.at[1 - core], got_ref.at[own], own_send.at[0], star_recv.at[0], 2 * star + 1 - core)

    @pl.when(is_star)
    def _():
        keep_copy().start()
        partner_copy().start()

    for half in range(2):
        @pl.when(own != 2 * star + half)
        def _():
            name_copy(half).start()

    @pl.loop(0, n_own)
    def _(k):
        half = lax.rem(k, 2)
        to_chip = turn(chip, k // 2)

        @pl.when((to_chip != star) & (2 * to_chip + half != own))
        def _():
            mail_copy(2 * to_chip + half, own).start()

        @pl.when((pick(to_chip, away_of, -1) >= 0) & (2 * to_chip + half != own))
        def _():
            extra_copy(to_chip, half).start()

    def relay_in(k):
        return remote(relay.at[k], relay.at[k], pass_send.at[0], relay_recv.at[k], own)

    def pass_near(k, half):
        group = k // 4
        origins = [pick(chip, {c: o[i] for c, o in origin_of.items()}) for i in range(4)]
        origin = jnp.where(group == 0, origins[0], jnp.where(group == 1, origins[1],
                           jnp.where(group == 2, origins[2], origins[3])))
        shifts = [pick(chip, {c: o[i] for c, o in shift_of.items()}) for i in range(2)]
        quarter = lax.rem(k, 4) + jnp.where(group == 1, shifts[0], jnp.where(group == 3, shifts[1], 0))
        frm = 2 * origin + core
        return remote(relay.at[k, half], got_ref.at[frm, pl.ds(4 * quarter, 4)],
                      pass_send.at[0], star_recv.at[0], 2 * star + half)

    def pass_diag(k):
        return remote(relay.at[k], relay.at[4 + k], pass_send.at[0], relay_recv.at[4 + k], 2 * up + core)

    def pass_third(k):
        return remote(relay.at[k], relay.at[k], pass_send.at[0], relay_recv.at[k], 2 * up + core)

    def near_order(i):
        return jnp.where(i < 4, i, jnp.where(i < 6, i + 8, i - 2))

    def pass_near_range(low, high):
        @pl.when(role == 1)
        def _():
            @pl.loop(low, high)
            def _(i):
                k = near_order(i)
                relay_in(k).wait_recv()
                for half in range(2):
                    pass_near(k, half).start()

    def pass_diag_range(low, high):
        @pl.when(role == 2)
        def _():
            @pl.loop(low, high)
            def _(k):
                relay_in(k).wait_recv()
                pass_diag(k).start()

    early_diag = jnp.where(count == 8, 8, 0)
    early_near = jnp.where(count == 14, 6, 6)
    pass_diag_range(0, early_diag)
    pass_near_range(0, early_near)

    def mail_part(size, which):
        ref = mail.at[pl.ds(0, size), :, pl.ds(0, WIDE)]
        return remote(ref, ref, mail_send.at[which], mail_recv.at[0], own)

    def name_part(size):
        ref = mail.at[pl.ds(0, size), :, pl.ds(PIECE, 128)]
        return remote(ref, ref, mail_send.at[1], mail_recv.at[0], own)

    def extra_part(size):
        ref = mail.at[pl.ds(0, size), :, pl.ds(WIDE, 128)]
        return remote(ref, ref, mail_send.at[2], mail_recv.at[1], own)

    @pl.when(not_star)
    def _():
        mail[own, :, :WIDE] = rest_ref[chip, core]
        mail_part(n_own - 1, 0).wait_recv()

    @pl.when(is_star)
    def _():
        mail[own, :, PIECE:WIDE] = rest_ref[chip, core, :, PIECE:]
        name_part(n_own - 1).wait_recv()

    @pl.when(tile >= 0)
    def _():
        mail[own, :, WIDE:] = rest_ref[star, core, :, lane_of(tile)]
        extra_part(n_own - 1).wait_recv()

    count_by_layer = sort_mail(mail, chip, key_ref, place_ref, select)

    parts = PIECE // 128

    @pl.loop(0, jnp.where(is_star, 0, jnp.where(tile >= 0, parts + 1, parts)))
    def _(part):
        data = mail[:, :, lane_of(jnp.where(part == parts, parts + 1, part))].reshape(n_own * REST, 128)
        for rows in range(2):
            size = CHIPS * ROOM // 2
            out = jnp.dot(select[rows * size:(rows + 1) * size], data, preferred_element_type=jnp.float32)
            chosen[rows * 8:(rows + 1) * 8, :, lane_of(part)] = out.astype(jnp.bfloat16).reshape(8, ROOM, 128)

    def few_copy(to):
        return remote(chosen.at[to, :, pl.ds(0, PIECE)], inbox.at[chip], few_send.at[0], few_recv.at[0], 2 * to + core)

    def tile_copy(to):
        return remote(chosen.at[to, :, pl.ds(PIECE, 128)], inbox.at[star, :, lane_of(tile)], few_send.at[1], few_recv.at[1], 2 * to + core)

    def few_part(size):
        part = pl.ds(0, size)
        return remote(inbox.at[part], inbox.at[part], few_send.at[0], few_recv.at[0], own)

    def tile_part(size, lanes):
        ref = inbox.at[pl.ds(0, size), :, pl.ds(0, lanes)]
        return remote(ref, ref, few_send.at[1], few_recv.at[1], own)

    @pl.loop(0, CHIPS)
    def _(k):
        to = turn(chip, k)

        @pl.when((to != star) & (to != chip) & not_star)
        def _():
            few_copy(to).start()

            @pl.when(tile >= 0)
            def _():
                tile_copy(to).start()

    @pl.when(role == 3)
    def _():
        @pl.loop(0, 2)
        def _(k):
            relay_in(k).wait_recv()
            pass_third(k).start()

    pass_diag_range(early_diag, count)
    pass_near_range(early_near, count)

    @pl.when(not_star)
    def _():
        inbox[chip] = chosen[chip, :, :PIECE]

        @pl.when(tile >= 0)
        def _():
            inbox[star, :, lane_of(tile)] = chosen[chip, :, PIECE:]
            tile_part(1, 1024).wait_recv()

        @pl.when(tile < 0)
        def _():
            tile_part(1, PIECE).wait_recv()


        few_part(CHIPS - 2).wait_recv()

        def largest(q, best):
            data = inbox[q]
            few_ref[q] = data
            return jnp.maximum(best, jnp.abs(data))

        best = lax.fori_loop(0, QS, largest, jnp.zeros((ROOM, PIECE), jnp.bfloat16))
        inrep[0] = pad_row(fold_max(jnp.max(best.astype(jnp.float32), axis=0, keepdims=True)))

    @pl.when(is_star)
    def _():
        others = pl.ds(0, n_own - 1)
        remote(tops.at[others], tops.at[others], top_send.at[0], top_recv.at[0], own).wait_recv()

        inrep[0] = jnp.max(tops[...], axis=0)

    full = jnp.max(jnp.where(count_by_layer > ROOM, 1.0, 0.0), axis=1, keepdims=True)
    tail = lax.broadcasted_iota(jnp.int32, (1, 384), 1)
    inrep[0] = jnp.where(tail < HALF, inrep[0], full)

    copies = [pltpu.make_async_remote_copy(
        src_ref=inrep.at[0], dst_ref=inrep.at[k], send_sem=rep_send.at[k], recv_sem=rep_recv.at[k],
        device_id={"rep": lax.rem(rep + k, 4)}, device_id_type=MESH) for k in range(1, 4)]
    for copy in copies:
        copy.start()
    for copy in copies:
        copy.wait()
    top = jnp.maximum(jnp.maximum(inrep[0], inrep[1]), jnp.maximum(inrep[2], inrep[3]))
    info_ref[...] = HEADROOM * jnp.maximum(top, 1.0) / 127.0
    full_ref[0] = jnp.max(jnp.where(tail < HALF, 0.0, top)).astype(jnp.int32)

    def own_all():
        return remote(star_ref, star_ref, own_send.at[0], star_recv.at[0], own)

    def pass_all(size):
        return remote(relay.at[pl.ds(0, size)], relay.at[pl.ds(0, size)], pass_send.at[0], star_recv.at[0], own)

    @pl.when(is_star)
    def _():
        others = pl.ds(0, n_own - 1)
        remote(got_ref.at[others], got_ref.at[others], own_send.at[0], star_recv.at[0], own).wait_recv()

        keep_copy().wait()
        partner_copy().wait_send()

    @pl.when(role == 1)
    def _():
        own_all().wait_send()

    @pl.when(role > 1)
    def _():
        own_all().wait_send()

    for size in (2, 8, 14):
        @pl.when(count == size)
        def _():
            pass_all(size).wait_send()

    for half in range(2):
        @pl.when(own != 2 * star + half)
        def _():
            top_copy(half, own).wait_send()

    @pl.when(is_star)
    def _():
        mail_part(n_own - 2, 0).wait_send()
        name_part(1).wait_send()

    @pl.when(not_star)
    def _():
        mail_part(n_own - 3, 0).wait_send()
        name_part(2).wait_send()

    @pl.when(tile >= 0)
    def _():
        extra_part(17).wait_send()

    @pl.when(tile < 0)
    def _():
        extra_part(18).wait_send()

    @pl.when(not_star)
    def _():
        few_part(CHIPS - 2).wait_send()

    @pl.when(tile >= 0)
    def _():
        tile_part(CHIPS - 2, 128).wait_send()


def move(star, star_data, rest_data, top_data):
    vmem = pl.BlockSpec(memory_space=pltpu.VMEM)
    dma = pltpu.SemaphoreType.DMA
    n_own = 2 * CHIPS
    return pl.pallas_call(
        functools.partial(move_kernel, star),
        out_shape=(
            jax.ShapeDtypeStruct((n_own, QS, CAP, PIECE), jnp.bfloat16),
            jax.ShapeDtypeStruct((QS, ROOM, PIECE), jnp.bfloat16),
            jax.ShapeDtypeStruct((BLOCKS, 1, BLOCK), jnp.float32),
            jax.ShapeDtypeStruct((BLOCKS, 1, BLOCK), jnp.float32),
            jax.ShapeDtypeStruct((1, 384), jnp.float32),
            jax.ShapeDtypeStruct((1,), jnp.int32),
        ),
        in_specs=[vmem, vmem, vmem],
        out_specs=(pl.BlockSpec(memory_space=pl.ANY), vmem, vmem, vmem, vmem, pl.BlockSpec(memory_space=pltpu.SMEM)),
        scratch_shapes=[
            pltpu.VMEM((n_own, REST, WIDE + 128), jnp.bfloat16),
            pltpu.VMEM((CHIPS * ROOM, n_own * REST), jnp.bfloat16),
            pltpu.VMEM((CHIPS, ROOM, WIDE), jnp.bfloat16),
            pltpu.VMEM((CHIPS, ROOM, PIECE), jnp.bfloat16),
            pltpu.VMEM((14, 2, 4, CAP, PIECE), jnp.bfloat16),
            pltpu.VMEM((n_own, 1, 384), jnp.float32),
            pltpu.VMEM((4, 1, 384), jnp.float32),
            dma((3,)), dma((2,)), dma((2,)), dma((2,)),
            dma((1,)), dma((1,)), dma((14,)), dma((1,)),
            dma((2,)), dma((1,)), dma((4,)), dma((4,)), dma((1,)),
        ],
        compiler_params=pltpu.CompilerParams(collective_id=2 + star, has_side_effects=True, vmem_limit_bytes=40 << 20),
        name="move",
    )(star_data, rest_data, top_data)


def finish_kernel(flag_ref, got_ref, few_ref, key_ref, place_ref, info_ref, codes_ref, sums_ref, steps_ref,
                  inv_ref, acc_ref, done_ref, map_ref):
    step = pl.program_id(0)
    star = flag_ref[0] != 0

    @pl.when(step == 0)
    def _():
        steps_ref[...] = info_ref[:, :HALF]
        inv = 1.0 / info_ref[:, :HALF]
        inv_ref[...] = jnp.broadcast_to(jnp.concatenate([inv] * 4, axis=1), inv_ref.shape)
        acc_ref[...] = jnp.zeros_like(acc_ref)

    def code_of(data):
        scaled = data.astype(jnp.float32) * inv_ref[...][None]
        code = jnp.clip(scaled, -127.0, 127.0).astype(jnp.bfloat16)
        gap = scaled - code.astype(jnp.float32)
        acc_ref[...] += jnp.sum(gap * gap, axis=0)
        return code

    @pl.when(star)
    def _():
        for q in range(QS):
            lanes = slice(q * PIECE, (q + 1) * PIECE)
            codes_ref[:, lanes] = code_of(got_ref[:, q]).reshape(ENC_ROWS, PIECE)

    @pl.when(jnp.logical_not(star))
    def _():
        @pl.when(step == 0)
        def _():
            for q in range(QS):
                done_ref[q] = code_of(few_ref[q].reshape(ROOM // 8, 8, PIECE)).reshape(ROOM, PIECE)
            rows = map_ref.shape[0]
            first = (lax.broadcasted_iota(jnp.int32, (ROOM, BLOCK), 0) + flag_ref[1] * ROOM).astype(jnp.float32)
            spot = lax.broadcasted_iota(jnp.int32, (rows, BLOCK), 0).astype(jnp.float32)
            total = jnp.zeros((rows, ROOM), jnp.float32)
            for i in range(BLOCKS):
                spread = jnp.where(spot == place_ref[i], 1.0, 0.0).astype(jnp.bfloat16)
                ranked = jnp.where(first == key_ref[i], 1.0, 0.0).astype(jnp.bfloat16)
                total += lax.dot_general(spread, ranked, (((1,), (1,)), ((), ())), preferred_element_type=jnp.float32)
            map_ref[...] = total.astype(jnp.bfloat16)

        spread = map_ref[pl.ds(pl.multiple_of(step * ENC_ROWS, ENC_ROWS), ENC_ROWS), :]
        for q in range(QS):
            lanes = slice(q * PIECE, (q + 1) * PIECE)
            codes_ref[:, lanes] = jnp.dot(spread, done_ref[q], preferred_element_type=jnp.float32).astype(jnp.bfloat16)

    @pl.when(step == pl.num_programs(0) - 1)
    def _():
        row = jnp.sum(acc_ref[...], axis=0, keepdims=True)
        a, b, c, d = fold4(row)
        sums_ref[...] = pad_row((a + b) + (c + d))


def finish(flag, got, few, keys, places, info):
    rows = got.shape[0] * CAP
    grid_spec = pltpu.PrefetchScalarGridSpec(
        num_scalar_prefetch=1,
        grid=(rows // ENC_ROWS,),
        in_specs=[
            pl.BlockSpec((ENC_ROWS // CAP, QS, CAP, PIECE), lambda i, flag: (i * flag[0], 0, 0, 0)),
            pl.BlockSpec((QS, ROOM, PIECE), lambda i, flag: (0, 0, 0)),
            pl.BlockSpec((BLOCKS, 1, BLOCK), lambda i, flag: (0, 0, 0)),
            pl.BlockSpec((BLOCKS, 1, BLOCK), lambda i, flag: (0, 0, 0)),
            pl.BlockSpec((1, 384), lambda i, flag: (0, 0)),
        ],
        out_specs=(
            pl.BlockSpec((ENC_ROWS, TOK * HALF), lambda i, flag: (i, 0)),
            pl.BlockSpec((1, 384), lambda i, flag: (0, 0)),
            pl.BlockSpec((1, HALF), lambda i, flag: (0, 0)),
        ),
        scratch_shapes=[
            pltpu.VMEM((8, PIECE), jnp.float32),
            pltpu.VMEM((8, PIECE), jnp.float32),
            pltpu.VMEM((QS, ROOM, PIECE), jnp.bfloat16),
            pltpu.VMEM((rows, ROOM), jnp.bfloat16),
        ],
    )
    return pl.pallas_call(
        finish_kernel,
        grid_spec=grid_spec,
        out_shape=(
            jax.ShapeDtypeStruct((rows, TOK * HALF), jnp.bfloat16),
            jax.ShapeDtypeStruct((1, 384), jnp.float32),
            jax.ShapeDtypeStruct((1, HALF), jnp.float32),
        ),
        compiler_params=pltpu.CompilerParams(dimension_semantics=("arbitrary",), vmem_limit_bytes=24 << 20),
        name="finish",
    )(flag, got, few, keys, places, info)


def body(block_pool, sel_index, sel_layer, counts):
    star = sel_layer[0]
    star_data, rest_data, top_data = pack(block_pool, sel_index, sel_layer, counts)
    got, few, keys, places, info, full = lax.switch(
        star, [functools.partial(move, layer) for layer in range(LAYERS)], star_data, rest_data, top_data)

    def sparse():
        chip = lax.axis_index("own") // 2
        flag = jnp.stack([(chip == star).astype(jnp.int32), chip.astype(jnp.int32)])
        codes, sums, steps = finish(flag, got, few, keys, places, info)
        return codes, steps, sums

    def dense():
        parted = flatten(block_pool, sel_index, sel_layer, counts).reshape(2 * LAYERS, CAP, TOK * HALF)
        arrived = lax.all_to_all(parted, "own", split_axis=0, concat_axis=0, tiled=True)
        arrived = arrived.reshape(2 * LAYERS * CAP, TOK * HALF)
        steps = peak_steps(arrived)
        codes, sums = encode(arrived, steps)
        return codes, steps, sums

    codes, steps, sums = lax.cond(full[0] > 0, dense, sparse)
    error = error_mean(sums)
    return codes.reshape(1, 1, 2 * LAYERS, CAP, TOK * HALF), steps, error


def solution(mesh):
    return jax.shard_map(
        body,
        mesh=mesh,
        in_specs=(
            P(("own", "rep"), None, None),
            P(("own", "rep")),
            P(("own", "rep")),
            P(("own", "rep")),
        ),
        out_specs=(P("own", "rep", None, None, None), P("own", None), P("own", None)),
        check_vma=False,
    )
```

```python
import functools
import jax
import jax.numpy as jnp
from jax import lax
from jax.experimental import pallas as pl
from jax.experimental.pallas import tpu as pltpu
from jax.sharding import PartitionSpec as P

HEADROOM = 0.5
HALF = 288
PIECE = 4 * HALF
TOK = 64
STEP_TOK = 16
CAP = 8
LAYERS = 16
SEL = 32
CHIPS = 16
QS = 16
REST = SEL - CAP
ROOM = 32
BLOCK = 384
BLOCKS = 2
WIDE = PIECE + 128
DENOM = 32.0 * 4.0 * 8.0 * 64.0


def flatten_kernel(idx_ref, layer_ref, count_ref, pool_ref, out_ref, blocks, picks, seen, sems):
    step = pl.program_id(0)
    rows = STEP_TOK * LAYERS * CAP
    cols = SEL * STEP_TOK

    @pl.when(step == 0)
    def _():
        for j in range(SEL):
            pltpu.make_async_copy(pool_ref.at[idx_ref[j]], blocks.at[j], sems.at[j]).start()
        for layer in range(LAYERS):
            seen[layer] = 0
        col = lax.broadcasted_iota(jnp.int32, (1, cols), 1)
        key = jnp.full((1, cols), -1, jnp.int32)
        live = count_ref[0]
        for j in range(SEL):
            layer = layer_ref[j]
            rank = seen[layer]
            seen[layer] = rank + 1
            slot = jnp.where(j < live, layer * CAP + rank, -1)
            key = jnp.where(col // STEP_TOK == j, slot, key)
        row = lax.broadcasted_iota(jnp.int32, (rows, cols), 0)
        hit = (row % (LAYERS * CAP) == key) & (row // (LAYERS * CAP) == col % STEP_TOK)
        picks[...] = jnp.where(hit, 1.0, 0.0).astype(jnp.bfloat16)
        for j in range(SEL):
            pltpu.make_async_copy(pool_ref.at[idx_ref[j]], blocks.at[j], sems.at[j]).wait()

    start = pl.multiple_of(step * STEP_TOK, STEP_TOK)
    data = blocks[:, pl.ds(start, STEP_TOK), :].reshape(cols, 2 * HALF)
    slots = LAYERS * CAP

    @pl.loop(0, STEP_TOK // 4)
    def _(part):
        rows = pl.ds(pl.multiple_of(part * 4 * slots, 4 * slots), 4 * slots)
        moved = jnp.dot(picks[rows, :], data, preferred_element_type=jnp.float32)
        at = pl.ds(pl.multiple_of(part * PIECE, 128), PIECE)
        for half in range(2):
            lanes = [moved[t * slots:(t + 1) * slots, half * HALF:(half + 1) * HALF] for t in range(4)]
            flat = jnp.concatenate(lanes, axis=1).astype(jnp.bfloat16)
            out_ref[:, half, :, at] = flat.reshape(LAYERS, CAP, PIECE)


def flatten(block_pool, sel_index, sel_layer, counts):
    smem = pl.BlockSpec(memory_space=pltpu.SMEM)
    return pl.pallas_call(
        flatten_kernel,
        grid=(TOK // STEP_TOK,),
        out_shape=jax.ShapeDtypeStruct((LAYERS, 2, CAP, TOK * HALF), jnp.bfloat16),
        in_specs=[smem, smem, smem, pl.BlockSpec(memory_space=pl.ANY)],
        out_specs=pl.BlockSpec((LAYERS, 2, CAP, STEP_TOK * HALF), lambda i: (0, 0, 0, i)),
        scratch_shapes=[
            pltpu.VMEM((SEL, TOK, 2 * HALF), jnp.bfloat16),
            pltpu.VMEM((STEP_TOK * LAYERS * CAP, SEL * STEP_TOK), jnp.bfloat16),
            pltpu.SMEM((LAYERS,), jnp.int32),
            pltpu.SemaphoreType.DMA((SEL,)),
        ],
        compiler_params=pltpu.CompilerParams(dimension_semantics=("arbitrary",), vmem_limit_bytes=48 << 20),
        name="flatten",
    )(sel_index, sel_layer, counts, block_pool)


def rep_exchange(value, inbox, send_sems, recv_sems):
    reps = lax.axis_size("rep")
    me = lax.axis_index("rep")
    inbox[0] = value
    copies = []
    for k in range(1, reps):
        copies.append(pltpu.make_async_remote_copy(
            src_ref=inbox.at[0], dst_ref=inbox.at[k],
            send_sem=send_sems.at[k], recv_sem=recv_sems.at[k],
            device_id={"rep": lax.rem(me + k, reps)}, device_id_type=pl.DeviceIdType.MESH))
    for copy in copies:
        copy.start()
    for copy in copies:
        copy.wait()


def rep_barrier_signal():
    reps = lax.axis_size("rep")
    me = lax.axis_index("rep")
    barrier = pltpu.get_barrier_semaphore()
    for k in range(1, reps):
        pl.semaphore_signal(barrier, inc=1, device_id={"rep": lax.rem(me + k, reps)},
                            device_id_type=pl.DeviceIdType.MESH)
    return barrier


def fold4(row):
    return [row[:, k * HALF:(k + 1) * HALF] for k in range(4)]


def peak_kernel(got_ref, steps_ref, inbox, send_sems, recv_sems):
    barrier = rep_barrier_signal()
    rows = got_ref.shape[0]

    def chunk(i, peak):
        at = pl.multiple_of(i * 16, 16)
        for q in range(TOK // 4):
            part = jnp.abs(got_ref[pl.ds(at, 16), q * PIECE:(q + 1) * PIECE])
            peak = jnp.maximum(peak, part)
        return peak

    peak = lax.fori_loop(0, rows // 16, chunk, jnp.zeros((16, PIECE), jnp.bfloat16))
    row = jnp.max(peak.astype(jnp.float32), axis=0, keepdims=True)
    a, b, c, d = fold4(row)
    row = jnp.maximum(jnp.maximum(a, b), jnp.maximum(c, d))
    pl.semaphore_wait(barrier, 3)
    rep_exchange(jnp.concatenate([row, row[:, :384 - HALF]], axis=1), inbox, send_sems, recv_sems)
    top = jnp.maximum(jnp.maximum(inbox[0], inbox[1]), jnp.maximum(inbox[2], inbox[3]))
    steps_ref[...] = HEADROOM * jnp.maximum(top[:, :HALF], 1.0) / 127.0


def small_scratch():
    return [
        pltpu.VMEM((4, 1, 384), jnp.float32),
        pltpu.SemaphoreType.DMA((4,)),
        pltpu.SemaphoreType.DMA((4,)),
    ]


def peak_steps(got):
    vmem = pl.BlockSpec(memory_space=pltpu.VMEM)
    return pl.pallas_call(
        peak_kernel,
        out_shape=jax.ShapeDtypeStruct((1, HALF), jnp.float32),
        in_specs=[vmem], out_specs=vmem,
        scratch_shapes=small_scratch(),
        compiler_params=pltpu.CompilerParams(collective_id=0, has_side_effects=True, vmem_limit_bytes=24 << 20),
        name="peak_steps",
    )(got)


def error_kernel(sums_ref, out_ref, inbox, send_sems, recv_sems):
    barrier = rep_barrier_signal()
    pl.semaphore_wait(barrier, 3)
    rep_exchange(sums_ref[...], inbox, send_sems, recv_sems)
    total = (inbox[0] + inbox[1]) + (inbox[2] + inbox[3])
    out_ref[...] = total[:, :HALF] * (1.0 / DENOM)


def error_mean(sums):
    vmem = pl.BlockSpec(memory_space=pltpu.VMEM)
    return pl.pallas_call(
        error_kernel,
        out_shape=jax.ShapeDtypeStruct((1, HALF), jnp.float32),
        in_specs=[vmem], out_specs=vmem,
        scratch_shapes=small_scratch(),
        compiler_params=pltpu.CompilerParams(collective_id=1, has_side_effects=True),
        name="error_mean",
    )(sums)


ENC_ROWS = 32


def encode_kernel(got_ref, steps_ref, codes_ref, sums_ref, inv_ref, acc_ref):
    step = pl.program_id(0)

    @pl.when(step == 0)
    def _():
        inv = 1.0 / steps_ref[...]
        inv_ref[...] = jnp.broadcast_to(jnp.concatenate([inv] * 4, axis=1), inv_ref.shape)
        acc_ref[...] = jnp.zeros_like(acc_ref)

    @pl.loop(0, QS)
    def _(q):
        lanes = pl.ds(pl.multiple_of(q * PIECE, 128), PIECE)
        data = got_ref[:, lanes].reshape(ENC_ROWS // 8, 8, PIECE)
        codes_ref[:, lanes] = code_of(data, inv_ref, acc_ref).reshape(ENC_ROWS, PIECE)

    @pl.when(step == pl.num_programs(0) - 1)
    def _():
        row = jnp.sum(acc_ref[...], axis=0, keepdims=True)
        a, b, c, d = fold4(row)
        row = (a + b) + (c + d)
        sums_ref[...] = jnp.concatenate([row, row[:, :384 - HALF]], axis=1)


def encode(got, steps):
    rows = got.shape[0]
    return pl.pallas_call(
        encode_kernel,
        grid=(rows // ENC_ROWS,),
        out_shape=(jax.ShapeDtypeStruct(got.shape, jnp.bfloat16), jax.ShapeDtypeStruct((1, 384), jnp.float32)),
        in_specs=[pl.BlockSpec((ENC_ROWS, TOK * HALF), lambda i: (i, 0)), pl.BlockSpec((1, HALF), lambda i: (0, 0))],
        out_specs=(pl.BlockSpec((ENC_ROWS, TOK * HALF), lambda i: (i, 0)), pl.BlockSpec((1, 384), lambda i: (0, 0))),
        scratch_shapes=[pltpu.VMEM((8, PIECE), jnp.float32), pltpu.VMEM((8, PIECE), jnp.float32)],
        compiler_params=pltpu.CompilerParams(dimension_semantics=("arbitrary",), vmem_limit_bytes=24 << 20),
        name="encode",
    )(got, steps)


def pack_kernel(idx_ref, layer_ref, count_ref, pool_ref, star_ref, rest_ref, top_ref, blocks, picks, tops, sems):
    step = pl.program_id(0)
    size = SEL * STEP_TOK

    @pl.when(step == 0)
    def _():
        for j in range(SEL):
            pltpu.make_async_copy(pool_ref.at[idx_ref[j]], blocks.at[j], sems.at[j]).start()
        row = lax.broadcasted_iota(jnp.int32, (size, size), 0)
        col = lax.broadcasted_iota(jnp.int32, (size, size), 1)
        hit = (row % SEL == col // STEP_TOK) & (row // SEL == col % STEP_TOK)
        picks[...] = jnp.where(hit, 1.0, 0.0).astype(jnp.bfloat16)
        tops[...] = jnp.zeros_like(tops)
        for j in range(SEL):
            pltpu.make_async_copy(pool_ref.at[idx_ref[j]], blocks.at[j], sems.at[j]).wait()

    line = lax.broadcasted_iota(jnp.int32, (REST, 128), 0)
    layers = jnp.full((REST, 128), -1.0, jnp.float32)
    live = count_ref[0]
    for j in range(CAP, SEL):
        name = jnp.where(j < live, layer_ref[j], -1).astype(jnp.float32)
        layers = jnp.where(line == j - CAP, name, layers)
    layers = layers.astype(jnp.bfloat16)

    start = pl.multiple_of(step * STEP_TOK, STEP_TOK)
    data = blocks[:, pl.ds(start, STEP_TOK), :].reshape(size, 2 * HALF)
    for part in range(STEP_TOK // 4):
        moved = jnp.dot(picks[part * 4 * SEL:(part + 1) * 4 * SEL, :], data, preferred_element_type=jnp.float32)
        for half in range(2):
            lanes = [moved[t * SEL:(t + 1) * SEL, half * HALF:(half + 1) * HALF] for t in range(4)]
            flat = jnp.concatenate(lanes, axis=1)
            star_ref[half, part] = flat[:CAP].astype(jnp.bfloat16)
            rest_ref[part, half, :, :PIECE] = flat[CAP:].astype(jnp.bfloat16)
            rest_ref[part, half, :, PIECE:] = layers
            tops[half] = jnp.maximum(tops[half], jnp.abs(flat[:CAP]))

    @pl.when(step == pl.num_programs(0) - 1)
    def _():
        for half in range(2):
            top_ref[half] = pad_row(fold_max(jnp.max(tops[half], axis=0, keepdims=True)))


def fold_max(row):
    a, b, c, d = fold4(row)
    return jnp.maximum(jnp.maximum(a, b), jnp.maximum(c, d))


def pad_row(row):
    return jnp.concatenate([row, jnp.zeros((1, 384 - HALF), jnp.float32)], axis=1)


def pack(block_pool, sel_index, sel_layer, counts):
    smem = pl.BlockSpec(memory_space=pltpu.SMEM)
    parts = STEP_TOK // 4
    return pl.pallas_call(
        pack_kernel,
        grid=(TOK // STEP_TOK,),
        out_shape=(
            jax.ShapeDtypeStruct((2, QS, CAP, PIECE), jnp.bfloat16),
            jax.ShapeDtypeStruct((QS, 2, REST, WIDE), jnp.bfloat16),
            jax.ShapeDtypeStruct((2, 1, 384), jnp.float32),
        ),
        in_specs=[smem, smem, smem, pl.BlockSpec(memory_space=pl.ANY)],
        out_specs=(
            pl.BlockSpec((2, parts, CAP, PIECE), lambda i: (0, i, 0, 0)),
            pl.BlockSpec((parts, 2, REST, WIDE), lambda i: (i, 0, 0, 0)),
            pl.BlockSpec((2, 1, 384), lambda i: (0, 0, 0)),
        ),
        scratch_shapes=[
            pltpu.VMEM((SEL, TOK, 2 * HALF), jnp.bfloat16),
            pltpu.VMEM((SEL * STEP_TOK, SEL * STEP_TOK), jnp.bfloat16),
            pltpu.VMEM((2, CAP, PIECE), jnp.float32),
            pltpu.SemaphoreType.DMA((SEL,)),
        ],
        compiler_params=pltpu.CompilerParams(dimension_semantics=("arbitrary",), vmem_limit_bytes=24 << 20),
        name="pack",
    )(sel_index, sel_layer, counts, block_pool)


def tree(star):
    sx, sz = divmod(star, 4)

    def at(dx, dz):
        return (sx + dx) % 4 * 4 + (sz + dz) % 4

    near = [at(0, 1), at(1, 0), at(0, 3), at(3, 0)]
    diag = [at(1, 1), at(1, 3), at(3, 3), at(3, 1)]
    third = [at(1, 2), at(2, 3), at(3, 2), at(2, 1)]
    far = at(2, 2)
    over_z, over_x = at(0, 2), at(2, 0)
    role = {star: 0, far: 4, over_z: 2, over_x: 4, third[0]: 4, third[2]: 4}
    count, hop, up, origin, shift = {over_z: 8}, {}, {over_z: near[0]}, {}, {}
    light = 2 if sz % 2 == 0 else 0
    for r in range(4):
        role[near[r]], role[diag[r]] = 1, 2
        up[near[r]], up[diag[r]] = star, near[r]
        count[near[r]], count[diag[r]] = (12, 4) if r % 2 == 0 else (8, 2)
        hop[diag[r]] = [(near[r], k) for k in range(4)]
    count[near[light]] = 16
    for r in (1, 3):
        role[third[r]] = 3
        up[third[r]] = diag[r]
        count[third[r]] = 2
    hop[third[0]] = [(over_z, k) for k in range(4)]
    hop[third[2]] = [(over_z, 4 + k) for k in range(4)]
    hop[third[3]] = [(diag[0], k) for k in range(4)]
    hop[third[1]] = [(diag[2], k) for k in range(4)]
    hop[far] = [(third[1], 0), (third[1], 1), (third[3], 0), (third[3], 1)]
    hop[over_z] = [(near[light], 12 + k) for k in range(4)]
    hop[over_x] = [(near[1], 12), (near[1], 13), (near[3], 12), (near[3], 13)]
    origin[near[0]] = (diag[0], third[0], third[3], over_z)
    origin[near[2]] = (diag[2], third[2], third[1], over_z)
    origin[near[1]] = (diag[1], far, far, over_x)
    origin[near[3]] = (diag[3], far, far, over_x)
    shift[near[0]], shift[near[1]], shift[near[2]], shift[near[3]] = (0, 0), (0, 0), (0, 0), (2, 2)
    away = {at(dx, dz): (dx - 1) * 3 + dz - 1 for dx in range(1, 4) for dz in range(1, 4)}
    arrival = [star, *near, *diag, over_x, over_z, third[0], third[2], far, third[1], third[3]]
    return role, count, hop, up, origin, shift, away, dict(enumerate(arrival))


ORDER = {4: 1, 5: 0, 6: 3, 7: 2, 12: 3, 13: 0, 14: 1, 15: 2, 8: 2, 9: 0, 10: 1, 11: 3, 0: 1, 1: 3, 2: 2, 3: 0}


def turn(chip, step):
    lead = lax.rem(step, 4)
    dx = jnp.where(lead == 0, 1, jnp.where(lead == 1, 3, jnp.where(lead == 2, 2, 0)))
    dz = pick(dx * 4 + step // 4, ORDER)
    return lax.rem(chip // 4 + dx, 4) * 4 + lax.rem(lax.rem(chip, 4) + dz, 4)


def pick(index, table, default=0):
    out = jnp.int32(default)
    for key, value in table.items():
        out = jnp.where(index == key, jnp.int32(value), out)
    return out


MESH = pl.DeviceIdType.MESH


def sort_mail(mail, chip, key_ref, place_ref, select):
    sources = BLOCK // REST
    lane = lax.broadcasted_iota(jnp.int32, (BLOCK, 128), 1).astype(jnp.float32)
    row = lax.broadcasted_iota(jnp.int32, (BLOCK, BLOCK), 0)
    col = lax.broadcasted_iota(jnp.int32, (BLOCK, BLOCK), 1)
    before = jnp.where(col < row, 1.0, 0.0).astype(jnp.bfloat16)
    same = jnp.where((col < row) & (col // REST == row // REST), 1.0, 0.0).astype(jnp.bfloat16)
    local = lax.broadcasted_iota(jnp.int32, (BLOCK, 128), 0) // REST
    mine = chip.astype(jnp.float32)

    def block(i, carry):
        names = mail[pl.ds(i * sources, sources), :, PIECE:WIDE].reshape(BLOCK, 128).astype(jnp.float32)
        hits = jnp.where(names == lane, 1.0, 0.0)
        hits16 = hits.astype(jnp.bfloat16)
        rank = jnp.dot(before, hits16, preferred_element_type=jnp.float32) + carry
        slot = jnp.dot(same, hits16, preferred_element_type=jnp.float32)
        rank = jnp.sum(rank * hits, axis=1, keepdims=True)
        slot = jnp.sum(slot * hits, axis=1, keepdims=True)
        source = (local + i * sources).astype(jnp.float32)
        key = jnp.where(rank < ROOM, names * ROOM + rank, -1.0)
        place = jnp.where(names == mine, source * CAP + slot, -1.0)
        key_ref[i] = jnp.transpose(key)[:1]
        place_ref[i] = jnp.transpose(place)[:1]
        return carry + jnp.sum(hits, axis=0, keepdims=True)

    total = lax.fori_loop(0, BLOCKS, block, jnp.zeros((1, 128), jnp.float32))

    @pl.loop(0, CHIPS)
    def _(layer):
        at = pl.multiple_of(layer * ROOM, ROOM)
        want = (lax.broadcasted_iota(jnp.int32, (ROOM, BLOCK), 0) + at).astype(jnp.float32)
        for i in range(BLOCKS):
            hit = jnp.where(want == key_ref[i], 1.0, 0.0).astype(jnp.bfloat16)
            select[pl.ds(at, ROOM), i * BLOCK:(i + 1) * BLOCK] = hit

    return total


def code_of(data, inv, acc):
    scaled = data.astype(jnp.float32) * inv[...][None]
    code = jnp.clip(scaled, -127.0, 127.0).astype(jnp.bfloat16)
    gap = scaled - code.astype(jnp.float32)
    acc[...] += jnp.sum(gap * gap, axis=0)
    return code


def move_kernel(star, star_ref, rest_ref, top_ref, got_ref, few_ref, key_ref, place_ref, steps_ref, error_ref, full_ref,
                mail, select, chosen, inbox, relay, tops, inrep, inrep2, land, stage, inv, acc,
                mail_send, mail_recv, few_send, few_recv, own_send, pass_send, relay_recv, star_recv,
                top_send, top_recv, rep_send, rep_recv, sum_send, sum_recv, out_sem):
    own = lax.axis_index("own")
    rep = lax.axis_index("rep")
    n_own = 2 * CHIPS
    chip = own // 2
    core = own % 2
    role_of, count_of, hop_of, up_of, origin_of, shift_of, away_of, arrival_of = tree(star)
    role = pick(chip, role_of)
    up = pick(chip, up_of)
    count = pick(chip, count_of)
    tile = pick(chip, away_of, -1)
    over_z = star // 4 * 4 + (star + 2) % 4
    other_near = star // 4 * 4 + (star + 3) % 4
    is_star = role == 0
    not_star = role != 0

    barrier = pltpu.get_barrier_semaphore()

    @pl.loop(1, n_own)
    def _(k):
        pl.semaphore_signal(barrier, inc=1, device_id={"own": lax.rem(own + k, n_own)}, device_id_type=MESH)

    for k in range(1, 4):
        pl.semaphore_signal(barrier, inc=1, device_id={"rep": lax.rem(rep + k, 4)}, device_id_type=MESH)
    pl.semaphore_wait(barrier, n_own - 1 + 3)

    def remote(src, dst, send, recv, to):
        return pltpu.make_async_remote_copy(src_ref=src, dst_ref=dst, send_sem=send, recv_sem=recv,
                                            device_id={"own": to}, device_id_type=MESH)

    def mail_copy(to, frm):
        return remote(rest_ref.at[to // 2, to % 2], mail.at[frm, :, pl.ds(0, WIDE)], mail_send.at[0], mail_recv.at[0], to)

    def name_copy(half):
        return remote(rest_ref.at[star, half, :, pl.ds(PIECE, 128)], mail.at[own, :, pl.ds(PIECE, 128)],
                      mail_send.at[1], mail_recv.at[0], 2 * star + half)

    def lane_of(which):
        return pl.ds(pl.multiple_of(which * 128, 128), 128)

    def extra_copy(to_chip, half):
        return remote(rest_ref.at[star, half, :, lane_of(pick(to_chip, away_of))], mail.at[own, :, pl.ds(WIDE, 128)],
                      mail_send.at[2], mail_recv.at[1], 2 * to_chip + half)

    def top_copy(half, frm):
        return remote(top_ref.at[half], tops.at[frm], top_send.at[half], top_recv.at[0], 2 * star + half)

    for half in range(2):
        @pl.when(own != 2 * star + half)
        def _():
            top_copy(half, own).start()

        @pl.when(own == 2 * star + half)
        def _():
            tops[own] = top_ref[half]

    def near_copy(half):
        return remote(star_ref.at[half], land.at[own], own_send.at[0], star_recv.at[own], 2 * star + half)

    def hop_copy(k):
        to = pick(chip, {c: h[k][0] for c, h in hop_of.items()}) * 2 + core
        slot = pick(chip, {c: h[k][1] for c, h in hop_of.items()})
        return remote(star_ref.at[:, pl.ds(4 * k, 4)], relay.at[slot], own_send.at[0], relay_recv.at[slot], to)

    @pl.when(role == 1)
    def _():
        for half in range(2):
            near_copy(half).start()

    @pl.when(role > 1)
    def _():
        for k in range(4):
            hop_copy(k).start()

    def partner_copy():
        return remote(star_ref.at[1 - core], land.at[own], own_send.at[0], star_recv.at[own], 2 * star + 1 - core)

    @pl.when(is_star)
    def _():
        partner_copy().start()

        @pl.loop(0, QS)
        def _(q):
            land[own, q] = star_ref[core, q]

    for half in range(2):
        @pl.when(own != 2 * star + half)
        def _():
            name_copy(half).start()

    @pl.loop(0, n_own)
    def _(k):
        half = lax.rem(k, 2)
        to_chip = turn(chip, k // 2)

        @pl.when((to_chip != star) & (2 * to_chip + half != own))
        def _():
            mail_copy(2 * to_chip + half, own).start()

        @pl.when((pick(to_chip, away_of, -1) >= 0) & (2 * to_chip + half != own))
        def _():
            extra_copy(to_chip, half).start()

    def relay_in(k):
        return remote(relay.at[k], relay.at[k], pass_send.at[0], relay_recv.at[k], own)

    def pass_near(k, half):
        group = k // 4
        origins = [pick(chip, {c: o[i] for c, o in origin_of.items()}) for i in range(4)]
        origin = jnp.where(group == 0, origins[0], jnp.where(group == 1, origins[1],
                           jnp.where(group == 2, origins[2], origins[3])))
        shifts = [pick(chip, {c: o[i] for c, o in shift_of.items()}) for i in range(2)]
        quarter = lax.rem(k, 4) + jnp.where(group == 1, shifts[0], jnp.where(group == 3, shifts[1], 0))
        frm = 2 * origin + core
        return remote(relay.at[k, half], land.at[frm, pl.ds(4 * quarter, 4)],
                      pass_send.at[0], star_recv.at[frm], 2 * star + half)

    def pass_diag(k):
        slot = jnp.where(chip == over_z, 4 + lax.rem(k, 4), jnp.where(count == 4, 8 + k, 4 + k))
        to = jnp.where((chip == over_z) & (k >= 4), other_near, up)
        return remote(relay.at[k], relay.at[slot], pass_send.at[0], relay_recv.at[slot], 2 * to + core)

    def pass_third(k):
        return remote(relay.at[k], relay.at[k], pass_send.at[0], relay_recv.at[k], 2 * up + core)

    def near_order(i):
        straight = jnp.where(count == 16, 4, jnp.where(count == 8, 2, 0))
        return jnp.where(i < 4, i, jnp.where(i < 4 + straight, i + 8, i - straight))

    def pass_near_range(low, high):
        @pl.when(role == 1)
        def _():
            @pl.loop(low, high)
            def _(i):
                k = near_order(i)
                relay_in(k).wait_recv()
                for half in range(2):
                    pass_near(k, half).start()

    def pass_diag_range(low, high):
        @pl.when(role == 2)
        def _():
            @pl.loop(low, high)
            def _(k):
                relay_in(k).wait_recv()
                pass_diag(k).start()

    early_diag = jnp.where(count == 2, 0, count)
    early_near = jnp.where(count == 16, 8, jnp.where(count == 12, 8, 6))
    pass_diag_range(0, early_diag)
    pass_near_range(0, early_near)

    def mail_part(size, which):
        ref = mail.at[pl.ds(0, size), :, pl.ds(0, WIDE)]
        return remote(ref, ref, mail_send.at[which], mail_recv.at[0], own)

    def name_part(size):
        ref = mail.at[pl.ds(0, size), :, pl.ds(PIECE, 128)]
        return remote(ref, ref, mail_send.at[1], mail_recv.at[0], own)

    def extra_part(size):
        ref = mail.at[pl.ds(0, size), :, pl.ds(WIDE, 128)]
        return remote(ref, ref, mail_send.at[2], mail_recv.at[1], own)

    @pl.when(not_star)
    def _():
        mail[own, :, :WIDE] = rest_ref[chip, core]
        mail_part(n_own - 1, 0).wait_recv()

    @pl.when(is_star)
    def _():
        mail[own, :, PIECE:WIDE] = rest_ref[chip, core, :, PIECE:]
        name_part(n_own - 1).wait_recv()

    @pl.when(tile >= 0)
    def _():
        mail[own, :, WIDE:] = rest_ref[star, core, :, lane_of(tile)]
        extra_part(n_own - 1).wait_recv()

    count_by_layer = sort_mail(mail, chip, key_ref, place_ref, select)

    parts = PIECE // 128

    @pl.loop(0, jnp.where(is_star, 0, jnp.where(tile >= 0, parts + 1, parts)))
    def _(part):
        data = mail[:, :, lane_of(jnp.where(part == parts, parts + 1, part))].reshape(n_own * REST, 128)
        for rows in range(2):
            size = CHIPS * ROOM // 2
            out = jnp.dot(select[rows * size:(rows + 1) * size], data, preferred_element_type=jnp.float32)
            chosen[rows * 8:(rows + 1) * 8, :, lane_of(part)] = out.astype(jnp.bfloat16).reshape(8, ROOM, 128)

    def few_copy(to):
        return remote(chosen.at[to, :, pl.ds(0, PIECE)], inbox.at[chip], few_send.at[0], few_recv.at[0], 2 * to + core)

    def tile_copy(to):
        return remote(chosen.at[to, :, pl.ds(PIECE, 128)], inbox.at[star, :, lane_of(tile)], few_send.at[1], few_recv.at[1], 2 * to + core)

    def few_part(size):
        part = pl.ds(0, size)
        return remote(inbox.at[part], inbox.at[part], few_send.at[0], few_recv.at[0], own)

    def tile_part(size, lanes):
        ref = inbox.at[pl.ds(0, size), :, pl.ds(0, lanes)]
        return remote(ref, ref, few_send.at[1], few_recv.at[1], own)

    @pl.loop(0, CHIPS)
    def _(k):
        to = turn(chip, k)

        @pl.when((to != star) & (to != chip) & not_star)
        def _():
            few_copy(to).start()

            @pl.when(tile >= 0)
            def _():
                tile_copy(to).start()

    @pl.when(role == 3)
    def _():
        @pl.loop(0, 2)
        def _(k):
            relay_in(k).wait_recv()
            pass_third(k).start()

    pass_diag_range(early_diag, count)
    pass_near_range(early_near, count)

    @pl.when(not_star)
    def _():
        inbox[chip] = chosen[chip, :, :PIECE]

        @pl.when(tile >= 0)
        def _():
            inbox[star, :, lane_of(tile)] = chosen[chip, :, PIECE:]
            tile_part(1, 1024).wait_recv()

        @pl.when(tile < 0)
        def _():
            tile_part(1, PIECE).wait_recv()


        few_part(CHIPS - 2).wait_recv()

        def largest(q, best):
            return jnp.maximum(best, jnp.abs(inbox[q]))

        best = lax.fori_loop(0, QS, largest, jnp.zeros((ROOM, PIECE), jnp.bfloat16))
        inrep[0] = pad_row(fold_max(jnp.max(best.astype(jnp.float32), axis=0, keepdims=True)))

    @pl.when(is_star)
    def _():
        others = pl.ds(0, n_own - 1)
        remote(tops.at[others], tops.at[others], top_send.at[0], top_recv.at[0], own).wait_recv()

        inrep[0] = jnp.max(tops[...], axis=0)

    full = jnp.max(jnp.where(count_by_layer > ROOM, 1.0, 0.0), axis=1, keepdims=True)
    tail = lax.broadcasted_iota(jnp.int32, (1, 384), 1)
    inrep[0] = jnp.where(tail < HALF, inrep[0], full)

    rep_exchange(inrep[0], inrep, rep_send, rep_recv)
    top = jnp.maximum(jnp.maximum(inrep[0], inrep[1]), jnp.maximum(inrep[2], inrep[3]))
    steps = HEADROOM * jnp.maximum(top[:, :HALF], 1.0) / 127.0
    steps_ref[...] = steps
    full_ref[0] = jnp.max(jnp.where(tail < HALF, 0.0, top)).astype(jnp.int32)
    inv[...] = jnp.broadcast_to(jnp.concatenate([1.0 / steps] * 4, axis=1), inv.shape)
    acc[...] = jnp.zeros_like(acc)

    @pl.when(not_star)
    def _():
        @pl.loop(0, QS)
        def _(q):
            few_ref[q] = code_of(inbox[q].reshape(ROOM // 8, 8, PIECE), inv, acc).reshape(ROOM, PIECE)

    @pl.when(is_star)
    def _():
        @pl.loop(0, n_own)
        def _(k):
            slot = lax.rem(k, 2)
            frm = 2 * pick(k // 2, arrival_of) + slot
            out = pltpu.make_async_copy(stage.at[slot], got_ref.at[pl.ds(pl.multiple_of(8 * frm, 8), 8)], out_sem.at[slot])

            @pl.when(frm != own)
            def _():
                remote(land.at[frm], land.at[frm], own_send.at[0], star_recv.at[frm], own).wait_recv()

            @pl.when(k > 1)
            def _():
                out.wait()

            @pl.loop(0, QS // 2)
            def _(pair):
                for half in range(2):
                    q = 2 * pair + half
                    code = code_of(land[frm, pl.ds(q, 1)], inv, acc)
                    stage[slot, :, pl.ds(pl.multiple_of(q * PIECE, 128), PIECE)] = code[0]

            out.start()

    row = jnp.sum(acc[...], axis=0, keepdims=True)
    a, b, c, d = fold4(row)
    rep_exchange(pad_row((a + b) + (c + d)), inrep2, sum_send, sum_recv)
    total = (inrep2[0] + inrep2[1]) + (inrep2[2] + inrep2[3])
    error_ref[...] = total[:, :HALF] * (1.0 / DENOM)

    def own_all():
        return remote(star_ref, star_ref, own_send.at[0], star_recv.at[0], own)

    def pass_all(size):
        return remote(relay.at[pl.ds(0, size)], relay.at[pl.ds(0, size)], pass_send.at[0], star_recv.at[0], own)

    @pl.when(is_star)
    def _():
        for c in range(2):
            pltpu.make_async_copy(stage.at[c], got_ref.at[pl.ds(0, 8)], out_sem.at[c]).wait()

        partner_copy().wait_send()

    @pl.when(role == 1)
    def _():
        own_all().wait_send()

    @pl.when(role > 1)
    def _():
        own_all().wait_send()

    for size in (2, 4, 8, 12, 16):
        @pl.when(count == size)
        def _():
            pass_all(size).wait_send()

    for half in range(2):
        @pl.when(own != 2 * star + half)
        def _():
            top_copy(half, own).wait_send()

    @pl.when(is_star)
    def _():
        mail_part(n_own - 2, 0).wait_send()
        name_part(1).wait_send()

    @pl.when(not_star)
    def _():
        mail_part(n_own - 3, 0).wait_send()
        name_part(2).wait_send()

    @pl.when(tile >= 0)
    def _():
        extra_part(17).wait_send()

    @pl.when(tile < 0)
    def _():
        extra_part(18).wait_send()

    @pl.when(not_star)
    def _():
        few_part(CHIPS - 2).wait_send()

    @pl.when(tile >= 0)
    def _():
        tile_part(CHIPS - 2, 128).wait_send()


def move(star, star_data, rest_data, top_data):
    vmem = pl.BlockSpec(memory_space=pltpu.VMEM)
    dma = pltpu.SemaphoreType.DMA
    n_own = 2 * CHIPS
    return pl.pallas_call(
        functools.partial(move_kernel, star),
        out_shape=(
            jax.ShapeDtypeStruct((n_own * CAP, TOK * HALF), jnp.bfloat16),
            jax.ShapeDtypeStruct((QS, ROOM, PIECE), jnp.bfloat16),
            jax.ShapeDtypeStruct((BLOCKS, 1, BLOCK), jnp.float32),
            jax.ShapeDtypeStruct((BLOCKS, 1, BLOCK), jnp.float32),
            jax.ShapeDtypeStruct((1, HALF), jnp.float32),
            jax.ShapeDtypeStruct((1, HALF), jnp.float32),
            jax.ShapeDtypeStruct((1,), jnp.int32),
        ),
        in_specs=[vmem, vmem, vmem],
        out_specs=(pl.BlockSpec(memory_space=pl.ANY), vmem, vmem, vmem, vmem, vmem, pl.BlockSpec(memory_space=pltpu.SMEM)),
        scratch_shapes=[
            pltpu.VMEM((n_own, REST, WIDE + 128), jnp.bfloat16),
            pltpu.VMEM((CHIPS * ROOM, n_own * REST), jnp.bfloat16),
            pltpu.VMEM((CHIPS, ROOM, WIDE), jnp.bfloat16),
            pltpu.VMEM((CHIPS, ROOM, PIECE), jnp.bfloat16),
            pltpu.VMEM((16, 2, 4, CAP, PIECE), jnp.bfloat16),
            pltpu.VMEM((n_own, 1, 384), jnp.float32),
            pltpu.VMEM((4, 1, 384), jnp.float32),
            pltpu.VMEM((4, 1, 384), jnp.float32),
            pltpu.VMEM((n_own, QS, CAP, PIECE), jnp.bfloat16),
            pltpu.VMEM((2, CAP, TOK * HALF), jnp.bfloat16),
            pltpu.VMEM((8, PIECE), jnp.float32),
            pltpu.VMEM((8, PIECE), jnp.float32),
            dma((3,)), dma((2,)), dma((2,)), dma((2,)),
            dma((1,)), dma((1,)), dma((16,)), dma((n_own,)),
            dma((2,)), dma((1,)), dma((4,)), dma((4,)), dma((4,)), dma((4,)), dma((2,)),
        ],
        compiler_params=pltpu.CompilerParams(collective_id=2 + star, has_side_effects=True, vmem_limit_bytes=40 << 20),
        name="move",
    )(star_data, rest_data, top_data)


def finish_kernel(flag_ref, got_ref, few_ref, key_ref, place_ref, codes_ref, buf, map_ref, in_sems, out_sem):
    rows = buf.shape[0]
    star = flag_ref[0] != 0

    def block(i):
        return pl.ds(pl.multiple_of(i * ENC_ROWS, ENC_ROWS), ENC_ROWS)

    def load(i):
        return pltpu.make_async_copy(got_ref.at[block(i)], buf.at[block(i)], in_sems.at[i])

    def save(i):
        return pltpu.make_async_copy(buf.at[block(i)], codes_ref.at[block(i)], out_sem)

    @pl.when(star)
    def _():
        @pl.loop(0, rows // ENC_ROWS)
        def _(i):
            load(i).start()

        @pl.loop(0, rows // ENC_ROWS)
        def _(i):
            load(i).wait()
            save(i).start()

    @pl.when(jnp.logical_not(star))
    def _():
        first = (lax.broadcasted_iota(jnp.int32, (ROOM, BLOCK), 0) + flag_ref[1] * ROOM).astype(jnp.float32)
        spot = lax.broadcasted_iota(jnp.int32, (rows, BLOCK), 0).astype(jnp.float32)
        total = jnp.zeros((rows, ROOM), jnp.float32)
        for i in range(BLOCKS):
            spread = jnp.where(spot == place_ref[i], 1.0, 0.0).astype(jnp.bfloat16)
            ranked = jnp.where(first == key_ref[i], 1.0, 0.0).astype(jnp.bfloat16)
            total += lax.dot_general(spread, ranked, (((1,), (1,)), ((), ())), preferred_element_type=jnp.float32)
        map_ref[...] = total.astype(jnp.bfloat16)

        @pl.loop(0, QS)
        def _(q):
            lanes = pl.ds(pl.multiple_of(q * PIECE, 128), PIECE)
            out = jnp.dot(map_ref[...], few_ref[q], preferred_element_type=jnp.float32)
            buf[:, lanes] = out.astype(jnp.bfloat16)
            pltpu.make_async_copy(buf.at[:, lanes], codes_ref.at[:, lanes], out_sem).start()

    pltpu.make_async_copy(buf, codes_ref, out_sem).wait()


def finish(flag, got, few, keys, places):
    vmem = pl.BlockSpec(memory_space=pltpu.VMEM)
    hbm = pl.BlockSpec(memory_space=pl.ANY)
    return pl.pallas_call(
        finish_kernel,
        out_shape=jax.ShapeDtypeStruct(got.shape, jnp.bfloat16),
        in_specs=[pl.BlockSpec(memory_space=pltpu.SMEM), hbm, vmem, vmem, vmem],
        out_specs=hbm,
        scratch_shapes=[
            pltpu.VMEM(got.shape, jnp.bfloat16),
            pltpu.VMEM((got.shape[0], ROOM), jnp.bfloat16),
            pltpu.SemaphoreType.DMA((got.shape[0] // ENC_ROWS,)),
            pltpu.SemaphoreType.DMA,
        ],
        compiler_params=pltpu.CompilerParams(vmem_limit_bytes=24 << 20),
        name="finish",
    )(flag, got, few, keys, places)


def body(block_pool, sel_index, sel_layer, counts):
    star = sel_layer[0]
    star_data, rest_data, top_data = pack(block_pool, sel_index, sel_layer, counts)
    got, few, keys, places, steps, error, full = lax.switch(
        star, [functools.partial(move, layer) for layer in range(LAYERS)], star_data, rest_data, top_data)

    def sparse():
        chip = lax.axis_index("own") // 2
        flag = jnp.stack([(chip == star).astype(jnp.int32), chip.astype(jnp.int32)])
        return finish(flag, got, few, keys, places), steps, error

    def dense():
        parted = flatten(block_pool, sel_index, sel_layer, counts).reshape(2 * LAYERS, CAP, TOK * HALF)
        arrived = lax.all_to_all(parted, "own", split_axis=0, concat_axis=0, tiled=True)
        arrived = arrived.reshape(2 * LAYERS * CAP, TOK * HALF)
        all_steps = peak_steps(arrived)
        codes, sums = encode(arrived, all_steps)
        return codes, all_steps, error_mean(sums)

    codes, steps, error = lax.cond(full[0] > 0, dense, sparse)
    return codes.reshape(1, 1, 2 * LAYERS, CAP, TOK * HALF), steps, error


def solution(mesh):
    return jax.shard_map(
        body,
        mesh=mesh,
        in_specs=(
            P(("own", "rep"), None, None),
            P(("own", "rep")),
            P(("own", "rep")),
            P(("own", "rep")),
        ),
        out_specs=(P("own", "rep", None, None, None), P("own", None), P("own", None)),
        check_vma=False,
    )
```

```python
import functools
import jax
import jax.numpy as jnp
from jax import lax
from jax.experimental import pallas as pl
from jax.experimental.pallas import tpu as pltpu
from jax.sharding import PartitionSpec as P

HEADROOM = 0.5
HALF = 288
PIECE = 4 * HALF
TOK = 64
STEP_TOK = 16
CAP = 8
LAYERS = 16
SEL = 32
CHIPS = 16
QS = 16
REST = SEL - CAP
ROOM = 32
BLOCK = 384
BLOCKS = 2
WIDE = PIECE + 128
DENOM = 32.0 * 4.0 * 8.0 * 64.0


def flatten_kernel(idx_ref, layer_ref, count_ref, pool_ref, out_ref, blocks, picks, seen, sems):
    step = pl.program_id(0)
    rows = STEP_TOK * LAYERS * CAP
    cols = SEL * STEP_TOK

    @pl.when(step == 0)
    def _():
        for j in range(SEL):
            pltpu.make_async_copy(pool_ref.at[idx_ref[j]], blocks.at[j], sems.at[j]).start()
        for layer in range(LAYERS):
            seen[layer] = 0
        col = lax.broadcasted_iota(jnp.int32, (1, cols), 1)
        key = jnp.full((1, cols), -1, jnp.int32)
        live = count_ref[0]
        for j in range(SEL):
            layer = layer_ref[j]
            rank = seen[layer]
            seen[layer] = rank + 1
            slot = jnp.where(j < live, layer * CAP + rank, -1)
            key = jnp.where(col // STEP_TOK == j, slot, key)
        row = lax.broadcasted_iota(jnp.int32, (rows, cols), 0)
        hit = (row % (LAYERS * CAP) == key) & (row // (LAYERS * CAP) == col % STEP_TOK)
        picks[...] = jnp.where(hit, 1.0, 0.0).astype(jnp.bfloat16)
        for j in range(SEL):
            pltpu.make_async_copy(pool_ref.at[idx_ref[j]], blocks.at[j], sems.at[j]).wait()

    start = pl.multiple_of(step * STEP_TOK, STEP_TOK)
    data = blocks[:, pl.ds(start, STEP_TOK), :].reshape(cols, 2 * HALF)
    slots = LAYERS * CAP

    @pl.loop(0, STEP_TOK // 4)
    def _(part):
        rows = pl.ds(pl.multiple_of(part * 4 * slots, 4 * slots), 4 * slots)
        moved = jnp.dot(picks[rows, :], data, preferred_element_type=jnp.float32)
        at = pl.ds(pl.multiple_of(part * PIECE, 128), PIECE)
        for half in range(2):
            lanes = [moved[t * slots:(t + 1) * slots, half * HALF:(half + 1) * HALF] for t in range(4)]
            flat = jnp.concatenate(lanes, axis=1).astype(jnp.bfloat16)
            out_ref[:, half, :, at] = flat.reshape(LAYERS, CAP, PIECE)


def flatten(block_pool, sel_index, sel_layer, counts):
    smem = pl.BlockSpec(memory_space=pltpu.SMEM)
    return pl.pallas_call(
        flatten_kernel,
        grid=(TOK // STEP_TOK,),
        out_shape=jax.ShapeDtypeStruct((LAYERS, 2, CAP, TOK * HALF), jnp.bfloat16),
        in_specs=[smem, smem, smem, pl.BlockSpec(memory_space=pl.ANY)],
        out_specs=pl.BlockSpec((LAYERS, 2, CAP, STEP_TOK * HALF), lambda i: (0, 0, 0, i)),
        scratch_shapes=[
            pltpu.VMEM((SEL, TOK, 2 * HALF), jnp.bfloat16),
            pltpu.VMEM((STEP_TOK * LAYERS * CAP, SEL * STEP_TOK), jnp.bfloat16),
            pltpu.SMEM((LAYERS,), jnp.int32),
            pltpu.SemaphoreType.DMA((SEL,)),
        ],
        compiler_params=pltpu.CompilerParams(dimension_semantics=("arbitrary",), vmem_limit_bytes=48 << 20),
        name="flatten",
    )(sel_index, sel_layer, counts, block_pool)


def rep_exchange(value, inbox, send_sems, recv_sems):
    reps = lax.axis_size("rep")
    me = lax.axis_index("rep")
    inbox[0] = value
    copies = []
    for k in range(1, reps):
        copies.append(pltpu.make_async_remote_copy(
            src_ref=inbox.at[0], dst_ref=inbox.at[k],
            send_sem=send_sems.at[k], recv_sem=recv_sems.at[k],
            device_id={"rep": lax.rem(me + k, reps)}, device_id_type=pl.DeviceIdType.MESH))
    for copy in copies:
        copy.start()
    for copy in copies:
        copy.wait()


def rep_barrier_signal():
    reps = lax.axis_size("rep")
    me = lax.axis_index("rep")
    barrier = pltpu.get_barrier_semaphore()
    for k in range(1, reps):
        pl.semaphore_signal(barrier, inc=1, device_id={"rep": lax.rem(me + k, reps)},
                            device_id_type=pl.DeviceIdType.MESH)
    return barrier


def fold4(row):
    return [row[:, k * HALF:(k + 1) * HALF] for k in range(4)]


def peak_kernel(got_ref, steps_ref, inbox, send_sems, recv_sems):
    barrier = rep_barrier_signal()
    rows = got_ref.shape[0]

    def chunk(i, peak):
        at = pl.multiple_of(i * 16, 16)
        for q in range(TOK // 4):
            part = jnp.abs(got_ref[pl.ds(at, 16), q * PIECE:(q + 1) * PIECE])
            peak = jnp.maximum(peak, part)
        return peak

    peak = lax.fori_loop(0, rows // 16, chunk, jnp.zeros((16, PIECE), jnp.bfloat16))
    row = jnp.max(peak.astype(jnp.float32), axis=0, keepdims=True)
    a, b, c, d = fold4(row)
    row = jnp.maximum(jnp.maximum(a, b), jnp.maximum(c, d))
    pl.semaphore_wait(barrier, 3)
    rep_exchange(jnp.concatenate([row, row[:, :384 - HALF]], axis=1), inbox, send_sems, recv_sems)
    top = jnp.maximum(jnp.maximum(inbox[0], inbox[1]), jnp.maximum(inbox[2], inbox[3]))
    steps_ref[...] = HEADROOM * jnp.maximum(top[:, :HALF], 1.0) / 127.0


def small_scratch():
    return [
        pltpu.VMEM((4, 1, 384), jnp.float32),
        pltpu.SemaphoreType.DMA((4,)),
        pltpu.SemaphoreType.DMA((4,)),
    ]


def peak_steps(got):
    vmem = pl.BlockSpec(memory_space=pltpu.VMEM)
    return pl.pallas_call(
        peak_kernel,
        out_shape=jax.ShapeDtypeStruct((1, HALF), jnp.float32),
        in_specs=[vmem], out_specs=vmem,
        scratch_shapes=small_scratch(),
        compiler_params=pltpu.CompilerParams(collective_id=0, has_side_effects=True, vmem_limit_bytes=24 << 20),
        name="peak_steps",
    )(got)


def error_kernel(sums_ref, out_ref, inbox, send_sems, recv_sems):
    barrier = rep_barrier_signal()
    pl.semaphore_wait(barrier, 3)
    rep_exchange(sums_ref[...], inbox, send_sems, recv_sems)
    total = (inbox[0] + inbox[1]) + (inbox[2] + inbox[3])
    out_ref[...] = total[:, :HALF] * (1.0 / DENOM)


def error_mean(sums):
    vmem = pl.BlockSpec(memory_space=pltpu.VMEM)
    return pl.pallas_call(
        error_kernel,
        out_shape=jax.ShapeDtypeStruct((1, HALF), jnp.float32),
        in_specs=[vmem], out_specs=vmem,
        scratch_shapes=small_scratch(),
        compiler_params=pltpu.CompilerParams(collective_id=1, has_side_effects=True),
        name="error_mean",
    )(sums)


ENC_ROWS = 32


def encode_kernel(got_ref, steps_ref, codes_ref, sums_ref, inv_ref, acc_ref):
    step = pl.program_id(0)

    @pl.when(step == 0)
    def _():
        inv = 1.0 / steps_ref[...]
        inv_ref[...] = jnp.broadcast_to(jnp.concatenate([inv] * 4, axis=1), inv_ref.shape)
        acc_ref[...] = jnp.zeros_like(acc_ref)

    @pl.loop(0, QS)
    def _(q):
        lanes = pl.ds(pl.multiple_of(q * PIECE, 128), PIECE)
        data = got_ref[:, lanes].reshape(ENC_ROWS // 8, 8, PIECE)
        codes_ref[:, lanes] = code_of(data, inv_ref, acc_ref).reshape(ENC_ROWS, PIECE)

    @pl.when(step == pl.num_programs(0) - 1)
    def _():
        row = jnp.sum(acc_ref[...], axis=0, keepdims=True)
        a, b, c, d = fold4(row)
        row = (a + b) + (c + d)
        sums_ref[...] = jnp.concatenate([row, row[:, :384 - HALF]], axis=1)


def encode(got, steps):
    rows = got.shape[0]
    return pl.pallas_call(
        encode_kernel,
        grid=(rows // ENC_ROWS,),
        out_shape=(jax.ShapeDtypeStruct(got.shape, jnp.bfloat16), jax.ShapeDtypeStruct((1, 384), jnp.float32)),
        in_specs=[pl.BlockSpec((ENC_ROWS, TOK * HALF), lambda i: (i, 0)), pl.BlockSpec((1, HALF), lambda i: (0, 0))],
        out_specs=(pl.BlockSpec((ENC_ROWS, TOK * HALF), lambda i: (i, 0)), pl.BlockSpec((1, 384), lambda i: (0, 0))),
        scratch_shapes=[pltpu.VMEM((8, PIECE), jnp.float32), pltpu.VMEM((8, PIECE), jnp.float32)],
        compiler_params=pltpu.CompilerParams(dimension_semantics=("arbitrary",), vmem_limit_bytes=24 << 20),
        name="encode",
    )(got, steps)


def pack_kernel(idx_ref, layer_ref, count_ref, pool_ref, star_ref, rest_ref, name_ref, top_ref, blocks, picks, tops, sems):
    step = pl.program_id(0)
    size = SEL * STEP_TOK

    @pl.when(step == 0)
    def _():
        for j in range(SEL):
            pltpu.make_async_copy(pool_ref.at[idx_ref[j]], blocks.at[j], sems.at[j]).start()
        row = lax.broadcasted_iota(jnp.int32, (size, size), 0)
        col = lax.broadcasted_iota(jnp.int32, (size, size), 1)
        hit = (row % SEL == col // STEP_TOK) & (row // SEL == col % STEP_TOK)
        picks[...] = jnp.where(hit, 1.0, 0.0).astype(jnp.bfloat16)
        tops[...] = jnp.zeros_like(tops)
        line = lax.broadcasted_iota(jnp.int32, (8, 128), 1)
        layers = jnp.full((8, 128), -1.0, jnp.float32)
        live = count_ref[0]
        for j in range(CAP, SEL):
            name = jnp.where(j < live, layer_ref[j], -1).astype(jnp.float32)
            layers = jnp.where(line == j - CAP, name, layers)
        name_ref[...] = layers.astype(jnp.bfloat16)

        for j in range(SEL):
            pltpu.make_async_copy(pool_ref.at[idx_ref[j]], blocks.at[j], sems.at[j]).wait()

    start = pl.multiple_of(step * STEP_TOK, STEP_TOK)
    data = blocks[:, pl.ds(start, STEP_TOK), :].reshape(size, 2 * HALF)
    moved = jnp.dot(picks[...], data, preferred_element_type=jnp.float32)
    for part in range(STEP_TOK // 4):
        for half in range(2):
            first = part * 4
            lanes = [moved[t * SEL:(t + 1) * SEL, half * HALF:(half + 1) * HALF] for t in range(first, first + 4)]
            flat = jnp.concatenate(lanes, axis=1)
            star_ref[half, part] = flat[:CAP].astype(jnp.bfloat16)
            rest_ref[part, half] = flat[CAP:].astype(jnp.bfloat16)
            tops[half] = jnp.maximum(tops[half], jnp.abs(flat[:CAP]))

    @pl.when(step == pl.num_programs(0) - 1)
    def _():
        for half in range(2):
            top_ref[half] = pad_row(fold_max(jnp.max(tops[half], axis=0, keepdims=True)))


def fold_max(row):
    a, b, c, d = fold4(row)
    return jnp.maximum(jnp.maximum(a, b), jnp.maximum(c, d))


def pad_row(row):
    return jnp.concatenate([row, jnp.zeros((1, 384 - HALF), jnp.float32)], axis=1)


def pack(block_pool, sel_index, sel_layer, counts):
    smem = pl.BlockSpec(memory_space=pltpu.SMEM)
    parts = STEP_TOK // 4
    return pl.pallas_call(
        pack_kernel,
        grid=(TOK // STEP_TOK,),
        out_shape=(
            jax.ShapeDtypeStruct((2, QS, CAP, PIECE), jnp.bfloat16),
            jax.ShapeDtypeStruct((QS, 2, REST, PIECE), jnp.bfloat16),
            jax.ShapeDtypeStruct((8, 128), jnp.bfloat16),
            jax.ShapeDtypeStruct((2, 1, 384), jnp.float32),
        ),
        in_specs=[smem, smem, smem, pl.BlockSpec(memory_space=pl.ANY)],
        out_specs=(
            pl.BlockSpec((2, parts, CAP, PIECE), lambda i: (0, i, 0, 0)),
            pl.BlockSpec((parts, 2, REST, PIECE), lambda i: (i, 0, 0, 0)),
            pl.BlockSpec((8, 128), lambda i: (0, 0)),
            pl.BlockSpec((2, 1, 384), lambda i: (0, 0, 0)),
        ),
        scratch_shapes=[
            pltpu.VMEM((SEL, TOK, 2 * HALF), jnp.bfloat16),
            pltpu.VMEM((SEL * STEP_TOK, SEL * STEP_TOK), jnp.bfloat16),
            pltpu.VMEM((2, CAP, PIECE), jnp.float32),
            pltpu.SemaphoreType.DMA((SEL,)),
        ],
        compiler_params=pltpu.CompilerParams(dimension_semantics=("arbitrary",), vmem_limit_bytes=24 << 20),
        name="pack",
    )(sel_index, sel_layer, counts, block_pool)


def tree(star):
    sx, sz = divmod(star, 4)

    def at(dx, dz):
        return (sx + dx) % 4 * 4 + (sz + dz) % 4

    near = [at(0, 1), at(1, 0), at(0, 3), at(3, 0)]
    diag = [at(1, 1), at(1, 3), at(3, 3), at(3, 1)]
    third = [at(1, 2), at(2, 3), at(3, 2), at(2, 1)]
    far = at(2, 2)
    over_z, over_x = at(0, 2), at(2, 0)
    role = {star: 0, far: 4, over_z: 2, over_x: 4, third[0]: 4, third[2]: 4}
    count, hop, up, origin, shift = {over_z: 8}, {}, {over_z: near[0]}, {}, {}
    light = 2 if sz % 2 == 0 else 0
    for r in range(4):
        role[near[r]], role[diag[r]] = 1, 2
        up[near[r]], up[diag[r]] = star, near[r]
        count[near[r]], count[diag[r]] = (12, 4) if r % 2 == 0 else (8, 2)
        hop[diag[r]] = [(near[r], k) for k in range(4)]
    count[near[light]] = 16
    for r in (1, 3):
        role[third[r]] = 3
        up[third[r]] = diag[r]
        count[third[r]] = 2
    hop[third[0]] = [(over_z, k) for k in range(4)]
    hop[third[2]] = [(over_z, 4 + k) for k in range(4)]
    hop[third[3]] = [(diag[0], k) for k in range(4)]
    hop[third[1]] = [(diag[2], k) for k in range(4)]
    hop[far] = [(third[1], 0), (third[1], 1), (third[3], 0), (third[3], 1)]
    hop[over_z] = [(near[light], 12 + k) for k in range(4)]
    hop[over_x] = [(near[1], 12), (near[1], 13), (near[3], 12), (near[3], 13)]
    origin[near[0]] = (diag[0], third[0], third[3], over_z)
    origin[near[2]] = (diag[2], third[2], third[1], over_z)
    origin[near[1]] = (diag[1], far, far, over_x)
    origin[near[3]] = (diag[3], far, far, over_x)
    shift[near[0]], shift[near[1]], shift[near[2]], shift[near[3]] = (0, 0), (0, 0), (0, 0), (2, 2)
    away = {at(dx, dz): (dx - 1) * 3 + dz - 1 for dx in range(1, 4) for dz in range(1, 4)}
    arrival = [star, *near, *diag, over_x, over_z, third[0], third[2], far, third[1], third[3]]
    return role, count, hop, up, origin, shift, away, dict(enumerate(arrival))


ORDER = {4: 1, 5: 0, 6: 3, 7: 2, 12: 3, 13: 0, 14: 1, 15: 2, 8: 2, 9: 0, 10: 1, 11: 3, 0: 1, 1: 3, 2: 2, 3: 0}


def turn(chip, step):
    lead = lax.rem(step, 4)
    dx = jnp.where(lead == 0, 1, jnp.where(lead == 1, 3, jnp.where(lead == 2, 2, 0)))
    dz = pick(dx * 4 + step // 4, ORDER)
    return lax.rem(chip // 4 + dx, 4) * 4 + lax.rem(lax.rem(chip, 4) + dz, 4)


def pick(index, table, default=0):
    out = jnp.int32(default)
    for key, value in table.items():
        out = jnp.where(index == key, jnp.int32(value), out)
    return out


MESH = pl.DeviceIdType.MESH


def sort_masks(before, same, spread, own_lane, local):
    @pl.loop(0, BLOCK // 16)
    def _(i):
        rows = pl.ds(pl.multiple_of(i * 16, 16), 16)

        def grid(width):
            row = lax.broadcasted_iota(jnp.int32, (16, width), 0) + i * 16
            return row, lax.broadcasted_iota(jnp.int32, (16, width), 1)

        row, col = grid(BLOCK)
        before[rows, :] = jnp.where(col < row, 1.0, 0.0).astype(jnp.bfloat16)
        same[rows, :] = jnp.where((col < row) & (col // REST == row // REST), 1.0, 0.0).astype(jnp.bfloat16)
        row, col = grid(BLOCK // REST)
        spread[rows, :] = jnp.where(row // REST == col, 1.0, 0.0).astype(jnp.bfloat16)
        row, col = grid(128)
        own_lane[rows, :] = jnp.where(row % REST == col, 1.0, 0.0)
        local[rows, :] = (row // REST).astype(jnp.float32)


def sort_mail(names_ref, chip, key_ref, place_ref, select, before, same, spread, own_lane, local):
    sources = BLOCK // REST
    lane = lax.broadcasted_iota(jnp.int32, (BLOCK, 128), 1).astype(jnp.float32)
    mine = chip.astype(jnp.float32)

    def block(i, carry):
        lists = jnp.max(names_ref[pl.ds(i * sources, sources)].astype(jnp.float32), axis=1).astype(jnp.bfloat16)
        lists = jnp.dot(spread[...], lists, preferred_element_type=jnp.float32)
        names = jnp.sum(lists * own_lane[...], axis=1, keepdims=True)
        hits = jnp.where(names == lane, 1.0, 0.0)
        hits16 = hits.astype(jnp.bfloat16)
        rank = jnp.dot(before[...], hits16, preferred_element_type=jnp.float32) + carry
        slot = jnp.dot(same[...], hits16, preferred_element_type=jnp.float32)
        rank = jnp.sum(rank * hits, axis=1, keepdims=True)
        slot = jnp.sum(slot * hits, axis=1, keepdims=True)
        source = local[...] + (i * sources).astype(jnp.float32)
        key = jnp.where(rank < ROOM, names * ROOM + rank, -1.0)
        place = jnp.where(names == mine, source * CAP + slot, -1.0)
        key_ref[i] = jnp.transpose(key)[:1]
        place_ref[i] = jnp.transpose(place)[:1]
        return carry + jnp.sum(hits, axis=0, keepdims=True)

    total = lax.fori_loop(0, BLOCKS, block, jnp.zeros((1, 128), jnp.float32))

    @pl.loop(0, CHIPS)
    def _(layer):
        at = pl.multiple_of(layer * ROOM, ROOM)
        want = (lax.broadcasted_iota(jnp.int32, (ROOM, BLOCK), 0) + at).astype(jnp.float32)
        for i in range(BLOCKS):
            hit = jnp.where(want == key_ref[i], 1.0, 0.0).astype(jnp.bfloat16)
            select[pl.ds(at, ROOM), i * BLOCK:(i + 1) * BLOCK] = hit

    return total


def code_of(data, inv, acc):
    scaled = data.astype(jnp.float32) * inv[...][None]
    code = jnp.clip(scaled, -127.0, 127.0).astype(jnp.bfloat16)
    gap = scaled - code.astype(jnp.float32)
    acc[...] += jnp.sum(gap * gap, axis=0)
    return code


def move_kernel(star, star_ref, rest_ref, name_ref, top_ref, got_ref, few_ref, key_ref, place_ref, steps_ref, error_ref, full_ref,
                before, same, spread, own_lane, local, mail, names, select, chosen, inbox, relay, tops, inrep, inrep2, land, stage, inv, acc,
                mail_send, mail_recv, few_send, few_recv, own_send, pass_send, relay_recv, star_recv,
                top_send, top_recv, rep_send, rep_recv, sum_send, sum_recv, out_sem):
    own = lax.axis_index("own")
    rep = lax.axis_index("rep")
    n_own = 2 * CHIPS
    chip = own // 2
    core = own % 2
    role_of, count_of, hop_of, up_of, origin_of, shift_of, away_of, arrival_of = tree(star)
    role = pick(chip, role_of)
    up = pick(chip, up_of)
    count = pick(chip, count_of)
    tile = pick(chip, away_of, -1)
    over_z = star // 4 * 4 + (star + 2) % 4
    other_near = star // 4 * 4 + (star + 3) % 4
    is_star = role == 0
    not_star = role != 0

    barrier = pltpu.get_barrier_semaphore()

    @pl.loop(1, n_own)
    def _(k):
        pl.semaphore_signal(barrier, inc=1, device_id={"own": lax.rem(own + k, n_own)}, device_id_type=MESH)

    for k in range(1, 4):
        pl.semaphore_signal(barrier, inc=1, device_id={"rep": lax.rem(rep + k, 4)}, device_id_type=MESH)
    pl.semaphore_wait(barrier, n_own - 1 + 3)

    def remote(src, dst, send, recv, to):
        return pltpu.make_async_remote_copy(src_ref=src, dst_ref=dst, send_sem=send, recv_sem=recv,
                                            device_id={"own": to}, device_id_type=MESH)

    def mail_copy(to, frm):
        return remote(rest_ref.at[to // 2, to % 2], mail.at[frm, :, pl.ds(0, PIECE)], mail_send.at[0], mail_recv.at[0], to)

    def name_copy(to):
        return remote(name_ref, names.at[own], mail_send.at[1], mail_recv.at[2], to)

    def lane_of(which):
        return pl.ds(pl.multiple_of(which * 128, 128), 128)

    def extra_copy(to_chip, half):
        return remote(rest_ref.at[star, half, :, lane_of(pick(to_chip, away_of))], mail.at[own, :, pl.ds(PIECE, 128)],
                      mail_send.at[2], mail_recv.at[1], 2 * to_chip + half)

    def top_copy(half, frm):
        return remote(top_ref.at[half], tops.at[frm], top_send.at[half], top_recv.at[0], 2 * star + half)

    for half in range(2):
        @pl.when(own != 2 * star + half)
        def _():
            top_copy(half, own).start()

        @pl.when(own == 2 * star + half)
        def _():
            tops[own] = top_ref[half]

    def near_copy(half):
        return remote(star_ref.at[half], land.at[own], own_send.at[0], star_recv.at[own], 2 * star + half)

    def hop_copy(k):
        to = pick(chip, {c: h[k][0] for c, h in hop_of.items()}) * 2 + core
        slot = pick(chip, {c: h[k][1] for c, h in hop_of.items()})
        return remote(star_ref.at[:, pl.ds(4 * k, 4)], relay.at[slot], own_send.at[0], relay_recv.at[slot], to)

    @pl.when(role == 1)
    def _():
        for half in range(2):
            near_copy(half).start()

    @pl.when(role > 1)
    def _():
        for k in range(4):
            hop_copy(k).start()

    def partner_copy():
        return remote(star_ref.at[1 - core], land.at[own], own_send.at[0], star_recv.at[own], 2 * star + 1 - core)

    @pl.when(is_star)
    def _():
        partner_copy().start()

        @pl.loop(0, QS)
        def _(q):
            land[own, q] = star_ref[core, q]

    @pl.loop(0, n_own)
    def _(k):
        half = lax.rem(k, 2)
        to_chip = turn(chip, k // 2)

        @pl.when(2 * to_chip + half != own)
        def _():
            name_copy(2 * to_chip + half).start()

        @pl.when((to_chip != star) & (2 * to_chip + half != own))
        def _():
            mail_copy(2 * to_chip + half, own).start()

        @pl.when((pick(to_chip, away_of, -1) >= 0) & (2 * to_chip + half != own))
        def _():
            extra_copy(to_chip, half).start()

    def relay_in(k):
        return remote(relay.at[k], relay.at[k], pass_send.at[0], relay_recv.at[k], own)

    def pass_near(k, half):
        group = k // 4
        origins = [pick(chip, {c: o[i] for c, o in origin_of.items()}) for i in range(4)]
        origin = jnp.where(group == 0, origins[0], jnp.where(group == 1, origins[1],
                           jnp.where(group == 2, origins[2], origins[3])))
        shifts = [pick(chip, {c: o[i] for c, o in shift_of.items()}) for i in range(2)]
        quarter = lax.rem(k, 4) + jnp.where(group == 1, shifts[0], jnp.where(group == 3, shifts[1], 0))
        frm = 2 * origin + core
        return remote(relay.at[k, half], land.at[frm, pl.ds(4 * quarter, 4)],
                      pass_send.at[0], star_recv.at[frm], 2 * star + half)

    def pass_diag(k):
        slot = jnp.where(chip == over_z, 4 + lax.rem(k, 4), jnp.where(count == 4, 8 + k, 4 + k))
        to = jnp.where((chip == over_z) & (k >= 4), other_near, up)
        return remote(relay.at[k], relay.at[slot], pass_send.at[0], relay_recv.at[slot], 2 * to + core)

    def pass_third(k):
        return remote(relay.at[k], relay.at[k], pass_send.at[0], relay_recv.at[k], 2 * up + core)

    def near_order(i):
        straight = jnp.where(count == 16, 4, jnp.where(count == 8, 2, 0))
        return jnp.where(i < 4, i, jnp.where(i < 4 + straight, i + 8, i - straight))

    def pass_near_range(low, high):
        @pl.when(role == 1)
        def _():
            @pl.loop(low, high)
            def _(i):
                k = near_order(i)
                relay_in(k).wait_recv()
                for half in range(2):
                    pass_near(k, half).start()

    def pass_diag_range(low, high):
        @pl.when(role == 2)
        def _():
            @pl.loop(low, high)
            def _(k):
                relay_in(k).wait_recv()
                pass_diag(k).start()

    sort_masks(before, same, spread, own_lane, local)
    early_diag = jnp.where(count == 2, 0, count)
    early_near = jnp.where(count == 16, 8, jnp.where(count == 12, 8, 6))
    pass_diag_range(0, early_diag)
    pass_near_range(0, early_near)

    def mail_part(size, which):
        ref = mail.at[pl.ds(0, size), :, pl.ds(0, PIECE)]
        return remote(ref, ref, mail_send.at[which], mail_recv.at[0], own)

    def name_all():
        ref = names.at[pl.ds(0, n_own - 1)]
        return remote(ref, ref, mail_send.at[1], mail_recv.at[2], own)

    def extra_part(size):
        ref = mail.at[pl.ds(0, size), :, pl.ds(PIECE, 128)]
        return remote(ref, ref, mail_send.at[2], mail_recv.at[1], own)

    @pl.when(not_star)
    def _():
        mail[own, :, :PIECE] = rest_ref[chip, core]
        mail_part(n_own - 1, 0).wait_recv()

    @pl.when(tile >= 0)
    def _():
        mail[own, :, PIECE:] = rest_ref[star, core, :, lane_of(tile)]
        extra_part(n_own - 1).wait_recv()

    names[own] = name_ref[...]
    name_all().wait_recv()
    count_by_layer = sort_mail(names, chip, key_ref, place_ref, select, before, same, spread, own_lane, local)

    parts = PIECE // 128

    @pl.loop(0, jnp.where(is_star, 0, jnp.where(tile >= 0, parts + 1, parts)))
    def _(part):
        data = mail[:, :, lane_of(part)].reshape(n_own * REST, 128)
        for rows in range(2):
            size = CHIPS * ROOM // 2
            out = jnp.dot(select[rows * size:(rows + 1) * size], data, preferred_element_type=jnp.float32)
            chosen[rows * 8:(rows + 1) * 8, :, lane_of(part)] = out.astype(jnp.bfloat16).reshape(8, ROOM, 128)

    def few_copy(to):
        return remote(chosen.at[to, :, pl.ds(0, PIECE)], inbox.at[chip], few_send.at[0], few_recv.at[0], 2 * to + core)

    def tile_copy(to):
        return remote(chosen.at[to, :, pl.ds(PIECE, 128)], inbox.at[star, :, lane_of(tile)], few_send.at[1], few_recv.at[1], 2 * to + core)

    def few_part(size):
        part = pl.ds(0, size)
        return remote(inbox.at[part], inbox.at[part], few_send.at[0], few_recv.at[0], own)

    def tile_part(size, lanes):
        ref = inbox.at[pl.ds(0, size), :, pl.ds(0, lanes)]
        return remote(ref, ref, few_send.at[1], few_recv.at[1], own)

    @pl.loop(0, CHIPS)
    def _(k):
        to = turn(chip, k)

        @pl.when((to != star) & (to != chip) & not_star)
        def _():
            few_copy(to).start()

            @pl.when(tile >= 0)
            def _():
                tile_copy(to).start()

    @pl.when(role == 3)
    def _():
        @pl.loop(0, 2)
        def _(k):
            relay_in(k).wait_recv()
            pass_third(k).start()

    pass_diag_range(early_diag, count)
    pass_near_range(early_near, count)

    @pl.when(not_star)
    def _():
        inbox[chip] = chosen[chip, :, :PIECE]

        @pl.when(tile >= 0)
        def _():
            inbox[star, :, lane_of(tile)] = chosen[chip, :, PIECE:]
            tile_part(1, 1024).wait_recv()

        @pl.when(tile < 0)
        def _():
            tile_part(1, PIECE).wait_recv()


        few_part(CHIPS - 2).wait_recv()

        def largest(q, best):
            return jnp.maximum(best, jnp.abs(inbox[q]))

        best = lax.fori_loop(0, QS, largest, jnp.zeros((ROOM, PIECE), jnp.bfloat16))
        inrep[0] = pad_row(fold_max(jnp.max(best.astype(jnp.float32), axis=0, keepdims=True)))

    @pl.when(is_star)
    def _():
        others = pl.ds(0, n_own - 1)
        remote(tops.at[others], tops.at[others], top_send.at[0], top_recv.at[0], own).wait_recv()

        inrep[0] = jnp.max(tops[...], axis=0)

    full = jnp.max(jnp.where(count_by_layer > ROOM, 1.0, 0.0), axis=1, keepdims=True)
    tail = lax.broadcasted_iota(jnp.int32, (1, 384), 1)
    inrep[0] = jnp.where(tail < HALF, inrep[0], full)

    rep_exchange(inrep[0], inrep, rep_send, rep_recv)
    top = jnp.maximum(jnp.maximum(inrep[0], inrep[1]), jnp.maximum(inrep[2], inrep[3]))
    steps = HEADROOM * jnp.maximum(top[:, :HALF], 1.0) / 127.0
    steps_ref[...] = steps
    full_ref[0] = jnp.max(jnp.where(tail < HALF, 0.0, top)).astype(jnp.int32)
    inv[...] = jnp.broadcast_to(jnp.concatenate([1.0 / steps] * 4, axis=1), inv.shape)
    acc[...] = jnp.zeros_like(acc)

    @pl.when(not_star)
    def _():
        @pl.loop(0, QS)
        def _(q):
            few_ref[q] = code_of(inbox[q].reshape(ROOM // 8, 8, PIECE), inv, acc).reshape(ROOM, PIECE)

    @pl.when(is_star)
    def _():
        @pl.loop(0, n_own)
        def _(k):
            slot = lax.rem(k, 2)
            frm = 2 * pick(k // 2, arrival_of) + slot
            out = pltpu.make_async_copy(stage.at[slot], got_ref.at[pl.ds(pl.multiple_of(8 * frm, 8), 8)], out_sem.at[slot])

            @pl.when(frm != own)
            def _():
                remote(land.at[frm], land.at[frm], own_send.at[0], star_recv.at[frm], own).wait_recv()

            @pl.when(k > 1)
            def _():
                out.wait()

            @pl.loop(0, QS // 2)
            def _(pair):
                for half in range(2):
                    q = 2 * pair + half
                    code = code_of(land[frm, pl.ds(q, 1)], inv, acc)
                    stage[slot, :, pl.ds(pl.multiple_of(q * PIECE, 128), PIECE)] = code[0]

            out.start()

    row = jnp.sum(acc[...], axis=0, keepdims=True)
    a, b, c, d = fold4(row)
    rep_exchange(pad_row((a + b) + (c + d)), inrep2, sum_send, sum_recv)
    total = (inrep2[0] + inrep2[1]) + (inrep2[2] + inrep2[3])
    error_ref[...] = total[:, :HALF] * (1.0 / DENOM)

    name_all().wait_send()

    def own_all():
        return remote(star_ref, star_ref, own_send.at[0], star_recv.at[0], own)

    def pass_all(size):
        return remote(relay.at[pl.ds(0, size)], relay.at[pl.ds(0, size)], pass_send.at[0], star_recv.at[0], own)

    @pl.when(is_star)
    def _():
        for c in range(2):
            pltpu.make_async_copy(stage.at[c], got_ref.at[pl.ds(0, 8)], out_sem.at[c]).wait()

        partner_copy().wait_send()

    @pl.when(role == 1)
    def _():
        own_all().wait_send()

    @pl.when(role > 1)
    def _():
        own_all().wait_send()

    for size in (2, 4, 8, 12, 16):
        @pl.when(count == size)
        def _():
            pass_all(size).wait_send()

    for half in range(2):
        @pl.when(own != 2 * star + half)
        def _():
            top_copy(half, own).wait_send()

    @pl.when(is_star)
    def _():
        mail_part(n_own - 2, 0).wait_send()

    @pl.when(not_star)
    def _():
        mail_part(n_own - 3, 0).wait_send()

    @pl.when(tile >= 0)
    def _():
        extra_part(17).wait_send()

    @pl.when(tile < 0)
    def _():
        extra_part(18).wait_send()

    @pl.when(not_star)
    def _():
        few_part(CHIPS - 2).wait_send()

    @pl.when(tile >= 0)
    def _():
        tile_part(CHIPS - 2, 128).wait_send()


def move(star, star_data, rest_data, name_data, top_data):
    vmem = pl.BlockSpec(memory_space=pltpu.VMEM)
    dma = pltpu.SemaphoreType.DMA
    n_own = 2 * CHIPS
    return pl.pallas_call(
        functools.partial(move_kernel, star),
        out_shape=(
            jax.ShapeDtypeStruct((n_own * CAP, TOK * HALF), jnp.bfloat16),
            jax.ShapeDtypeStruct((QS, ROOM, PIECE), jnp.bfloat16),
            jax.ShapeDtypeStruct((BLOCKS, 1, BLOCK), jnp.float32),
            jax.ShapeDtypeStruct((BLOCKS, 1, BLOCK), jnp.float32),
            jax.ShapeDtypeStruct((1, HALF), jnp.float32),
            jax.ShapeDtypeStruct((1, HALF), jnp.float32),
            jax.ShapeDtypeStruct((1,), jnp.int32),
        ),
        in_specs=[vmem, vmem, vmem, vmem],
        out_specs=(pl.BlockSpec(memory_space=pl.ANY), vmem, vmem, vmem, vmem, vmem, pl.BlockSpec(memory_space=pltpu.SMEM)),
        scratch_shapes=[
            pltpu.VMEM((BLOCK, BLOCK), jnp.bfloat16),
            pltpu.VMEM((BLOCK, BLOCK), jnp.bfloat16),
            pltpu.VMEM((BLOCK, BLOCK // REST), jnp.bfloat16),
            pltpu.VMEM((BLOCK, 128), jnp.float32),
            pltpu.VMEM((BLOCK, 128), jnp.float32),
            pltpu.VMEM((n_own, REST, WIDE), jnp.bfloat16),
            pltpu.VMEM((n_own, 8, 128), jnp.bfloat16),
            pltpu.VMEM((CHIPS * ROOM, n_own * REST), jnp.bfloat16),
            pltpu.VMEM((CHIPS, ROOM, WIDE), jnp.bfloat16),
            pltpu.VMEM((CHIPS, ROOM, PIECE), jnp.bfloat16),
            pltpu.VMEM((16, 2, 4, CAP, PIECE), jnp.bfloat16),
            pltpu.VMEM((n_own, 1, 384), jnp.float32),
            pltpu.VMEM((4, 1, 384), jnp.float32),
            pltpu.VMEM((4, 1, 384), jnp.float32),
            pltpu.VMEM((n_own, QS, CAP, PIECE), jnp.bfloat16),
            pltpu.VMEM((2, CAP, TOK * HALF), jnp.bfloat16),
            pltpu.VMEM((8, PIECE), jnp.float32),
            pltpu.VMEM((8, PIECE), jnp.float32),
            dma((3,)), dma((3,)), dma((2,)), dma((2,)),
            dma((1,)), dma((1,)), dma((16,)), dma((n_own,)),
            dma((2,)), dma((1,)), dma((4,)), dma((4,)), dma((4,)), dma((4,)), dma((2,)),
        ],
        compiler_params=pltpu.CompilerParams(collective_id=2 + star, has_side_effects=True, vmem_limit_bytes=40 << 20),
        name="move",
    )(star_data, rest_data, name_data, top_data)


COPY_ROWS = 16


def finish_kernel(flag_ref, got_ref, few_ref, key_ref, place_ref, codes_ref, buf, map_ref, in_sems, out_sem):
    rows = buf.shape[0]
    star = flag_ref[0] != 0

    def block(i):
        return pl.ds(pl.multiple_of(i * COPY_ROWS, COPY_ROWS), COPY_ROWS)

    def load(i):
        return pltpu.make_async_copy(got_ref.at[block(i)], buf.at[block(i)], in_sems.at[i])

    def save(i):
        return pltpu.make_async_copy(buf.at[block(i)], codes_ref.at[block(i)], out_sem)

    @pl.when(star)
    def _():
        @pl.loop(0, rows // COPY_ROWS)
        def _(i):
            load(i).start()

        @pl.loop(0, rows // COPY_ROWS)
        def _(i):
            load(i).wait()
            save(i).start()

    @pl.when(jnp.logical_not(star))
    def _():
        first = (lax.broadcasted_iota(jnp.int32, (ROOM, BLOCK), 0) + flag_ref[1] * ROOM).astype(jnp.float32)
        spot = lax.broadcasted_iota(jnp.int32, (rows, BLOCK), 0).astype(jnp.float32)
        total = jnp.zeros((rows, ROOM), jnp.float32)
        for i in range(BLOCKS):
            spread = jnp.where(spot == place_ref[i], 1.0, 0.0).astype(jnp.bfloat16)
            ranked = jnp.where(first == key_ref[i], 1.0, 0.0).astype(jnp.bfloat16)
            total += lax.dot_general(spread, ranked, (((1,), (1,)), ((), ())), preferred_element_type=jnp.float32)
        map_ref[...] = total.astype(jnp.bfloat16)

        @pl.loop(0, QS)
        def _(q):
            lanes = pl.ds(pl.multiple_of(q * PIECE, 128), PIECE)
            out = jnp.dot(map_ref[...], few_ref[q], preferred_element_type=jnp.float32)
            buf[:, lanes] = out.astype(jnp.bfloat16)
            pltpu.make_async_copy(buf.at[:, lanes], codes_ref.at[:, lanes], out_sem).start()

    pltpu.make_async_copy(buf, codes_ref, out_sem).wait()


def finish(flag, got, few, keys, places):
    vmem = pl.BlockSpec(memory_space=pltpu.VMEM)
    hbm = pl.BlockSpec(memory_space=pl.ANY)
    return pl.pallas_call(
        finish_kernel,
        out_shape=jax.ShapeDtypeStruct(got.shape, jnp.bfloat16),
        in_specs=[pl.BlockSpec(memory_space=pltpu.SMEM), hbm, vmem, vmem, vmem],
        out_specs=hbm,
        scratch_shapes=[
            pltpu.VMEM(got.shape, jnp.bfloat16),
            pltpu.VMEM((got.shape[0], ROOM), jnp.bfloat16),
            pltpu.SemaphoreType.DMA((got.shape[0] // COPY_ROWS,)),
            pltpu.SemaphoreType.DMA,
        ],
        compiler_params=pltpu.CompilerParams(vmem_limit_bytes=24 << 20),
        name="finish",
    )(flag, got, few, keys, places)


def body(block_pool, sel_index, sel_layer, counts):
    star = sel_layer[0]
    star_data, rest_data, name_data, top_data = pack(block_pool, sel_index, sel_layer, counts)
    got, few, keys, places, steps, error, full = lax.switch(
        star, [functools.partial(move, layer) for layer in range(LAYERS)],
        star_data, rest_data, name_data, top_data)

    def sparse():
        chip = lax.axis_index("own") // 2
        flag = jnp.stack([(chip == star).astype(jnp.int32), chip.astype(jnp.int32)])
        return finish(flag, got, few, keys, places), steps, error

    def dense():
        parted = flatten(block_pool, sel_index, sel_layer, counts).reshape(2 * LAYERS, CAP, TOK * HALF)
        arrived = lax.all_to_all(parted, "own", split_axis=0, concat_axis=0, tiled=True)
        arrived = arrived.reshape(2 * LAYERS * CAP, TOK * HALF)
        all_steps = peak_steps(arrived)
        codes, sums = encode(arrived, all_steps)
        return codes, all_steps, error_mean(sums)

    codes, steps, error = lax.cond(full[0] > 0, dense, sparse)
    return codes.reshape(1, 1, 2 * LAYERS, CAP, TOK * HALF), steps, error


def solution(mesh):
    return jax.shard_map(
        body,
        mesh=mesh,
        in_specs=(
            P(("own", "rep"), None, None),
            P(("own", "rep")),
            P(("own", "rep")),
            P(("own", "rep")),
        ),
        out_specs=(P("own", "rep", None, None, None), P("own", None), P("own", None)),
        check_vma=False,
    )
```

```python
import functools
import jax
import jax.numpy as jnp
from jax import lax
from jax.experimental import pallas as pl
from jax.experimental.pallas import tpu as pltpu
from jax.sharding import PartitionSpec as P

HEADROOM = 0.5
HALF = 288
PIECE = 4 * HALF
TOK = 64
STEP_TOK = 16
CAP = 8
LAYERS = 16
SEL = 32
CHIPS = 16
QS = 16
REST = SEL - CAP
ROOM = 32
BLOCK = 384
BLOCKS = 2
WIDE = PIECE + 128
DENOM = 32.0 * 4.0 * 8.0 * 64.0


def flatten_kernel(idx_ref, layer_ref, count_ref, pool_ref, out_ref, blocks, picks, seen, sems):
    step = pl.program_id(0)
    rows = STEP_TOK * LAYERS * CAP
    cols = SEL * STEP_TOK

    @pl.when(step == 0)
    def _():
        for j in range(SEL):
            pltpu.make_async_copy(pool_ref.at[idx_ref[j]], blocks.at[j], sems.at[j]).start()
        for layer in range(LAYERS):
            seen[layer] = 0
        col = lax.broadcasted_iota(jnp.int32, (1, cols), 1)
        key = jnp.full((1, cols), -1, jnp.int32)
        live = count_ref[0]
        for j in range(SEL):
            layer = layer_ref[j]
            rank = seen[layer]
            seen[layer] = rank + 1
            slot = jnp.where(j < live, layer * CAP + rank, -1)
            key = jnp.where(col // STEP_TOK == j, slot, key)
        row = lax.broadcasted_iota(jnp.int32, (rows, cols), 0)
        hit = (row % (LAYERS * CAP) == key) & (row // (LAYERS * CAP) == col % STEP_TOK)
        picks[...] = jnp.where(hit, 1.0, 0.0).astype(jnp.bfloat16)
        for j in range(SEL):
            pltpu.make_async_copy(pool_ref.at[idx_ref[j]], blocks.at[j], sems.at[j]).wait()

    start = pl.multiple_of(step * STEP_TOK, STEP_TOK)
    data = blocks[:, pl.ds(start, STEP_TOK), :].reshape(cols, 2 * HALF)
    slots = LAYERS * CAP

    @pl.loop(0, STEP_TOK // 4)
    def _(part):
        rows = pl.ds(pl.multiple_of(part * 4 * slots, 4 * slots), 4 * slots)
        moved = jnp.dot(picks[rows, :], data, preferred_element_type=jnp.float32)
        at = pl.ds(pl.multiple_of(part * PIECE, 128), PIECE)
        for half in range(2):
            lanes = [moved[t * slots:(t + 1) * slots, half * HALF:(half + 1) * HALF] for t in range(4)]
            flat = jnp.concatenate(lanes, axis=1).astype(jnp.bfloat16)
            out_ref[:, half, :, at] = flat.reshape(LAYERS, CAP, PIECE)


def flatten(block_pool, sel_index, sel_layer, counts):
    smem = pl.BlockSpec(memory_space=pltpu.SMEM)
    return pl.pallas_call(
        flatten_kernel,
        grid=(TOK // STEP_TOK,),
        out_shape=jax.ShapeDtypeStruct((LAYERS, 2, CAP, TOK * HALF), jnp.bfloat16),
        in_specs=[smem, smem, smem, pl.BlockSpec(memory_space=pl.ANY)],
        out_specs=pl.BlockSpec((LAYERS, 2, CAP, STEP_TOK * HALF), lambda i: (0, 0, 0, i)),
        scratch_shapes=[
            pltpu.VMEM((SEL, TOK, 2 * HALF), jnp.bfloat16),
            pltpu.VMEM((STEP_TOK * LAYERS * CAP, SEL * STEP_TOK), jnp.bfloat16),
            pltpu.SMEM((LAYERS,), jnp.int32),
            pltpu.SemaphoreType.DMA((SEL,)),
        ],
        compiler_params=pltpu.CompilerParams(dimension_semantics=("arbitrary",), vmem_limit_bytes=48 << 20),
        name="flatten",
    )(sel_index, sel_layer, counts, block_pool)


def rep_exchange(value, inbox, send_sems, recv_sems):
    reps = lax.axis_size("rep")
    me = lax.axis_index("rep")
    inbox[0] = value
    copies = []
    for k in range(1, reps):
        copies.append(pltpu.make_async_remote_copy(
            src_ref=inbox.at[0], dst_ref=inbox.at[k],
            send_sem=send_sems.at[k], recv_sem=recv_sems.at[k],
            device_id={"rep": lax.rem(me + k, reps)}, device_id_type=pl.DeviceIdType.MESH))
    for copy in copies:
        copy.start()
    for copy in copies:
        copy.wait()


def rep_barrier_signal():
    reps = lax.axis_size("rep")
    me = lax.axis_index("rep")
    barrier = pltpu.get_barrier_semaphore()
    for k in range(1, reps):
        pl.semaphore_signal(barrier, inc=1, device_id={"rep": lax.rem(me + k, reps)},
                            device_id_type=pl.DeviceIdType.MESH)
    return barrier


def fold4(row):
    return [row[:, k * HALF:(k + 1) * HALF] for k in range(4)]


def peak_kernel(got_ref, steps_ref, inbox, send_sems, recv_sems):
    barrier = rep_barrier_signal()
    rows = got_ref.shape[0]

    def chunk(i, peak):
        at = pl.multiple_of(i * 16, 16)
        for q in range(TOK // 4):
            part = jnp.abs(got_ref[pl.ds(at, 16), q * PIECE:(q + 1) * PIECE])
            peak = jnp.maximum(peak, part)
        return peak

    peak = lax.fori_loop(0, rows // 16, chunk, jnp.zeros((16, PIECE), jnp.bfloat16))
    row = jnp.max(peak.astype(jnp.float32), axis=0, keepdims=True)
    a, b, c, d = fold4(row)
    row = jnp.maximum(jnp.maximum(a, b), jnp.maximum(c, d))
    pl.semaphore_wait(barrier, 3)
    rep_exchange(jnp.concatenate([row, row[:, :384 - HALF]], axis=1), inbox, send_sems, recv_sems)
    top = jnp.maximum(jnp.maximum(inbox[0], inbox[1]), jnp.maximum(inbox[2], inbox[3]))
    steps_ref[...] = HEADROOM * jnp.maximum(top[:, :HALF], 1.0) / 127.0


def small_scratch():
    return [
        pltpu.VMEM((4, 1, 384), jnp.float32),
        pltpu.SemaphoreType.DMA((4,)),
        pltpu.SemaphoreType.DMA((4,)),
    ]


def peak_steps(got):
    vmem = pl.BlockSpec(memory_space=pltpu.VMEM)
    return pl.pallas_call(
        peak_kernel,
        out_shape=jax.ShapeDtypeStruct((1, HALF), jnp.float32),
        in_specs=[vmem], out_specs=vmem,
        scratch_shapes=small_scratch(),
        compiler_params=pltpu.CompilerParams(collective_id=0, has_side_effects=True, vmem_limit_bytes=24 << 20),
        name="peak_steps",
    )(got)


def error_kernel(sums_ref, out_ref, inbox, send_sems, recv_sems):
    barrier = rep_barrier_signal()
    pl.semaphore_wait(barrier, 3)
    rep_exchange(sums_ref[...], inbox, send_sems, recv_sems)
    total = (inbox[0] + inbox[1]) + (inbox[2] + inbox[3])
    out_ref[...] = total[:, :HALF] * (1.0 / DENOM)


def error_mean(sums):
    vmem = pl.BlockSpec(memory_space=pltpu.VMEM)
    return pl.pallas_call(
        error_kernel,
        out_shape=jax.ShapeDtypeStruct((1, HALF), jnp.float32),
        in_specs=[vmem], out_specs=vmem,
        scratch_shapes=small_scratch(),
        compiler_params=pltpu.CompilerParams(collective_id=1, has_side_effects=True),
        name="error_mean",
    )(sums)


ENC_ROWS = 32


def encode_kernel(got_ref, steps_ref, codes_ref, sums_ref, inv_ref, acc_ref):
    step = pl.program_id(0)

    @pl.when(step == 0)
    def _():
        inv = 1.0 / steps_ref[...]
        inv_ref[...] = jnp.broadcast_to(jnp.concatenate([inv] * 4, axis=1), inv_ref.shape)
        acc_ref[...] = jnp.zeros_like(acc_ref)

    @pl.loop(0, QS)
    def _(q):
        lanes = pl.ds(pl.multiple_of(q * PIECE, 128), PIECE)
        data = got_ref[:, lanes].reshape(ENC_ROWS // 8, 8, PIECE)
        codes_ref[:, lanes] = code_of(data, inv_ref, acc_ref).reshape(ENC_ROWS, PIECE)

    @pl.when(step == pl.num_programs(0) - 1)
    def _():
        row = jnp.sum(acc_ref[...], axis=0, keepdims=True)
        a, b, c, d = fold4(row)
        row = (a + b) + (c + d)
        sums_ref[...] = jnp.concatenate([row, row[:, :384 - HALF]], axis=1)


def encode(got, steps):
    rows = got.shape[0]
    return pl.pallas_call(
        encode_kernel,
        grid=(rows // ENC_ROWS,),
        out_shape=(jax.ShapeDtypeStruct(got.shape, jnp.bfloat16), jax.ShapeDtypeStruct((1, 384), jnp.float32)),
        in_specs=[pl.BlockSpec((ENC_ROWS, TOK * HALF), lambda i: (i, 0)), pl.BlockSpec((1, HALF), lambda i: (0, 0))],
        out_specs=(pl.BlockSpec((ENC_ROWS, TOK * HALF), lambda i: (i, 0)), pl.BlockSpec((1, 384), lambda i: (0, 0))),
        scratch_shapes=[pltpu.VMEM((8, PIECE), jnp.float32), pltpu.VMEM((8, PIECE), jnp.float32)],
        compiler_params=pltpu.CompilerParams(dimension_semantics=("arbitrary",), vmem_limit_bytes=24 << 20),
        name="encode",
    )(got, steps)


def pack_kernel(idx_ref, layer_ref, count_ref, pool_ref, star_ref, rest_ref, name_ref, top_ref, blocks, picks, tops, sems):
    step = pl.program_id(0)
    size = SEL * STEP_TOK

    @pl.when(step == 0)
    def _():
        for group in range(TOK // STEP_TOK):
            part = pl.ds(group * STEP_TOK, STEP_TOK)
            for j in range(SEL):
                pltpu.make_async_copy(pool_ref.at[idx_ref[j], part], blocks.at[j, part], sems.at[group]).start()
        row = lax.broadcasted_iota(jnp.int32, (size, size), 0)
        col = lax.broadcasted_iota(jnp.int32, (size, size), 1)
        hit = (row % SEL == col // STEP_TOK) & (row // SEL == col % STEP_TOK)
        picks[...] = jnp.where(hit, 1.0, 0.0).astype(jnp.bfloat16)
        tops[...] = jnp.zeros_like(tops)
        line = lax.broadcasted_iota(jnp.int32, (8, 128), 1)
        layers = jnp.full((8, 128), -1.0, jnp.float32)
        live = count_ref[0]
        for j in range(CAP, SEL):
            name = jnp.where(j < live, layer_ref[j], -1).astype(jnp.float32)
            layers = jnp.where(line == j - CAP, name, layers)
        name_ref[...] = layers.astype(jnp.bfloat16)

    start = pl.multiple_of(step * STEP_TOK, STEP_TOK)
    now = pl.ds(start, STEP_TOK)
    pltpu.make_async_copy(pool_ref.at[pl.ds(0, SEL), now], blocks.at[:, now], sems.at[step]).wait()
    data = blocks[:, pl.ds(start, STEP_TOK), :].reshape(size, 2 * HALF)
    moved = jnp.dot(picks[...], data, preferred_element_type=jnp.float32)
    for part in range(STEP_TOK // 4):
        for half in range(2):
            first = part * 4
            lanes = [moved[t * SEL:(t + 1) * SEL, half * HALF:(half + 1) * HALF] for t in range(first, first + 4)]
            flat = jnp.concatenate(lanes, axis=1)
            star_ref[half, part] = flat[:CAP].astype(jnp.bfloat16)
            rest_ref[part, half] = flat[CAP:].astype(jnp.bfloat16)
            tops[half] = jnp.maximum(tops[half], jnp.abs(flat[:CAP]))

    @pl.when(step == pl.num_programs(0) - 1)
    def _():
        for half in range(2):
            top_ref[half] = pad_row(fold_max(jnp.max(tops[half], axis=0, keepdims=True)))


def fold_max(row):
    a, b, c, d = fold4(row)
    return jnp.maximum(jnp.maximum(a, b), jnp.maximum(c, d))


def pad_row(row):
    return jnp.concatenate([row, jnp.zeros((1, 384 - HALF), jnp.float32)], axis=1)


def pack(block_pool, sel_index, sel_layer, counts):
    smem = pl.BlockSpec(memory_space=pltpu.SMEM)
    parts = STEP_TOK // 4
    return pl.pallas_call(
        pack_kernel,
        grid=(TOK // STEP_TOK,),
        out_shape=(
            jax.ShapeDtypeStruct((2, QS, CAP, PIECE), jnp.bfloat16),
            jax.ShapeDtypeStruct((QS, 2, REST, PIECE), jnp.bfloat16),
            jax.ShapeDtypeStruct((8, 128), jnp.bfloat16),
            jax.ShapeDtypeStruct((2, 1, 384), jnp.float32),
        ),
        in_specs=[smem, smem, smem, pl.BlockSpec(memory_space=pl.ANY)],
        out_specs=(
            pl.BlockSpec((2, parts, CAP, PIECE), lambda i: (0, i, 0, 0)),
            pl.BlockSpec((parts, 2, REST, PIECE), lambda i: (i, 0, 0, 0)),
            pl.BlockSpec((8, 128), lambda i: (0, 0)),
            pl.BlockSpec((2, 1, 384), lambda i: (0, 0, 0)),
        ),
        scratch_shapes=[
            pltpu.VMEM((SEL, TOK, 2 * HALF), jnp.bfloat16),
            pltpu.VMEM((SEL * STEP_TOK, SEL * STEP_TOK), jnp.bfloat16),
            pltpu.VMEM((2, CAP, PIECE), jnp.float32),
            pltpu.SemaphoreType.DMA((TOK // STEP_TOK,)),
        ],
        compiler_params=pltpu.CompilerParams(dimension_semantics=("arbitrary",), vmem_limit_bytes=24 << 20),
        name="pack",
    )(sel_index, sel_layer, counts, block_pool)


def tree(star):
    sx, sz = divmod(star, 4)

    def at(dx, dz):
        return (sx + dx) % 4 * 4 + (sz + dz) % 4

    near = [at(0, 1), at(1, 0), at(0, 3), at(3, 0)]
    diag = [at(1, 1), at(1, 3), at(3, 3), at(3, 1)]
    third = [at(1, 2), at(2, 3), at(3, 2), at(2, 1)]
    far = at(2, 2)
    over_z, over_x = at(0, 2), at(2, 0)
    role = {star: 0, far: 4, over_z: 2, over_x: 4, third[0]: 4, third[2]: 4}
    count, hop, up, origin, shift = {over_z: 8}, {}, {over_z: near[0]}, {}, {}
    light = 2 if sz % 2 == 0 else 0
    for r in range(4):
        role[near[r]], role[diag[r]] = 1, 2
        up[near[r]], up[diag[r]] = star, near[r]
        count[near[r]], count[diag[r]] = (12, 4) if r % 2 == 0 else (8, 2)
        hop[diag[r]] = [(near[r], k) for k in range(4)]
    count[near[light]] = 16
    for r in (1, 3):
        role[third[r]] = 3
        up[third[r]] = diag[r]
        count[third[r]] = 2
    hop[third[0]] = [(over_z, k) for k in range(4)]
    hop[third[2]] = [(over_z, 4 + k) for k in range(4)]
    hop[third[3]] = [(diag[0], k) for k in range(4)]
    hop[third[1]] = [(diag[2], k) for k in range(4)]
    hop[far] = [(third[1], 0), (third[1], 1), (third[3], 0), (third[3], 1)]
    hop[over_z] = [(near[light], 12 + k) for k in range(4)]
    hop[over_x] = [(near[1], 12), (near[1], 13), (near[3], 12), (near[3], 13)]
    origin[near[0]] = (diag[0], third[0], third[3], over_z)
    origin[near[2]] = (diag[2], third[2], third[1], over_z)
    origin[near[1]] = (diag[1], far, far, over_x)
    origin[near[3]] = (diag[3], far, far, over_x)
    shift[near[0]], shift[near[1]], shift[near[2]], shift[near[3]] = (0, 0), (0, 0), (0, 0), (2, 2)
    away = {at(dx, dz): (dx - 1) * 3 + dz - 1 for dx in range(1, 4) for dz in range(1, 4)}
    arrival = [star, *near, *diag, over_x, over_z, third[0], third[2], far, third[1], third[3]]
    return role, count, hop, up, origin, shift, away, dict(enumerate(arrival))


ORDER = {4: 1, 5: 0, 6: 3, 7: 2, 12: 3, 13: 0, 14: 1, 15: 2, 8: 2, 9: 0, 10: 1, 11: 3, 0: 1, 1: 3, 2: 2, 3: 0}


def turn(chip, step):
    lead = lax.rem(step, 4)
    dx = jnp.where(lead == 0, 1, jnp.where(lead == 1, 3, jnp.where(lead == 2, 2, 0)))
    dz = pick(dx * 4 + step // 4, ORDER)
    return lax.rem(chip // 4 + dx, 4) * 4 + lax.rem(lax.rem(chip, 4) + dz, 4)


def pick(index, table, default=0):
    out = jnp.int32(default)
    for key, value in table.items():
        out = jnp.where(index == key, jnp.int32(value), out)
    return out


MESH = pl.DeviceIdType.MESH


def sort_masks(before, same, spread, own_lane, local):
    @pl.loop(0, BLOCK // 16)
    def _(i):
        rows = pl.ds(pl.multiple_of(i * 16, 16), 16)

        def grid(width):
            row = lax.broadcasted_iota(jnp.int32, (16, width), 0) + i * 16
            return row, lax.broadcasted_iota(jnp.int32, (16, width), 1)

        row, col = grid(BLOCK)
        before[rows, :] = jnp.where(col < row, 1.0, 0.0).astype(jnp.bfloat16)
        same[rows, :] = jnp.where((col < row) & (col // REST == row // REST), 1.0, 0.0).astype(jnp.bfloat16)
        row, col = grid(BLOCK // REST)
        spread[rows, :] = jnp.where(row // REST == col, 1.0, 0.0).astype(jnp.bfloat16)
        row, col = grid(128)
        own_lane[rows, :] = jnp.where(row % REST == col, 1.0, 0.0)
        local[rows, :] = (row // REST).astype(jnp.float32)


def sort_mail(names_ref, chip, key_ref, place_ref, select, before, same, spread, own_lane, local):
    sources = BLOCK // REST
    lane = lax.broadcasted_iota(jnp.int32, (BLOCK, 128), 1).astype(jnp.float32)
    mine = chip.astype(jnp.float32)

    def block(i, carry):
        lists = jnp.max(names_ref[pl.ds(i * sources, sources)].astype(jnp.float32), axis=1).astype(jnp.bfloat16)
        lists = jnp.dot(spread[...], lists, preferred_element_type=jnp.float32)
        names = jnp.sum(lists * own_lane[...], axis=1, keepdims=True)
        hits = jnp.where(names == lane, 1.0, 0.0)
        hits16 = hits.astype(jnp.bfloat16)
        rank = jnp.dot(before[...], hits16, preferred_element_type=jnp.float32) + carry
        slot = jnp.dot(same[...], hits16, preferred_element_type=jnp.float32)
        rank = jnp.sum(rank * hits, axis=1, keepdims=True)
        slot = jnp.sum(slot * hits, axis=1, keepdims=True)
        source = local[...] + (i * sources).astype(jnp.float32)
        key = jnp.where(rank < ROOM, names * ROOM + rank, -1.0)
        place = jnp.where(names == mine, source * CAP + slot, -1.0)
        key_ref[i] = jnp.transpose(key)[:1]
        place_ref[i] = jnp.transpose(place)[:1]
        return carry + jnp.sum(hits, axis=0, keepdims=True)

    total = lax.fori_loop(0, BLOCKS, block, jnp.zeros((1, 128), jnp.float32))

    @pl.loop(0, CHIPS)
    def _(layer):
        at = pl.multiple_of(layer * ROOM, ROOM)
        want = (lax.broadcasted_iota(jnp.int32, (ROOM, BLOCK), 0) + at).astype(jnp.float32)
        for i in range(BLOCKS):
            hit = jnp.where(want == key_ref[i], 1.0, 0.0).astype(jnp.bfloat16)
            select[pl.ds(at, ROOM), i * BLOCK:(i + 1) * BLOCK] = hit

    return total


def code_of(data, inv, acc):
    scaled = data.astype(jnp.float32) * inv[...][None]
    code = jnp.clip(scaled, -127.0, 127.0).astype(jnp.bfloat16)
    gap = scaled - code.astype(jnp.float32)
    acc[...] += jnp.sum(gap * gap, axis=0)
    return code


def move_kernel(star, star_ref, rest_ref, name_ref, top_ref, got_ref, few_ref, key_ref, place_ref, steps_ref, error_ref, full_ref,
                before, same, spread, own_lane, local, mail, names, select, chosen, inbox, relay, tops, inrep, inrep2, land, stage, inv, acc,
                mail_send, mail_recv, few_send, few_recv, own_send, pass_send, relay_recv, star_recv,
                top_send, top_recv, rep_send, rep_recv, sum_send, sum_recv, out_sem):
    own = lax.axis_index("own")
    rep = lax.axis_index("rep")
    n_own = 2 * CHIPS
    chip = own // 2
    core = own % 2
    role_of, count_of, hop_of, up_of, origin_of, shift_of, away_of, arrival_of = tree(star)
    role = pick(chip, role_of)
    up = pick(chip, up_of)
    count = pick(chip, count_of)
    tile = pick(chip, away_of, -1)
    over_z = star // 4 * 4 + (star + 2) % 4
    other_near = star // 4 * 4 + (star + 3) % 4
    is_star = role == 0
    not_star = role != 0

    barrier = pltpu.get_barrier_semaphore()

    @pl.loop(1, n_own)
    def _(k):
        pl.semaphore_signal(barrier, inc=1, device_id={"own": lax.rem(own + k, n_own)}, device_id_type=MESH)

    for k in range(1, 4):
        pl.semaphore_signal(barrier, inc=1, device_id={"rep": lax.rem(rep + k, 4)}, device_id_type=MESH)
    pl.semaphore_wait(barrier, n_own - 1 + 3)

    def remote(src, dst, send, recv, to):
        return pltpu.make_async_remote_copy(src_ref=src, dst_ref=dst, send_sem=send, recv_sem=recv,
                                            device_id={"own": to}, device_id_type=MESH)

    def mail_copy(to, frm):
        return remote(rest_ref.at[to // 2, to % 2], mail.at[frm, :, pl.ds(0, PIECE)], mail_send.at[0], mail_recv.at[0], to)

    def name_copy(to):
        return remote(name_ref, names.at[own], mail_send.at[1], mail_recv.at[2], to)

    def lane_of(which):
        return pl.ds(pl.multiple_of(which * 128, 128), 128)

    def extra_copy(to_chip, half):
        return remote(rest_ref.at[star, half, :, lane_of(pick(to_chip, away_of))], mail.at[own, :, pl.ds(PIECE, 128)],
                      mail_send.at[2], mail_recv.at[1], 2 * to_chip + half)

    def top_copy(half, frm):
        return remote(top_ref.at[half], tops.at[frm], top_send.at[half], top_recv.at[0], 2 * star + half)

    for half in range(2):
        @pl.when(own != 2 * star + half)
        def _():
            top_copy(half, own).start()

        @pl.when(own == 2 * star + half)
        def _():
            tops[own] = top_ref[half]

    def near_copy(half):
        return remote(star_ref.at[half], land.at[own], own_send.at[0], star_recv.at[own], 2 * star + half)

    def hop_copy(k):
        to = pick(chip, {c: h[k][0] for c, h in hop_of.items()}) * 2 + core
        slot = pick(chip, {c: h[k][1] for c, h in hop_of.items()})
        return remote(star_ref.at[:, pl.ds(4 * k, 4)], relay.at[slot], own_send.at[0], relay_recv.at[slot], to)

    @pl.when(role == 1)
    def _():
        for half in range(2):
            near_copy(half).start()

    @pl.when(role > 1)
    def _():
        for k in range(4):
            hop_copy(k).start()

    def partner_copy():
        return remote(star_ref.at[1 - core], land.at[own], own_send.at[0], star_recv.at[own], 2 * star + 1 - core)

    @pl.when(is_star)
    def _():
        partner_copy().start()

        @pl.loop(0, QS)
        def _(q):
            land[own, q] = star_ref[core, q]

    @pl.loop(0, n_own)
    def _(k):
        half = lax.rem(k, 2)
        to_chip = turn(chip, k // 2)

        @pl.when(2 * to_chip + half != own)
        def _():
            name_copy(2 * to_chip + half).start()

        @pl.when((to_chip != star) & (2 * to_chip + half != own))
        def _():
            mail_copy(2 * to_chip + half, own).start()

        @pl.when((pick(to_chip, away_of, -1) >= 0) & (2 * to_chip + half != own))
        def _():
            extra_copy(to_chip, half).start()

    def relay_in(k):
        return remote(relay.at[k], relay.at[k], pass_send.at[0], relay_recv.at[k], own)

    def pass_near(k, half):
        group = k // 4
        origins = [pick(chip, {c: o[i] for c, o in origin_of.items()}) for i in range(4)]
        origin = jnp.where(group == 0, origins[0], jnp.where(group == 1, origins[1],
                           jnp.where(group == 2, origins[2], origins[3])))
        shifts = [pick(chip, {c: o[i] for c, o in shift_of.items()}) for i in range(2)]
        quarter = lax.rem(k, 4) + jnp.where(group == 1, shifts[0], jnp.where(group == 3, shifts[1], 0))
        frm = 2 * origin + core
        return remote(relay.at[k, half], land.at[frm, pl.ds(4 * quarter, 4)],
                      pass_send.at[0], star_recv.at[frm], 2 * star + half)

    def pass_diag(k):
        slot = jnp.where(chip == over_z, 4 + lax.rem(k, 4), jnp.where(count == 4, 8 + k, 4 + k))
        to = jnp.where((chip == over_z) & (k >= 4), other_near, up)
        return remote(relay.at[k], relay.at[slot], pass_send.at[0], relay_recv.at[slot], 2 * to + core)

    def pass_third(k):
        return remote(relay.at[k], relay.at[k], pass_send.at[0], relay_recv.at[k], 2 * up + core)

    def near_order(i):
        straight = jnp.where(count == 16, 4, jnp.where(count == 8, 2, 0))
        return jnp.where(i < 4, i, jnp.where(i < 4 + straight, i + 8, i - straight))

    def pass_near_range(low, high):
        @pl.when(role == 1)
        def _():
            @pl.loop(low, high)
            def _(i):
                k = near_order(i)
                relay_in(k).wait_recv()
                for half in range(2):
                    pass_near(k, half).start()

    def pass_diag_range(low, high):
        @pl.when(role == 2)
        def _():
            @pl.loop(low, high)
            def _(k):
                relay_in(k).wait_recv()
                pass_diag(k).start()

    sort_masks(before, same, spread, own_lane, local)
    early_diag = jnp.where(count == 2, 0, count)
    early_near = jnp.where(count == 16, 8, jnp.where(count == 12, 8, 6))
    pass_diag_range(0, early_diag)
    pass_near_range(0, early_near)

    def mail_part(size, which):
        ref = mail.at[pl.ds(0, size), :, pl.ds(0, PIECE)]
        return remote(ref, ref, mail_send.at[which], mail_recv.at[0], own)

    def name_all():
        ref = names.at[pl.ds(0, n_own - 1)]
        return remote(ref, ref, mail_send.at[1], mail_recv.at[2], own)

    def extra_part(size):
        ref = mail.at[pl.ds(0, size), :, pl.ds(PIECE, 128)]
        return remote(ref, ref, mail_send.at[2], mail_recv.at[1], own)

    @pl.when(not_star)
    def _():
        mail[own, :, :PIECE] = rest_ref[chip, core]
        mail_part(n_own - 1, 0).wait_recv()

    @pl.when(tile >= 0)
    def _():
        mail[own, :, PIECE:] = rest_ref[star, core, :, lane_of(tile)]
        extra_part(n_own - 1).wait_recv()

    names[own] = name_ref[...]
    name_all().wait_recv()
    count_by_layer = sort_mail(names, chip, key_ref, place_ref, select, before, same, spread, own_lane, local)

    parts = PIECE // 128

    @pl.loop(0, jnp.where(is_star, 0, jnp.where(tile >= 0, parts + 1, parts)))
    def _(part):
        data = mail[:, :, lane_of(part)].reshape(n_own * REST, 128)
        for rows in range(2):
            size = CHIPS * ROOM // 2
            out = jnp.dot(select[rows * size:(rows + 1) * size], data, preferred_element_type=jnp.float32)
            chosen[rows * 8:(rows + 1) * 8, :, lane_of(part)] = out.astype(jnp.bfloat16).reshape(8, ROOM, 128)

    def few_copy(to):
        return remote(chosen.at[to, :, pl.ds(0, PIECE)], inbox.at[chip], few_send.at[0], few_recv.at[0], 2 * to + core)

    def tile_copy(to):
        return remote(chosen.at[to, :, pl.ds(PIECE, 128)], inbox.at[star, :, lane_of(tile)], few_send.at[1], few_recv.at[1], 2 * to + core)

    def few_part(size):
        part = pl.ds(0, size)
        return remote(inbox.at[part], inbox.at[part], few_send.at[0], few_recv.at[0], own)

    def tile_part(size, lanes):
        ref = inbox.at[pl.ds(0, size), :, pl.ds(0, lanes)]
        return remote(ref, ref, few_send.at[1], few_recv.at[1], own)

    @pl.loop(0, CHIPS)
    def _(k):
        to = turn(chip, k)

        @pl.when((to != star) & (to != chip) & not_star)
        def _():
            few_copy(to).start()

            @pl.when(tile >= 0)
            def _():
                tile_copy(to).start()

    @pl.when(role == 3)
    def _():
        @pl.loop(0, 2)
        def _(k):
            relay_in(k).wait_recv()
            pass_third(k).start()

    pass_diag_range(early_diag, count)
    pass_near_range(early_near, count)

    @pl.when(not_star)
    def _():
        inbox[chip] = chosen[chip, :, :PIECE]

        @pl.when(tile >= 0)
        def _():
            inbox[star, :, lane_of(tile)] = chosen[chip, :, PIECE:]
            tile_part(1, 1024).wait_recv()

        @pl.when(tile < 0)
        def _():
            tile_part(1, PIECE).wait_recv()


        few_part(CHIPS - 2).wait_recv()

        def largest(q, best):
            return jnp.maximum(best, jnp.abs(inbox[q]))

        best = lax.fori_loop(0, QS, largest, jnp.zeros((ROOM, PIECE), jnp.bfloat16))
        inrep[0] = pad_row(fold_max(jnp.max(best.astype(jnp.float32), axis=0, keepdims=True)))

    @pl.when(is_star)
    def _():
        others = pl.ds(0, n_own - 1)
        remote(tops.at[others], tops.at[others], top_send.at[0], top_recv.at[0], own).wait_recv()

        inrep[0] = jnp.max(tops[...], axis=0)

    full = jnp.max(jnp.where(count_by_layer > ROOM, 1.0, 0.0), axis=1, keepdims=True)
    tail = lax.broadcasted_iota(jnp.int32, (1, 384), 1)
    inrep[0] = jnp.where(tail < HALF, inrep[0], full)

    rep_exchange(inrep[0], inrep, rep_send, rep_recv)
    top = jnp.maximum(jnp.maximum(inrep[0], inrep[1]), jnp.maximum(inrep[2], inrep[3]))
    steps = HEADROOM * jnp.maximum(top[:, :HALF], 1.0) / 127.0
    steps_ref[...] = steps
    full_ref[0] = jnp.max(jnp.where(tail < HALF, 0.0, top)).astype(jnp.int32)
    inv[...] = jnp.broadcast_to(jnp.concatenate([1.0 / steps] * 4, axis=1), inv.shape)
    acc[...] = jnp.zeros_like(acc)

    @pl.when(not_star)
    def _():
        @pl.loop(0, QS)
        def _(q):
            few_ref[q] = code_of(inbox[q].reshape(ROOM // 8, 8, PIECE), inv, acc).reshape(ROOM, PIECE)

    @pl.when(is_star)
    def _():
        @pl.loop(0, n_own)
        def _(k):
            slot = lax.rem(k, 2)
            frm = 2 * pick(k // 2, arrival_of) + slot
            out = pltpu.make_async_copy(stage.at[slot], got_ref.at[pl.ds(pl.multiple_of(8 * frm, 8), 8)], out_sem.at[slot])

            @pl.when(frm != own)
            def _():
                remote(land.at[frm], land.at[frm], own_send.at[0], star_recv.at[frm], own).wait_recv()

            @pl.when(k > 1)
            def _():
                out.wait()

            @pl.loop(0, QS // 2)
            def _(pair):
                for half in range(2):
                    q = 2 * pair + half
                    code = code_of(land[frm, pl.ds(q, 1)], inv, acc)
                    stage[slot, :, pl.ds(pl.multiple_of(q * PIECE, 128), PIECE)] = code[0]

            out.start()

    row = jnp.sum(acc[...], axis=0, keepdims=True)
    a, b, c, d = fold4(row)
    rep_exchange(pad_row((a + b) + (c + d)), inrep2, sum_send, sum_recv)
    total = (inrep2[0] + inrep2[1]) + (inrep2[2] + inrep2[3])
    error_ref[...] = total[:, :HALF] * (1.0 / DENOM)

    name_all().wait_send()

    def own_all():
        return remote(star_ref, star_ref, own_send.at[0], star_recv.at[0], own)

    def pass_all(size):
        return remote(relay.at[pl.ds(0, size)], relay.at[pl.ds(0, size)], pass_send.at[0], star_recv.at[0], own)

    @pl.when(is_star)
    def _():
        for c in range(2):
            pltpu.make_async_copy(stage.at[c], got_ref.at[pl.ds(0, 8)], out_sem.at[c]).wait()

        partner_copy().wait_send()

    @pl.when(role == 1)
    def _():
        own_all().wait_send()

    @pl.when(role > 1)
    def _():
        own_all().wait_send()

    for size in (2, 4, 8, 12, 16):
        @pl.when(count == size)
        def _():
            pass_all(size).wait_send()

    for half in range(2):
        @pl.when(own != 2 * star + half)
        def _():
            top_copy(half, own).wait_send()

    @pl.when(is_star)
    def _():
        mail_part(n_own - 2, 0).wait_send()

    @pl.when(not_star)
    def _():
        mail_part(n_own - 3, 0).wait_send()

    @pl.when(tile >= 0)
    def _():
        extra_part(17).wait_send()

    @pl.when(tile < 0)
    def _():
        extra_part(18).wait_send()

    @pl.when(not_star)
    def _():
        few_part(CHIPS - 2).wait_send()

    @pl.when(tile >= 0)
    def _():
        tile_part(CHIPS - 2, 128).wait_send()


def move(star, star_data, rest_data, name_data, top_data):
    vmem = pl.BlockSpec(memory_space=pltpu.VMEM)
    dma = pltpu.SemaphoreType.DMA
    n_own = 2 * CHIPS
    return pl.pallas_call(
        functools.partial(move_kernel, star),
        out_shape=(
            jax.ShapeDtypeStruct((n_own * CAP, TOK * HALF), jnp.bfloat16),
            jax.ShapeDtypeStruct((QS, ROOM, PIECE), jnp.bfloat16),
            jax.ShapeDtypeStruct((BLOCKS, 1, BLOCK), jnp.float32),
            jax.ShapeDtypeStruct((BLOCKS, 1, BLOCK), jnp.float32),
            jax.ShapeDtypeStruct((1, HALF), jnp.float32),
            jax.ShapeDtypeStruct((1, HALF), jnp.float32),
            jax.ShapeDtypeStruct((1,), jnp.int32),
        ),
        in_specs=[vmem, vmem, vmem, vmem],
        out_specs=(pl.BlockSpec(memory_space=pl.ANY), vmem, vmem, vmem, vmem, vmem, pl.BlockSpec(memory_space=pltpu.SMEM)),
        scratch_shapes=[
            pltpu.VMEM((BLOCK, BLOCK), jnp.bfloat16),
            pltpu.VMEM((BLOCK, BLOCK), jnp.bfloat16),
            pltpu.VMEM((BLOCK, BLOCK // REST), jnp.bfloat16),
            pltpu.VMEM((BLOCK, 128), jnp.float32),
            pltpu.VMEM((BLOCK, 128), jnp.float32),
            pltpu.VMEM((n_own, REST, WIDE), jnp.bfloat16),
            pltpu.VMEM((n_own, 8, 128), jnp.bfloat16),
            pltpu.VMEM((CHIPS * ROOM, n_own * REST), jnp.bfloat16),
            pltpu.VMEM((CHIPS, ROOM, WIDE), jnp.bfloat16),
            pltpu.VMEM((CHIPS, ROOM, PIECE), jnp.bfloat16),
            pltpu.VMEM((16, 2, 4, CAP, PIECE), jnp.bfloat16),
            pltpu.VMEM((n_own, 1, 384), jnp.float32),
            pltpu.VMEM((4, 1, 384), jnp.float32),
            pltpu.VMEM((4, 1, 384), jnp.float32),
            pltpu.VMEM((n_own, QS, CAP, PIECE), jnp.bfloat16),
            pltpu.VMEM((2, CAP, TOK * HALF), jnp.bfloat16),
            pltpu.VMEM((8, PIECE), jnp.float32),
            pltpu.VMEM((8, PIECE), jnp.float32),
            dma((3,)), dma((3,)), dma((2,)), dma((2,)),
            dma((1,)), dma((1,)), dma((16,)), dma((n_own,)),
            dma((2,)), dma((1,)), dma((4,)), dma((4,)), dma((4,)), dma((4,)), dma((2,)),
        ],
        compiler_params=pltpu.CompilerParams(collective_id=2 + star, has_side_effects=True, vmem_limit_bytes=40 << 20),
        name="move",
    )(star_data, rest_data, name_data, top_data)


COPY_ROWS = 16


def finish_kernel(flag_ref, got_ref, few_ref, key_ref, place_ref, codes_ref, buf, map_ref, in_sems, out_sem):
    rows = buf.shape[0]
    star = flag_ref[0] != 0

    def block(i):
        return pl.ds(pl.multiple_of(i * COPY_ROWS, COPY_ROWS), COPY_ROWS)

    def load(i):
        return pltpu.make_async_copy(got_ref.at[block(i)], buf.at[block(i)], in_sems.at[i])

    def save(i):
        return pltpu.make_async_copy(buf.at[block(i)], codes_ref.at[block(i)], out_sem)

    @pl.when(star)
    def _():
        @pl.loop(0, rows // COPY_ROWS)
        def _(i):
            load(i).start()

        @pl.loop(0, rows // COPY_ROWS)
        def _(i):
            load(i).wait()
            save(i).start()

    @pl.when(jnp.logical_not(star))
    def _():
        first = (lax.broadcasted_iota(jnp.int32, (ROOM, BLOCK), 0) + flag_ref[1] * ROOM).astype(jnp.float32)
        spot = lax.broadcasted_iota(jnp.int32, (rows, BLOCK), 0).astype(jnp.float32)
        total = jnp.zeros((rows, ROOM), jnp.float32)
        for i in range(BLOCKS):
            spread = jnp.where(spot == place_ref[i], 1.0, 0.0).astype(jnp.bfloat16)
            ranked = jnp.where(first == key_ref[i], 1.0, 0.0).astype(jnp.bfloat16)
            total += lax.dot_general(spread, ranked, (((1,), (1,)), ((), ())), preferred_element_type=jnp.float32)
        map_ref[...] = total.astype(jnp.bfloat16)

        @pl.loop(0, QS)
        def _(q):
            lanes = pl.ds(pl.multiple_of(q * PIECE, 128), PIECE)
            out = jnp.dot(map_ref[...], few_ref[q], preferred_element_type=jnp.float32)
            buf[:, lanes] = out.astype(jnp.bfloat16)
            pltpu.make_async_copy(buf.at[:, lanes], codes_ref.at[:, lanes], out_sem).start()

    pltpu.make_async_copy(buf, codes_ref, out_sem).wait()


def finish(flag, got, few, keys, places):
    vmem = pl.BlockSpec(memory_space=pltpu.VMEM)
    hbm = pl.BlockSpec(memory_space=pl.ANY)
    return pl.pallas_call(
        finish_kernel,
        out_shape=jax.ShapeDtypeStruct(got.shape, jnp.bfloat16),
        in_specs=[pl.BlockSpec(memory_space=pltpu.SMEM), hbm, vmem, vmem, vmem],
        out_specs=hbm,
        scratch_shapes=[
            pltpu.VMEM(got.shape, jnp.bfloat16),
            pltpu.VMEM((got.shape[0], ROOM), jnp.bfloat16),
            pltpu.SemaphoreType.DMA((got.shape[0] // COPY_ROWS,)),
            pltpu.SemaphoreType.DMA,
        ],
        compiler_params=pltpu.CompilerParams(vmem_limit_bytes=24 << 20),
        name="finish",
    )(flag, got, few, keys, places)


def body(block_pool, sel_index, sel_layer, counts):
    star = sel_layer[0]
    star_data, rest_data, name_data, top_data = pack(block_pool, sel_index, sel_layer, counts)
    got, few, keys, places, steps, error, full = lax.switch(
        star, [functools.partial(move, layer) for layer in range(LAYERS)],
        star_data, rest_data, name_data, top_data)

    def sparse():
        chip = lax.axis_index("own") // 2
        flag = jnp.stack([(chip == star).astype(jnp.int32), chip.astype(jnp.int32)])
        return finish(flag, got, few, keys, places), steps, error

    def dense():
        parted = flatten(block_pool, sel_index, sel_layer, counts).reshape(2 * LAYERS, CAP, TOK * HALF)
        arrived = lax.all_to_all(parted, "own", split_axis=0, concat_axis=0, tiled=True)
        arrived = arrived.reshape(2 * LAYERS * CAP, TOK * HALF)
        all_steps = peak_steps(arrived)
        codes, sums = encode(arrived, all_steps)
        return codes, all_steps, error_mean(sums)

    codes, steps, error = lax.cond(full[0] > 0, dense, sparse)
    return codes.reshape(1, 1, 2 * LAYERS, CAP, TOK * HALF), steps, error


def solution(mesh):
    return jax.shard_map(
        body,
        mesh=mesh,
        in_specs=(
            P(("own", "rep"), None, None),
            P(("own", "rep")),
            P(("own", "rep")),
            P(("own", "rep")),
        ),
        out_specs=(P("own", "rep", None, None, None), P("own", None), P("own", None)),
        check_vma=False,
    )
```
